32 devices in a mesh: gx: 8 (over z, x), gy: 4 (over y, core).
Axes of the slice: x: 2, y: 2, z: 4, core: 2. Of those that a mesh axis runs over, the one named last changes fastest.
Arguments:
- velocity: float32 [2, 1024, 1024], P(None, 'gy', 'gx'), may hold values from -3 to 3
- stress: float32 [3, 1024, 1024], P(None, 'gy', 'gx'), may hold values from -3 to 3
- ice_mass: float32 [1024, 1024], P('gy', 'gx'), may hold values from 0.5 to 4
- strength: float32 [1024, 1024], P('gy', 'gx'), may hold values from 0.2 to 2
- land_mask: int32 [1024, 1024], P('gy', 'gx'), may hold values from 0 to 1
- ocean_forcing: float32 [4, 1024, 1024], P(None, ('gy', 'gx')), may hold values from -3 to 3
Outputs:
- velocity_out: float32 [2, 1024, 1024], P(None, 'gy', 'gx')
- stress_out: float32 [3, 1024, 1024], P(None, 'gy', 'gx')
- residuals: float32 [4], replicated
- ocean_stress: float32 [2, 1024, 1024], P(None, ('gy', 'gx'))
The draws below stay inside these ranges and needn't reach their ends.
All inputs are finite; a program needn't handle non-finite values.
Results may differ from the reference program's by a relative error of at most 0.0001.
Values sent between devices are 32-bit elements; how exact they have to be, the bound alone decides.
A program may use at most 64 MiB of HBM per device.

```python
import math
import jax
import jax.numpy as jnp
from jax import lax

ITERS = 4
NX = 1024
NY = 1024


def draw_land_mask(key, part):
    lon_index = lax.broadcasted_iota(jnp.int32, (NY, NX), 1)
    lat_index = lax.broadcasted_iota(jnp.int32, (NY, NX), 0)
    threshold = 100 + 300 * lon_index // NX + 300 * lat_index // NY
    rolled = jax.random.randint(jax.random.fold_in(key, 17), (NY, NX), 0, 1000)
    return (rolled >= threshold).astype(jnp.int32)


def levels(stream_key, shape, pieces, low, largest):
    def one(axis_at, blocks):
        steps = jax.random.uniform(jax.random.fold_in(jax.random.fold_in(stream_key, 6), axis_at), (blocks,), jnp.float32, low / len(pieces), largest / len(pieces))
        return jnp.repeat(jnp.exp(steps), shape[axis_at] // blocks).reshape((-1,) + (1,) * (len(shape) - axis_at - 1))

    gain = one(*pieces[0])
    for cut in pieces[1:]:
        gain = gain * one(*cut)
    return gain


def normal_values(key, shape, deviation, bound, cuts=(), dtype=jnp.bfloat16):
    level = levels(key, shape, cuts, -0.22, 0.18) if cuts else 1.0
    values = jax.random.normal(key, shape, jnp.float32) * deviation * level
    return jnp.minimum(jnp.maximum(values, -bound), bound).astype(dtype)


def setup_inputs(seed: int = 0) -> dict:
    key_list = jax.random.split(jax.random.key(seed), 7)
    return {
        "velocity": normal_values(key_list[0], (2, NY, NX), 0.5, 3.0, ((1, 4), (2, 8)), jnp.float32),
        "stress": normal_values(key_list[1], (3, NY, NX), 0.5, 3.0, ((1, 4), (2, 8)), jnp.float32),
        "ice_mass": jnp.clip(jnp.exp(math.log(4.0) - 2.0794415 * jax.random.uniform(key_list[2], (NY, NX), jnp.float32) ** levels(key_list[2], (NY, NX), ((0, 4), (1, 8)), -0.2, 0.2)), 0.5, 4.0),
        "strength": jnp.clip(jnp.exp(math.log(2.0) - 2.3025851 * jax.random.uniform(key_list[3], (NY, NX), jnp.float32) ** levels(key_list[3], (NY, NX), ((0, 4), (1, 8)), -0.2, 0.2)), 0.2, 2.0),
        "land_mask": draw_land_mask(jax.random.fold_in(key_list[6], 71), 0),
        "ocean_forcing": normal_values(key_list[5], (4, NY, NX), 0.5, 3.0, ((1, 32),), jnp.float32),
    }


ALPHA = 4.0
BETA = 4.0
WATER_DRAG = 1.0
DELTA_FLOOR = 0.0025

def extend_field(field):
    wrapped = jnp.concatenate([field[..., -1:], field, field[..., :1]], axis=-1)
    padding = [(0, 0)] * (field.ndim - 2) + [(1, 1), (0, 0)]
    return jnp.pad(wrapped, padding)

def diff_east(padded):
    return 0.5 * (padded[..., 1:-1, 2:] - padded[..., 1:-1, :-2])

def diff_north(padded):
    return 0.5 * (padded[..., 2:, 1:-1] - padded[..., :-2, 1:-1])

def relax_stress(padded_vel, stress, strength, ice_frac):
    east_dx = diff_east(padded_vel[0])
    east_dy = diff_north(padded_vel[0])
    north_dx = diff_east(padded_vel[1])
    north_dy = diff_north(padded_vel[1])
    divergence = east_dx + north_dy
    tension = east_dx - north_dy
    shear_rate = east_dy + north_dx
    delta_rate = jnp.sqrt(divergence * divergence + 0.25 * (tension * tension + shear_rate * shear_rate) + DELTA_FLOOR)
    target = jnp.stack([strength * (divergence / delta_rate - 1.0), strength * tension / (4.0 * delta_rate), strength * shear_rate / (8.0 * delta_rate)])
    return (stress + (target - stress) / ALPHA) * ice_frac

def drag_coeff(vel, currents):
    east_gap = currents[0] - vel[0]
    north_gap = currents[1] - vel[1]
    return WATER_DRAG * jnp.sqrt(east_gap * east_gap + north_gap * north_gap + 0.01)

def relax_velocity(padded_stress, vel, vel_start, forcing, ice_mass, coriolis, ice_frac):
    normal_xx = 0.5 * (padded_stress[0] + padded_stress[1])
    normal_yy = 0.5 * (padded_stress[0] - padded_stress[1])
    shear_xy = padded_stress[2]
    force_east = diff_east(normal_xx) + diff_north(shear_xy)
    force_north = diff_east(shear_xy) + diff_north(normal_yy)
    drag_rate = drag_coeff(vel, forcing[2:4])
    denominator = BETA + 1.0 + drag_rate / ice_mass
    new_east = (BETA * vel[0] + vel_start[0] + (force_east + forcing[0] + drag_rate * forcing[2]) / ice_mass + coriolis * vel[1]) / denominator * ice_frac
    new_north = (BETA * vel[1] + vel_start[1] + (force_north + forcing[1] + drag_rate * forcing[3]) / ice_mass - coriolis * vel[0]) / denominator * ice_frac
    return jnp.stack([new_east, new_north])

def reference(velocity, stress, ice_mass, strength, land_mask, ocean_forcing):
    ice_frac = land_mask.astype(jnp.float32)
    lat_rows = jnp.arange(NY).astype(jnp.float32)
    coriolis = (0.3 + 1.2 * (lat_rows + 0.5) / NY)[:, None]
    vel = velocity
    history = []
    for subcycle in range(ITERS):
        stress = relax_stress(extend_field(vel), stress, strength, ice_frac)
        new_vel = relax_velocity(extend_field(stress), vel, velocity, ocean_forcing, ice_mass, coriolis, ice_frac)
        change = new_vel - vel
        history.append(jnp.sum(change * change))
        vel = new_vel
    drag_rate = drag_coeff(vel, ocean_forcing[2:4])
    ocean_stress = drag_rate * (vel - ocean_forcing[2:4]) * ice_frac
    return (vel, stress, jnp.stack(history), ocean_stress)
```

```python
import functools

import jax
import jax.numpy as jnp
from jax import lax
from jax.experimental import pallas as pl
from jax.experimental.pallas import tpu as pltpu
from jax.sharding import PartitionSpec as P

ITERS = 4
DEEP = 8
PAD = 16
LANES = 128
CHUNK = 16
MESH = pl.DeviceIdType.MESH
SW, SE, NW, NE = range(4)


def kernel(
    G, Y, R, C, B,
    vel_in, sig_in, mass_in, strength_in, mask_in, forcing_in,
    vel_out, sig_out, res_out, os_out,
    vel, sig, raw_sig, raw_mass, raw_strength, raw_mask, pull, inv_mass, ice, base, force, edge_force, cor,
    bands, ocean, low, high, corner_out, corner_in, strip, f_out, f_in, sums, partial_y, partial_x,
    in_sem, f_send, f_recv, h_send, h_recv, y_send, y_recv, p_send, p_recv, o_sem, r_send, r_recv,
):
    gx = lax.axis_index("gx")
    gy = lax.axis_index("gy")
    f32 = jnp.float32
    T = PAD + R

    def at(dx, dy):
        return {"gx": lax.rem(gx + dx + G, G), "gy": lax.rem(gy + dy + Y, Y)}

    def remote(src, dst, send, recv, where):
        return pltpu.make_async_remote_copy(
            src_ref=src, dst_ref=dst, send_sem=send, recv_sem=recv, device_id=where, device_id_type=MESH
        )

    def settle(ref, sem):
        pltpu.make_async_copy(ref, ref, sem).wait()

    barrier = pltpu.get_barrier_semaphore()
    partners = [(d, 0) for d in range(1, G)] + [(0, d) for d in range(1, Y)]
    partners += [(dx, dy) for dx in (-1, 1) for dy in (-1, 1)]
    for dx, dy in partners:
        pl.semaphore_signal(barrier, inc=1, device_id=at(dx, dy), device_id_type=MESH)
    inner = pl.ds(PAD, R)
    loads = [
        pltpu.make_async_copy(forcing_in, bands, in_sem.at[0]),
        pltpu.make_async_copy(vel_in, vel.at[:, 0, inner], in_sem.at[1]),
        pltpu.make_async_copy(sig_in, raw_sig.at[:, inner], in_sem.at[2]),
        pltpu.make_async_copy(mass_in, raw_mass.at[inner], in_sem.at[3]),
        pltpu.make_async_copy(strength_in, raw_strength.at[inner], in_sem.at[4]),
        pltpu.make_async_copy(mask_in, raw_mask.at[inner], in_sem.at[5]),
    ]
    for copy in loads:
        copy.start()

    under, over = pl.ds(PAD - DEEP, DEEP), pl.ds(T, DEEP)
    lane8 = lax.broadcasted_iota(jnp.int32, (DEEP, LANES), 1)

    def outside(rows, slot, corners):
        for c in range(2):
            vel[c, 0, rows] = jnp.zeros((DEEP, C), f32)
        for c in range(3):
            raw_sig[c, rows] = jnp.zeros((DEEP, C), f32)
        raw_mass[rows] = jnp.ones((DEEP, C), f32)
        raw_strength[rows] = jnp.zeros((DEEP, C), f32)
        raw_mask[rows] = jnp.zeros((DEEP, C), jnp.int32)
        for c in range(4):
            force[c, rows] = jnp.zeros((DEEP, C), f32)
        f_in[slot] = jnp.zeros((2 * DEEP, LANES), f32)
        for c in corners:
            corner_in[c] = jnp.where(lane8 // (2 * DEEP) == 5, 1.0, 0.0)

    has_south, has_north = gy > 0, gy < Y - 1
    pl.when(jnp.logical_not(has_south))(lambda: outside(under, 0, (SW, SE)))
    pl.when(jnp.logical_not(has_north))(lambda: outside(over, G + 1, (NW, NE)))

    for ref in (vel, sig):
        for c in range(ref.shape[0]):
            for w in range(2):
                for r in (0, T + DEEP):
                    ref[c, w, r : r + DEEP] = jnp.zeros((DEEP, C), f32)
    for n in range(PAD - DEEP, T + DEEP, DEEP):
        lat = (gy * R + (n - PAD) + lax.broadcasted_iota(jnp.int32, (DEEP, C), 0)).astype(f32)
        cor[n : n + DEEP] = 0.3 + 1.2 * (lat + 0.5) / (R * Y)

    loads[0].wait()
    for c in range(G):
        t = bands[:, :, c * C : (c + 1) * C].reshape(4 * B, C).T
        f_out[(c + 1) % G, 0:DEEP, 0 : 4 * B] = t[C - DEEP : C]
        f_out[(c + G - 1) % G, DEEP : 2 * DEEP, 0 : 4 * B] = t[0:DEEP]
    f_in[gx + 1] = f_out[gx]
    own_columns = pl.ds(pl.multiple_of(gx * C, C), C)
    mine = pl.ds(pl.multiple_of(gx * B, B), B)
    padded_mine = pl.ds(pl.multiple_of(PAD + gx * B, DEEP), B)
    force[:, padded_mine] = bands[:, :, own_columns]
    for copy in loads[1:]:
        copy.wait()
    fields = [vel.at[0, 0], vel.at[1, 0], raw_sig.at[0], raw_sig.at[1], raw_sig.at[2], raw_mass, raw_strength, raw_mask]
    west_tile = jnp.zeros((DEEP, LANES), f32)
    east_tile = jnp.zeros((DEEP, LANES), f32)
    for q, field in enumerate(fields):
        t = field[PAD:T, :].astype(f32).T
        lo, hi = t[0:DEEP], t[C - DEEP : C]
        low[q] = lo
        high[q] = hi
        spot = lane8 // (2 * DEEP) == q
        turn = 2 * DEEP * q + DEEP

        def corner(rows):
            both = jnp.where(lane8 < DEEP, rows[:, 0:LANES], rows[:, R - LANES : R])
            return pltpu.roll(both, turn, 1)

        west_tile = jnp.where(spot, corner(lo), west_tile)
        east_tile = jnp.where(spot, corner(hi), east_tile)
    corner_out[0] = west_tile
    corner_out[1] = east_tile

    pl.semaphore_wait(barrier, len(partners))
    low_half = gx < G // 2

    def others(j):
        down = G - 1 - j
        down = down - (down <= gx).astype(jnp.int32)
        return jnp.where(low_half, down, j + (j >= gx).astype(jnp.int32))

    def forcing_sends(js):
        for j in js:
            to = others(j)
            where = {"gx": to, "gy": gy}
            columns = pl.ds(pl.multiple_of(to * C, C), C)
            remote(bands.at[:, :, columns], force.at[:, padded_mine], f_send.at[0], f_recv.at[gx], where).start()
            remote(f_out.at[to], f_in.at[gx + 1], f_send.at[1], f_recv.at[gx], where).start()

    near, far = pl.ds(0, DEEP), pl.ds(DEEP, DEEP)
    centre = pl.ds(LANES, R)
    bottom, top = pl.ds(PAD, DEEP), pl.ds(T - DEEP, DEEP)
    stacks = (vel, raw_sig, raw_mass, raw_strength, raw_mask)

    def rows_of(ref, rows):
        if ref is vel:
            return ref.at[:, 0, rows]
        return ref.at[:, rows] if len(ref.shape) == 3 else ref.at[rows]

    forcing_sends(range(2))
    sides = [
        remote(low, strip.at[:, far, centre], h_send.at[0], h_recv.at[0], at(-1, 0)),
        remote(high, strip.at[:, near, centre], h_send.at[1], h_recv.at[1], at(1, 0)),
    ]
    south = [
        remote(corner_out.at[0], corner_in.at[NE], h_send.at[2], h_recv.at[2], at(-1, -1)),
        remote(corner_out.at[1], corner_in.at[NW], h_send.at[3], h_recv.at[3], at(1, -1)),
    ]
    north = [
        remote(corner_out.at[0], corner_in.at[SE], h_send.at[4], h_recv.at[4], at(-1, 1)),
        remote(corner_out.at[1], corner_in.at[SW], h_send.at[5], h_recv.at[5], at(1, 1)),
    ]
    for copy in sides:
        copy.start()

    @pl.when(has_south)
    def _():
        for copy in south:
            copy.start()
        for ref in stacks:
            remote(rows_of(ref, bottom), rows_of(ref, over), y_send.at[0], y_recv.at[0], at(0, -1)).start()

    @pl.when(has_north)
    def _():
        for copy in north:
            copy.start()
        for ref in stacks:
            remote(rows_of(ref, top), rows_of(ref, under), y_send.at[1], y_recv.at[1], at(0, 1)).start()

    forcing_sends(range(2, G - 1))

    chunks = [(n, CHUNK) for n in range(PAD, T, CHUNK)]
    skirts = [(PAD - DEEP, DEEP), (T, DEEP)]

    def prepare(w, p, n, s0, s1, s2, mass, strength, mask):
        ice[w, p : p + n] = mask
        pull[w, p : p + n] = 0.25 * strength * mask
        inv_mass[w, p : p + n] = 1.0 / mass
        sig[0, w, p : p + n] = (s0 + s1) * mask
        sig[1, w, p : p + n] = (s0 - s1) * mask
        sig[2, w, p : p + n] = 2.0 * s2 * mask

    def prepare_main(p, n):
        rows = pl.ds(p, n)
        prepare(
            0, p, n, raw_sig[0, rows], raw_sig[1, rows], raw_sig[2, rows],
            raw_mass[rows], raw_strength[rows], raw_mask[rows].astype(f32),
        )

    for p, n in chunks:
        prepare_main(p, n)
    pack8 = pl.ds(0, 8 * DEEP)

    @pl.when(has_north)
    def _():
        settle(cor.at[pack8], y_recv.at[0])
        for copy in south:
            copy.wait_recv()

    @pl.when(has_south)
    def _():
        settle(cor.at[pack8], y_recv.at[1])
        for copy in north:
            copy.wait_recv()

    for copy in sides:
        copy.wait_recv()
    for p, n in skirts:
        prepare_main(p, n)
    for q in range(8):
        turn = LANES - (2 * DEEP * q + DEEP)
        for side, (s, n) in ((near, (SW, NW)), (far, (SE, NE))):
            strip[q, side, 0:LANES] = pltpu.roll(corner_in[s], turn, 1)
            strip[q, side, LANES + R : 2 * LANES + R] = pltpu.roll(corner_in[n], turn, 1)
    for tile in range(R // LANES + 2):
        t = strip[:, :, tile * LANES : (tile + 1) * LANES].reshape(8 * 2 * DEEP, LANES).T
        if tile == 0:
            t, p = t[LANES - DEEP :], PAD - DEEP
        elif tile == R // LANES + 1:
            t, p = t[:DEEP], T
        else:
            p = PAD + (tile - 1) * LANES
        for r in range(0, t.shape[0], CHUNK):
            part = t[r : r + CHUNK]
            n = part.shape[0]
            turned = [pltpu.roll(part, LANES - (2 * DEEP * q + DEEP), 1) for q in range(8)]
            vel[0, 1, p + r : p + r + n] = turned[0]
            vel[1, 1, p + r : p + r + n] = turned[1]
            prepare(1, p + r, n, *turned[2:])

    def shifted(a, b, lane):
        ra, rb = pltpu.roll(a, C - 1, 1), pltpu.roll(b, C - 1, 1)
        la, lb = pltpu.roll(a, 1, 1), pltpu.roll(b, 1, 1)
        right, left = lane == C - 1, lane == 0
        return (
            jnp.where(right, rb, ra) - jnp.where(left, lb, la),
            jnp.where(right, ra, rb) - jnp.where(left, la, lb),
        )

    everywhere = skirts[:1] + chunks + skirts[1:]

    def stress_step(last):
        for p, n in everywhere:
            lane = lax.broadcasted_iota(jnp.int32, (n, C), 1)
            rows = pl.ds(p, n)
            dxu = shifted(vel[0, 0, rows], vel[0, 1, rows], lane)
            dxv = shifted(vel[1, 0, rows], vel[1, 1, rows], lane)
            for w in range(2):
                dyu = vel[0, w, p + 1 : p + n + 1] - vel[0, w, p - 1 : p + n - 1]
                dyv = vel[1, w, p + 1 : p + n + 1] - vel[1, w, p - 1 : p + n - 1]
                div = dxu[w] + dyv
                ten = dxu[w] - dyv
                shear = dyu + dxv[w]
                inv = lax.rsqrt(div * div + 0.25 * (ten * ten + shear * shear) + 0.01)
                hold = pull[w, rows]
                scaled = hold * inv
                quarter = 0.25 * scaled
                spread = scaled * div - hold
                twist = quarter * ten
                xx = 0.75 * sig[0, w, rows] + (spread + twist)
                yy = 0.75 * sig[1, w, rows] + (spread - twist)
                xy = 0.75 * sig[2, w, rows] + quarter * shear
                sig[0, w, rows] = xx
                sig[1, w, rows] = yy
                sig[2, w, rows] = xy
                if last and w == 0 and PAD <= p < T:
                    sig_out[0, p - PAD : p - PAD + n] = 0.5 * (xx + yy)
                    sig_out[1, p - PAD : p - PAD + n] = 0.5 * (xx - yy)
                    sig_out[2, p - PAD : p - PAD + n] = 0.5 * xy

    def drag_of(u, v, cu, cv):
        a = cu - u
        b = cv - v
        y = a * a + b * b + 0.01
        return y * lax.rsqrt(y)

    def velocity_step(k):
        last = k == ITERS - 1
        total = jnp.zeros((DEEP, C), f32)
        for p, n in chunks if last else everywhere:
            lane = lax.broadcasted_iota(jnp.int32, (n, C), 1)
            rows = pl.ds(p, n)
            dxx = shifted(sig[0, 0, rows], sig[0, 1, rows], lane)
            dxy = shifted(sig[2, 0, rows], sig[2, 1, rows], lane)
            spin = cor[rows]
            for w in range(1 if last else 2):
                src = edge_force if w else force
                hi, lo = pl.ds(p + 1, n), pl.ds(p - 1, n)
                east = dxx[w] + (sig[2, w, hi] - sig[2, w, lo])
                north = dxy[w] + (sig[1, w, hi] - sig[1, w, lo])
                u, v = vel[0, w, rows], vel[1, w, rows]
                cu, cv = src[2, rows], src[3, rows]
                im = inv_mass[w, rows]
                if k == 0:
                    bu = u + src[0, rows] * im
                    bv = v + src[1, rows] * im
                    base[0, w, rows] = bu
                    base[1, w, rows] = bv
                else:
                    bu, bv = base[0, w, rows], base[1, w, rows]
                grip = drag_of(u, v, cu, cv) * im
                scale = ice[w, rows] / (5.0 + grip)
                push = 0.25 * im
                new_u = (4.0 * u + bu + east * push + grip * cu + spin * v) * scale
                new_v = (4.0 * v + bv + north * push + grip * cv - spin * u) * scale
                if last:
                    vel_out[0, p - PAD : p - PAD + n] = new_u
                    vel_out[1, p - PAD : p - PAD + n] = new_v
                    drag = drag_of(new_u, new_v, cu, cv) * ice[w, rows]
                    ocean[0, p - PAD : p - PAD + n] = drag * (new_u - cu)
                    ocean[1, p - PAD : p - PAD + n] = drag * (new_v - cv)
                else:
                    vel[0, w, rows] = new_u
                    vel[1, w, rows] = new_v
                if w == 0 and PAD <= p < T:
                    du = new_u - u
                    dv = new_v - v
                    square = du * du + dv * dv
                    for g in range(0, n, DEEP):
                        total = total + square[g : g + DEEP]
        sums[k : k + 1] = jnp.sum(total, axis=0, keepdims=True)

    stress_step(False)

    share = pl.ds(0, 4 * B + 2 * DEEP)

    def forward(to_north):
        band = jnp.where(to_north, G - 1, 0)

        @pl.when(band != gx)
        def _():
            settle(cor.at[share], f_recv.at[band])

        src = pl.ds(pl.multiple_of(jnp.where(to_north, T - DEEP, PAD), DEEP), DEEP)
        dst = pl.ds(pl.multiple_of(jnp.where(to_north, PAD - DEEP, T), DEEP), DEEP)
        step = jnp.where(to_north, 1, Y - 1)
        way = to_north.astype(jnp.int32)

        @pl.when(jnp.where(to_north, gy < Y - 1, gy > 0))
        def _():
            remote(force.at[:, src], force.at[:, dst], p_send.at[way], p_recv.at[way], at(0, step)).start()
            remote(
                f_in.at[band + 1], f_in.at[jnp.where(to_north, 0, G + 1)], p_send.at[way], p_recv.at[way], at(0, step)
            ).start()

    forward(low_half)
    forward(jnp.logical_not(low_half))
    for b in range(1, G - 1):

        @pl.when(gx != b)
        def _():
            settle(cor.at[share], f_recv.at[b])

    skirt = pl.ds(0, 4 * DEEP + 2 * DEEP)

    @pl.when(has_south)
    def _():
        settle(cor.at[pack8], y_send.at[0])
        settle(cor.at[skirt], p_recv.at[1])

    @pl.when(has_north)
    def _():
        settle(cor.at[pack8], y_send.at[1])
        settle(cor.at[skirt], p_recv.at[0])

    for s in range(0, G + 2, 8):
        t = f_in[s : s + 8].reshape(8 * 2 * DEEP, LANES).T
        for b in range(s, min(s + 8, G + 2)):
            turn = LANES - (2 * DEEP * (b - s) + DEEP)
            for c in range(4):
                part = t[c * B : (c + 1) * B]
                if b == 0:
                    edge_force[c, under] = pltpu.roll(part[B - DEEP :], turn, 1)
                elif b == G + 1:
                    edge_force[c, over] = pltpu.roll(part[:DEEP], turn, 1)
                else:
                    edge_force[c, PAD + (b - 1) * B : PAD + b * B] = pltpu.roll(part, turn, 1)

    sums[...] = jnp.zeros_like(sums)
    velocity_step(0)
    for k in range(1, ITERS):
        stress_step(k == ITERS - 1)
        velocity_step(k)

    for j in range(G - 1):
        to = others(j)
        remote(
            ocean.at[:, pl.ds(pl.multiple_of(to * B, B), B)], os_out.at[:, :, own_columns],
            o_sem.at[0], o_sem.at[1], {"gx": to, "gy": gy},
        ).start()
    for d in range(1, Y):
        remote(sums, partial_y.at[gy], r_send.at[0], r_recv.at[0], at(0, d)).start()
    partial_y[gy] = sums[...]
    os_out[:, :, own_columns] = ocean[:, mine]
    settle(partial_y.at[pl.ds(0, Y - 1)], r_recv.at[0])
    partial_x[gx] = jnp.sum(partial_y[...], axis=0)
    for d in range(1, G):
        remote(partial_x.at[gx], partial_x.at[gx], r_send.at[1], r_recv.at[1], at(d, 0)).start()
    most = pl.ds(0, (G - 1) * C)
    settle(os_out.at[:, :, most], o_sem.at[1])
    settle(partial_x.at[pl.ds(0, G - 1)], r_recv.at[1])
    total = jnp.sum(partial_x[...], axis=0)
    lane1 = lax.broadcasted_iota(jnp.int32, (1, LANES), 1)
    answer = jnp.zeros((1, LANES), f32)
    for k in range(ITERS):
        answer = jnp.where(lane1 == k, jnp.sum(total[k : k + 1]), answer)
    res_out[...] = answer[0, :ITERS]
    settle(bands.at[:, :, most], f_send.at[0])
    settle(f_out.at[pl.ds(0, G - 1)], f_send.at[1])
    settle(os_out.at[:, :, most], o_sem.at[0])
    for copy in sides:
        copy.wait_send()

    @pl.when(has_south)
    def _():
        for copy in south:
            copy.wait_send()
        settle(cor.at[skirt], p_send.at[0])

    @pl.when(has_north)
    def _():
        for copy in north:
            copy.wait_send()
        settle(cor.at[skirt], p_send.at[1])

    settle(partial_y.at[pl.ds(0, Y - 1)], r_send.at[0])
    settle(partial_x.at[pl.ds(0, G - 1)], r_send.at[1])


def store(vel, sig, res, ocean, vel_out, sig_out, res_out, ocean_out, sem):
    pairs = ((sig, sig_out), (vel, vel_out), (ocean, ocean_out), (res, res_out))
    copies = [pltpu.make_async_copy(src, dst, sem.at[n]) for n, (src, dst) in enumerate(pairs)]
    for copy in copies:
        copy.start()
    for copy in copies:
        copy.wait()


def local(velocity, stress, ice_mass, strength, land_mask, ocean_forcing):
    G, Y = lax.axis_size("gx"), lax.axis_size("gy")
    R, C = velocity.shape[1:]
    B = ocean_forcing.shape[1]
    f32 = jnp.float32
    rows = R + 2 * PAD
    slots = (G + 2 + 7) // 8 * 8
    dma = pltpu.SemaphoreType.DMA
    any_space = pl.BlockSpec(memory_space=pl.ANY)
    vmem_space = pl.BlockSpec(memory_space=pltpu.VMEM)
    done = pl.pallas_call(
        functools.partial(kernel, G, Y, R, C, B),
        out_shape=(
            pltpu.VMEM(velocity.shape, f32),
            pltpu.VMEM(stress.shape, f32),
            pltpu.VMEM((ITERS,), f32),
            pltpu.VMEM((2,) + ocean_forcing.shape[1:], f32),
        ),
        in_specs=[any_space] * 6,
        out_specs=(vmem_space,) * 4,
        scratch_shapes=[
            pltpu.VMEM((2, 2, rows, C), f32),
            pltpu.VMEM((3, 2, rows, C), f32),
            pltpu.VMEM((3, rows, C), f32),
            pltpu.VMEM((rows, C), f32),
            pltpu.VMEM((rows, C), f32),
            pltpu.VMEM((rows, C), jnp.int32),
            pltpu.VMEM((2, rows, C), f32),
            pltpu.VMEM((2, rows, C), f32),
            pltpu.VMEM((2, rows, C), f32),
            pltpu.VMEM((2, 2, rows, C), f32),
            pltpu.VMEM((4, rows, C), f32),
            pltpu.VMEM((4, rows, C), f32),
            pltpu.VMEM((rows, C), f32),
            pltpu.VMEM(ocean_forcing.shape, f32),
            pltpu.VMEM((2, R, C), f32),
            pltpu.VMEM((8, DEEP, R), f32),
            pltpu.VMEM((8, DEEP, R), f32),
            pltpu.VMEM((2, DEEP, LANES), f32),
            pltpu.VMEM((4, DEEP, LANES), f32),
            pltpu.VMEM((8, 2 * DEEP, R + 2 * LANES), f32),
            pltpu.VMEM((G, 2 * DEEP, LANES), f32),
            pltpu.VMEM((slots, 2 * DEEP, LANES), f32),
            pltpu.VMEM((DEEP, LANES), f32),
            pltpu.VMEM((Y, DEEP, LANES), f32),
            pltpu.VMEM((G, DEEP, LANES), f32),
            dma((6,)),
            dma((2,)),
            dma((G,)),
            dma((6,)),
            dma((6,)),
            dma((2,)),
            dma((2,)),
            dma((2,)),
            dma((2,)),
            dma((2,)),
            dma((2,)),
            dma((2,)),
        ],
        compiler_params=pltpu.CompilerParams(collective_id=0, has_side_effects=True),
    )(velocity, stress, ice_mass, strength, land_mask, ocean_forcing)
    return pl.pallas_call(
        store,
        out_shape=tuple(jax.ShapeDtypeStruct(x.shape, f32) for x in done),
        in_specs=[vmem_space] * 4,
        out_specs=(any_space,) * 4,
        scratch_shapes=[dma((4,))],
    )(*[pltpu.with_memory_space_constraint(x, pltpu.VMEM) for x in done])


def solution(mesh):
    placed = (
        P(None, "gy", "gx"),
        P(None, "gy", "gx"),
        P("gy", "gx"),
        P("gy", "gx"),
        P("gy", "gx"),
        P(None, ("gy", "gx"), None),
    )
    return jax.shard_map(
        local,
        mesh=mesh,
        in_specs=placed,
        out_specs=(P(None, "gy", "gx"), P(None, "gy", "gx"), P(), P(None, ("gy", "gx"), None)),
        check_vma=False,
    )
```

```python
import functools

import jax
import jax.numpy as jnp
from jax import lax
from jax.experimental import pallas as pl
from jax.experimental.pallas import tpu as pltpu
from jax.sharding import PartitionSpec as P

ITERS = 4
DEEP = 8
PAD = 16
LANES = 128
CHUNK = 16
REACH = 6
MESH = pl.DeviceIdType.MESH
SW, SE, NW, NE = range(4)


def kernel(
    G, Y, R, C, B,
    vel_in, sig_in, mass_in, strength_in, mask_in, forcing_in,
    vel_out, sig_out, res_out, os_out,
    vel, sig, raw_sig, raw_mass, raw_strength, raw_mask, pull, inv_mass, ice, base, force, edge_force, cor,
    bands, ocean, low, high, corner_out, corner_in, strip, f_out, f_in, sums, partial,
    in_sem, f_send, f_recv, h_send, h_recv, y_send, y_recv, p_send, p_recv, o_sem, r_send, r_recv,
):
    gx = lax.axis_index("gx")
    gy = lax.axis_index("gy")
    f32 = jnp.float32
    T = PAD + R

    def at(dx, dy):
        return {"gx": lax.rem(gx + dx + G, G), "gy": lax.rem(gy + dy + Y, Y)}

    def remote(src, dst, send, recv, where):
        return pltpu.make_async_remote_copy(
            src_ref=src, dst_ref=dst, send_sem=send, recv_sem=recv, device_id=where, device_id_type=MESH
        )

    def settle(ref, sem):
        pltpu.make_async_copy(ref, ref, sem).wait()

    barrier = pltpu.get_barrier_semaphore()
    partners = [(dx, dy) for dx in range(G) for dy in range(Y) if dx or dy]
    for dx, dy in partners:
        pl.semaphore_signal(barrier, inc=1, device_id=at(dx, dy), device_id_type=MESH)
    inner = pl.ds(PAD, R)
    loads = [
        pltpu.make_async_copy(forcing_in, bands, in_sem.at[0]),
        pltpu.make_async_copy(vel_in, vel.at[:, 0, inner], in_sem.at[1]),
        pltpu.make_async_copy(sig_in, raw_sig.at[:, inner], in_sem.at[2]),
        pltpu.make_async_copy(mass_in, raw_mass.at[inner], in_sem.at[3]),
        pltpu.make_async_copy(strength_in, raw_strength.at[inner], in_sem.at[4]),
        pltpu.make_async_copy(mask_in, raw_mask.at[inner], in_sem.at[5]),
    ]
    for copy in loads:
        copy.start()

    under, over = pl.ds(PAD - DEEP, DEEP), pl.ds(T, DEEP)
    lane8 = lax.broadcasted_iota(jnp.int32, (DEEP, LANES), 1)

    def outside(rows, slot, corners):
        for c in range(2):
            vel[c, 0, rows] = jnp.zeros((DEEP, C), f32)
        for c in range(3):
            raw_sig[c, rows] = jnp.zeros((DEEP, C), f32)
        raw_mass[rows] = jnp.ones((DEEP, C), f32)
        raw_strength[rows] = jnp.zeros((DEEP, C), f32)
        raw_mask[rows] = jnp.zeros((DEEP, C), jnp.int32)
        for c in range(4):
            force[c, rows] = jnp.zeros((DEEP, C), f32)
        f_in[slot] = jnp.zeros((2 * REACH, LANES), f32)
        for c in corners:
            corner_in[c] = jnp.where(lane8 // (2 * DEEP) == 5, 1.0, 0.0)

    has_south, has_north = gy > 0, gy < Y - 1
    pl.when(jnp.logical_not(has_south))(lambda: outside(under, 0, (SW, SE)))
    pl.when(jnp.logical_not(has_north))(lambda: outside(over, G + 1, (NW, NE)))

    for ref in (vel, sig):
        for c in range(ref.shape[0]):
            for w in range(2):
                for r in (0, T + DEEP):
                    ref[c, w, r : r + DEEP] = jnp.zeros((DEEP, C), f32)
    for n in range(PAD - DEEP, T + DEEP, DEEP):
        lat = (gy * R + (n - PAD) + lax.broadcasted_iota(jnp.int32, (DEEP, C), 0)).astype(f32)
        cor[n : n + DEEP] = 0.3 + 1.2 * (lat + 0.5) / (R * Y)

    loads[0].wait()
    low_half = gx < G // 2
    own_columns = pl.ds(pl.multiple_of(gx * C, C), C)
    mine = pl.ds(pl.multiple_of(gx * B, B), B)
    padded_mine = pl.ds(pl.multiple_of(PAD + gx * B, DEEP), B)
    pl.semaphore_wait(barrier, len(partners))
    def others(j):
        down = G - 1 - j
        down = down - (down <= gx).astype(jnp.int32)
        return jnp.where(low_half, down, j + (j >= gx).astype(jnp.int32))

    def send_block(j):
        to = others(j)
        columns = pl.ds(pl.multiple_of(to * C, C), C)
        where = {"gx": to, "gy": gy}
        remote(bands.at[:, :, columns], force.at[:, padded_mine], f_send.at[0], f_recv.at[gx], where).start()

    def send_strip(j):
        to = others(j)
        where = {"gx": to, "gy": gy}
        remote(f_out.at[to], f_in.at[gx + 1], f_send.at[1], f_recv.at[gx], where).start()

    for j in range(2):
        send_block(j)
    for copy in loads[1:]:
        copy.wait()
    fields = [vel.at[0, 0], vel.at[1, 0], raw_sig.at[0], raw_sig.at[1], raw_sig.at[2], raw_mass, raw_strength, raw_mask]
    west_tile = jnp.zeros((DEEP, LANES), f32)
    east_tile = jnp.zeros((DEEP, LANES), f32)
    for q, field in enumerate(fields):
        t = field[PAD:T, :].astype(f32).T
        lo, hi = t[0:DEEP], t[C - DEEP : C]
        low[q] = lo
        high[q] = hi
        spot = lane8 // (2 * DEEP) == q
        turn = 2 * DEEP * q + DEEP

        def corner(rows):
            both = jnp.where(lane8 < DEEP, rows[:, 0:LANES], rows[:, R - LANES : R])
            return pltpu.roll(both, turn, 1)

        west_tile = jnp.where(spot, corner(lo), west_tile)
        east_tile = jnp.where(spot, corner(hi), east_tile)
    corner_out[0] = west_tile
    corner_out[1] = east_tile

    near, far = pl.ds(0, DEEP), pl.ds(DEEP, DEEP)
    centre = pl.ds(LANES, R)
    bottom, top = pl.ds(PAD, DEEP), pl.ds(T - DEEP, DEEP)
    stacks = (vel, raw_sig, raw_mass, raw_strength, raw_mask)

    def rows_of(ref, rows):
        if ref is vel:
            return ref.at[:, 0, rows]
        return ref.at[:, rows] if len(ref.shape) == 3 else ref.at[rows]

    sides = [
        remote(low, strip.at[:, far, centre], h_send.at[0], h_recv.at[0], at(-1, 0)),
        remote(high, strip.at[:, near, centre], h_send.at[1], h_recv.at[1], at(1, 0)),
    ]
    south = [
        remote(corner_out.at[0], corner_in.at[NE], h_send.at[2], h_recv.at[2], at(-1, -1)),
        remote(corner_out.at[1], corner_in.at[NW], h_send.at[3], h_recv.at[3], at(1, -1)),
    ]
    north = [
        remote(corner_out.at[0], corner_in.at[SE], h_send.at[4], h_recv.at[4], at(-1, 1)),
        remote(corner_out.at[1], corner_in.at[SW], h_send.at[5], h_recv.at[5], at(1, 1)),
    ]
    for copy in sides:
        copy.start()

    @pl.when(has_south)
    def _():
        for copy in south:
            copy.start()
        for ref in stacks:
            remote(rows_of(ref, bottom), rows_of(ref, over), y_send.at[0], y_recv.at[0], at(0, -1)).start()

    @pl.when(has_north)
    def _():
        for copy in north:
            copy.start()
        for ref in stacks:
            remote(rows_of(ref, top), rows_of(ref, under), y_send.at[1], y_recv.at[1], at(0, 1)).start()

    for c in range(G):
        t = bands[:, :, c * C : (c + 1) * C].reshape(4 * B, C).T
        f_out[(c + 1) % G, 0:REACH, 0 : 4 * B] = t[C - REACH : C]
        f_out[(c + G - 1) % G, REACH : 2 * REACH, 0 : 4 * B] = t[0:REACH]
    for j in range(2):
        send_strip(j)
    for j in range(2, G - 1):
        send_block(j)
        send_strip(j)
    f_in[gx + 1] = f_out[gx]
    force[:, padded_mine] = bands[:, :, own_columns]

    chunks = [(n, CHUNK) for n in range(PAD, T, CHUNK)]
    skirts = [(PAD - DEEP, DEEP), (T, DEEP)]

    def prepare(w, p, n, s0, s1, s2, mass, strength, mask):
        ice[w, p : p + n] = mask
        pull[w, p : p + n] = 0.25 * strength * mask
        inv_mass[w, p : p + n] = 1.0 / mass
        sig[0, w, p : p + n] = (s0 + s1) * mask
        sig[1, w, p : p + n] = (s0 - s1) * mask
        sig[2, w, p : p + n] = 2.0 * s2 * mask

    def prepare_main(p, n):
        rows = pl.ds(p, n)
        prepare(
            0, p, n, raw_sig[0, rows], raw_sig[1, rows], raw_sig[2, rows],
            raw_mass[rows], raw_strength[rows], raw_mask[rows].astype(f32),
        )

    for p, n in chunks:
        prepare_main(p, n)
    pack8 = pl.ds(0, 8 * DEEP)

    @pl.when(has_north)
    def _():
        settle(cor.at[pack8], y_recv.at[0])
        for copy in south:
            copy.wait_recv()

    @pl.when(has_south)
    def _():
        settle(cor.at[pack8], y_recv.at[1])
        for copy in north:
            copy.wait_recv()

    for copy in sides:
        copy.wait_recv()
    for p, n in skirts:
        prepare_main(p, n)
    for q in range(8):
        turn = LANES - (2 * DEEP * q + DEEP)
        for side, (s, n) in ((near, (SW, NW)), (far, (SE, NE))):
            strip[q, side, 0:LANES] = pltpu.roll(corner_in[s], turn, 1)
            strip[q, side, LANES + R : 2 * LANES + R] = pltpu.roll(corner_in[n], turn, 1)
    for tile in range(R // LANES + 2):
        t = strip[:, :, tile * LANES : (tile + 1) * LANES].reshape(8 * 2 * DEEP, LANES).T
        if tile == 0:
            t, p = t[LANES - DEEP :], PAD - DEEP
        elif tile == R // LANES + 1:
            t, p = t[:DEEP], T
        else:
            p = PAD + (tile - 1) * LANES
        for r in range(0, t.shape[0], CHUNK):
            part = t[r : r + CHUNK]
            n = part.shape[0]
            turned = [pltpu.roll(part, LANES - (2 * DEEP * q + DEEP), 1) for q in range(8)]
            vel[0, 1, p + r : p + r + n] = turned[0]
            vel[1, 1, p + r : p + r + n] = turned[1]
            prepare(1, p + r, n, *turned[2:])

    def shifted(a, b, lane):
        ra, rb = pltpu.roll(a, C - 1, 1), pltpu.roll(b, C - 1, 1)
        la, lb = pltpu.roll(a, 1, 1), pltpu.roll(b, 1, 1)
        right, left = lane == C - 1, lane == 0
        return (
            jnp.where(right, rb, ra) - jnp.where(left, lb, la),
            jnp.where(right, ra, rb) - jnp.where(left, la, lb),
        )

    everywhere = skirts[:1] + chunks + skirts[1:]
    row8 = lax.broadcasted_iota(jnp.int32, (DEEP, C), 0)

    def stress_step(last, spans, merge=False):
        for p, n, keep in spans:
            lane = lax.broadcasted_iota(jnp.int32, (n, C), 1)
            rows = pl.ds(p, n)
            dxu = shifted(vel[0, 0, rows], vel[0, 1, rows], lane)
            dxv = shifted(vel[1, 0, rows], vel[1, 1, rows], lane)
            for w in range(2):
                dyu = vel[0, w, p + 1 : p + n + 1] - vel[0, w, p - 1 : p + n - 1]
                dyv = vel[1, w, p + 1 : p + n + 1] - vel[1, w, p - 1 : p + n - 1]
                div = dxu[w] + dyv
                ten = dxu[w] - dyv
                shear = dyu + dxv[w]
                inv = lax.rsqrt(div * div + 0.25 * (ten * ten + shear * shear) + 0.01)
                hold = pull[w, rows]
                scaled = hold * inv
                quarter = 0.25 * scaled
                spread = scaled * div - hold
                twist = quarter * ten
                old = [sig[c, w, rows] for c in range(3)]
                new = [
                    0.75 * old[0] + (spread + twist),
                    0.75 * old[1] + (spread - twist),
                    0.75 * old[2] + quarter * shear,
                ]
                if keep is not None:
                    new = [jnp.where(keep, a, b) for a, b in zip(new, old)]
                for c in range(3):
                    sig[c, w, rows] = new[c]
                if last and w == 0 and PAD <= p < T and (keep is None or merge):
                    sig_out[0, p - PAD : p - PAD + n] = 0.5 * (new[0] + new[1])
                    sig_out[1, p - PAD : p - PAD + n] = 0.5 * (new[0] - new[1])
                    sig_out[2, p - PAD : p - PAD + n] = 0.5 * new[2]

    def drag_of(u, v, cu, cv):
        a = cu - u
        b = cv - v
        y = a * a + b * b + 0.01
        return y * lax.rsqrt(y)

    def velocity_step(k, spans, total, merge=False):
        last = k == ITERS - 1
        for p, n, keep in spans:
            inside = PAD <= p < T
            if last and not inside:
                continue
            lane = lax.broadcasted_iota(jnp.int32, (n, C), 1)
            rows = pl.ds(p, n)
            dxx = shifted(sig[0, 0, rows], sig[0, 1, rows], lane)
            dxy = shifted(sig[2, 0, rows], sig[2, 1, rows], lane)
            spin = cor[rows]
            for w in range(1 if last else 2):
                src = edge_force if w else force
                hi, lo = pl.ds(p + 1, n), pl.ds(p - 1, n)
                east = dxx[w] + (sig[2, w, hi] - sig[2, w, lo])
                north = dxy[w] + (sig[1, w, hi] - sig[1, w, lo])
                u, v = vel[0, w, rows], vel[1, w, rows]
                cu, cv = src[2, rows], src[3, rows]
                im = inv_mass[w, rows]
                if k == 0:
                    bu = u + src[0, rows] * im
                    bv = v + src[1, rows] * im
                    base[0, w, rows] = bu
                    base[1, w, rows] = bv
                else:
                    bu, bv = base[0, w, rows], base[1, w, rows]
                grip = drag_of(u, v, cu, cv) * im
                scale = ice[w, rows] / (5.0 + grip)
                push = 0.25 * im
                new_u = (4.0 * u + bu + east * push + grip * cu + spin * v) * scale
                new_v = (4.0 * v + bv + north * push + grip * cv - spin * u) * scale
                if keep is not None:
                    new_u = jnp.where(keep, new_u, u)
                    new_v = jnp.where(keep, new_v, v)
                if last and (keep is None or merge):
                    vel_out[0, p - PAD : p - PAD + n] = new_u
                    vel_out[1, p - PAD : p - PAD + n] = new_v
                    drag = drag_of(new_u, new_v, cu, cv) * ice[w, rows]
                    ocean[0, p - PAD : p - PAD + n] = drag * (new_u - cu)
                    ocean[1, p - PAD : p - PAD + n] = drag * (new_v - cv)
                else:
                    vel[0, w, rows] = new_u
                    vel[1, w, rows] = new_v
                if w == 0 and inside:
                    du = new_u - u
                    dv = new_v - v
                    square = du * du + dv * dv
                    for g in range(0, n, DEEP):
                        total = total + square[g : g + DEEP]
        return total

    def spans_of(lo, hi):
        return [(p, min(CHUNK, hi - p), None) for p in range(lo, hi, CHUNK)]

    stress_step(False, [(p, n, None) for p, n in everywhere])

    share = pl.ds(0, 4 * B + 2 * REACH)

    def forward(to_north):
        band = jnp.where(to_north, G - 1, 0)

        @pl.when(band != gx)
        def _():
            settle(cor.at[share], f_recv.at[band])

        src = pl.ds(pl.multiple_of(jnp.where(to_north, T - DEEP, PAD), DEEP), DEEP)
        dst = pl.ds(pl.multiple_of(jnp.where(to_north, PAD - DEEP, T), DEEP), DEEP)
        step = jnp.where(to_north, 1, Y - 1)
        way = to_north.astype(jnp.int32)

        @pl.when(jnp.where(to_north, gy < Y - 1, gy > 0))
        def _():
            remote(force.at[:, src], force.at[:, dst], p_send.at[way], p_recv.at[way], at(0, step)).start()
            remote(
                f_in.at[band + 1], f_in.at[jnp.where(to_north, 0, G + 1)], p_send.at[way], p_recv.at[way], at(0, step)
            ).start()

    forward(low_half)
    forward(jnp.logical_not(low_half))
    skirt = pl.ds(0, 4 * DEEP + 2 * REACH)

    def arrive(bs):
        for b in bs:

            @pl.when(gx != b)
            def _():
                settle(cor.at[share], f_recv.at[b])

    def edges(bs):
        for s in range(0, len(bs), 8):
            group = bs[s : s + 8]
            parts = [f_in[b + 1] for b in group]
            fill = LANES - 2 * REACH * len(group)
            t = jnp.concatenate(parts + [jnp.zeros((fill, LANES), f32)], axis=0).T
            for n, b in enumerate(group):
                turn = LANES - (2 * REACH * n + REACH)
                for c in range(4):
                    part = t[c * B : (c + 1) * B]
                    if b == -1:
                        edge_force[c, under] = pltpu.roll(part[B - DEEP :], turn, 1)
                    elif b == G:
                        edge_force[c, over] = pltpu.roll(part[:DEEP], turn, 1)
                    else:
                        edge_force[c, PAD + b * B : PAD + (b + 1) * B] = pltpu.roll(part, turn, 1)

    def send_rows(b, r, n):
        @pl.when(gx != b)
        def _():
            remote(
                ocean.at[:, pl.ds(b * B + r, n)], os_out.at[:, pl.ds(r, n), own_columns],
                o_sem.at[0], o_sem.at[1], {"gx": b, "gy": gy},
            ).start()

    def phases(is_low):
        late = list(range(G // 2, G // 2 + G // 4)) if is_low else list(range(G // 2 - G // 4, G // 2))
        early = [b for b in range(G) if b not in late]
        w0, w1 = PAD + late[0] * B, PAD + (late[-1] + 1) * B
        arrive([b for b in early if 0 < b < G - 1])

        @pl.when(has_south)
        def _():
            settle(cor.at[pack8], y_send.at[0])
            settle(cor.at[skirt], p_recv.at[1])

        @pl.when(has_north)
        def _():
            settle(cor.at[pack8], y_send.at[1])
            settle(cor.at[skirt], p_recv.at[0])

        edges([-1] + early + [G])
        outer = (
            [(PAD - DEEP, DEEP, None)] + spans_of(PAD, w0 - DEEP) + spans_of(w1 + DEEP, T) + [(T, DEEP, None)]
        )
        rims = ((w0 - DEEP, DEEP), (w1, DEEP))

        def first(h):
            if h == 0:
                return outer + [(p, n, None) for p, n in rims]
            return outer + [(*rims[0], row8 < DEEP - h), (*rims[1], row8 >= h)]

        def second(h):
            inside = spans_of(w0, w1)
            if h == 0:
                return inside
            return inside + [(*rims[0], row8 >= DEEP - h), (*rims[1], row8 < h)]

        totals = [jnp.zeros((DEEP, C), f32)] * ITERS
        totals[0] = velocity_step(0, first(0), totals[0])
        for k in range(1, ITERS):
            stress_step(k == ITERS - 1, first(2 * k - 1))
            totals[k] = velocity_step(k, first(2 * k), totals[k])
        order = list(range(G - 1, -1, -1)) if is_low else list(range(G))
        rest = []
        for b in order:
            if b in late:
                rest.append((b, 0, B))
                continue
            r, n = 0, B
            if b == late[0] - 1:
                n -= DEEP
                rest.append((b, n, DEEP))
            elif b == late[-1] + 1:
                r, n = DEEP, n - DEEP
                rest.append((b, 0, DEEP))
            if n:
                send_rows(b, r, n)
        arrive(late)
        edges(late)
        totals[0] = velocity_step(0, second(0), totals[0])
        for k in range(1, ITERS):
            stress_step(k == ITERS - 1, second(2 * k - 1), True)
            totals[k] = velocity_step(k, second(2 * k), totals[k], True)
        answer = jnp.zeros((1, LANES), f32)
        for k in range(ITERS):
            answer = jnp.where(lane1 == k, jnp.sum(totals[k]), answer)
        sums[...] = answer
        me = gx * Y + gy
        for dx, dy in partners:
            remote(sums, partial.at[me], r_send.at[0], r_recv.at[0], at(dx, dy)).start()
        partial[me] = answer
        for b, r, n in rest:
            send_rows(b, r, n)

    lane1 = lax.broadcasted_iota(jnp.int32, (1, LANES), 1)
    pl.when(low_half)(lambda: phases(True))
    pl.when(jnp.logical_not(low_half))(lambda: phases(False))
    os_out[:, :, own_columns] = ocean[:, mine]
    most = pl.ds(0, (G - 1) * C)
    settle(os_out.at[:, :, most], o_sem.at[1])
    peers = pl.ds(0, len(partners))
    settle(partial.at[peers], r_recv.at[0])
    res_out[...] = jnp.sum(partial[...], axis=0)[0, :ITERS]
    settle(bands.at[:, :, most], f_send.at[0])
    settle(f_out.at[pl.ds(0, G - 1)], f_send.at[1])
    settle(os_out.at[:, :, most], o_sem.at[0])
    for copy in sides:
        copy.wait_send()

    @pl.when(has_south)
    def _():
        for copy in south:
            copy.wait_send()
        settle(cor.at[skirt], p_send.at[0])

    @pl.when(has_north)
    def _():
        for copy in north:
            copy.wait_send()
        settle(cor.at[skirt], p_send.at[1])

    settle(partial.at[peers], r_send.at[0])


def store(vel, sig, res, ocean, vel_out, sig_out, res_out, ocean_out, sem):
    pairs = ((sig, sig_out), (vel, vel_out), (ocean, ocean_out), (res, res_out))
    copies = [pltpu.make_async_copy(src, dst, sem.at[n]) for n, (src, dst) in enumerate(pairs)]
    for copy in copies:
        copy.start()
    for copy in copies:
        copy.wait()


def local(velocity, stress, ice_mass, strength, land_mask, ocean_forcing):
    G, Y = lax.axis_size("gx"), lax.axis_size("gy")
    R, C = velocity.shape[1:]
    B = ocean_forcing.shape[1]
    f32 = jnp.float32
    rows = R + 2 * PAD
    dma = pltpu.SemaphoreType.DMA
    any_space = pl.BlockSpec(memory_space=pl.ANY)
    vmem_space = pl.BlockSpec(memory_space=pltpu.VMEM)
    done = pl.pallas_call(
        functools.partial(kernel, G, Y, R, C, B),
        out_shape=(
            pltpu.VMEM(velocity.shape, f32),
            pltpu.VMEM(stress.shape, f32),
            pltpu.VMEM((ITERS,), f32),
            pltpu.VMEM((2,) + ocean_forcing.shape[1:], f32),
        ),
        in_specs=[any_space] * 6,
        out_specs=(vmem_space,) * 4,
        scratch_shapes=[
            pltpu.VMEM((2, 2, rows, C), f32),
            pltpu.VMEM((3, 2, rows, C), f32),
            pltpu.VMEM((3, rows, C), f32),
            pltpu.VMEM((rows, C), f32),
            pltpu.VMEM((rows, C), f32),
            pltpu.VMEM((rows, C), jnp.int32),
            pltpu.VMEM((2, rows, C), f32),
            pltpu.VMEM((2, rows, C), f32),
            pltpu.VMEM((2, rows, C), f32),
            pltpu.VMEM((2, 2, rows, C), f32),
            pltpu.VMEM((4, rows, C), f32),
            pltpu.VMEM((4, rows, C), f32),
            pltpu.VMEM((rows, C), f32),
            pltpu.VMEM(ocean_forcing.shape, f32),
            pltpu.VMEM((2, R, C), f32),
            pltpu.VMEM((8, DEEP, R), f32),
            pltpu.VMEM((8, DEEP, R), f32),
            pltpu.VMEM((2, DEEP, LANES), f32),
            pltpu.VMEM((4, DEEP, LANES), f32),
            pltpu.VMEM((8, 2 * DEEP, R + 2 * LANES), f32),
            pltpu.VMEM((G, 2 * REACH, LANES), f32),
            pltpu.VMEM((G + 2, 2 * REACH, LANES), f32),
            pltpu.VMEM((1, LANES), f32),
            pltpu.VMEM((G * Y, 1, LANES), f32),
            dma((6,)),
            dma((2,)),
            dma((G,)),
            dma((6,)),
            dma((6,)),
            dma((2,)),
            dma((2,)),
            dma((2,)),
            dma((2,)),
            dma((2,)),
            dma((1,)),
            dma((1,)),
        ],
        compiler_params=pltpu.CompilerParams(collective_id=0, has_side_effects=True),
    )(velocity, stress, ice_mass, strength, land_mask, ocean_forcing)
    return pl.pallas_call(
        store,
        out_shape=tuple(jax.ShapeDtypeStruct(x.shape, f32) for x in done),
        in_specs=[vmem_space] * 4,
        out_specs=(any_space,) * 4,
        scratch_shapes=[dma((4,))],
    )(*[pltpu.with_memory_space_constraint(x, pltpu.VMEM) for x in done])


def solution(mesh):
    placed = (
        P(None, "gy", "gx"),
        P(None, "gy", "gx"),
        P("gy", "gx"),
        P("gy", "gx"),
        P("gy", "gx"),
        P(None, ("gy", "gx"), None),
    )
    return jax.shard_map(
        local,
        mesh=mesh,
        in_specs=placed,
        out_specs=(P(None, "gy", "gx"), P(None, "gy", "gx"), P(), P(None, ("gy", "gx"), None)),
        check_vma=False,
    )
```

```python
import functools

import jax
import jax.numpy as jnp
from jax import lax
from jax.experimental import pallas as pl
from jax.experimental.pallas import tpu as pltpu
from jax.sharding import PartitionSpec as P

ITERS = 4
DEEP = 8
PAD = 16
LANES = 128
CHUNK = 16
REACH = 6
MESH = pl.DeviceIdType.MESH
SW, SE, NW, NE = range(4)


def kernel(
    G, Y, R, C, B,
    vel_in, sig_in, mass_in, strength_in, mask_in, forcing_in,
    vel_out, sig_out, res_out, os_out,
    vel, sig, raw_sig, raw_mass, raw_strength, raw_mask, pull, inv_mass, ice, base, force, edge_force, cor,
    bands, ocean, low, high, corner_out, corner_in, strip, f_out, f_in, sums, partial,
    in_sem, f_send, f_recv, h_send, h_recv, y_send, y_recv, p_send, p_recv, o_sem, r_send, r_recv, ready,
):
    gx = lax.axis_index("gx")
    gy = lax.axis_index("gy")
    f32 = jnp.float32
    T = PAD + R

    def at(dx, dy):
        return {"gx": lax.rem(gx + dx + G, G), "gy": lax.rem(gy + dy + Y, Y)}

    def remote(src, dst, send, recv, where):
        return pltpu.make_async_remote_copy(
            src_ref=src, dst_ref=dst, send_sem=send, recv_sem=recv, device_id=where, device_id_type=MESH
        )

    def settle(ref, sem):
        pltpu.make_async_copy(ref, ref, sem).wait()

    barrier = pltpu.get_barrier_semaphore()
    partners = [(dx, dy) for dx in range(G) for dy in range(Y) if dx or dy]
    hop = G // 4
    rounds = 5
    known = Y - 1
    for n in range(1, hop + 1):
        known = known + (gx >= n).astype(jnp.int32) + (gx + n < G).astype(jnp.int32)

    def greet(sem):
        for n in range(1, hop + 1):
            for d, there in ((-n, gx >= n), (n, gx + n < G)):

                @pl.when(there)
                def _():
                    pl.semaphore_signal(sem, inc=1, device_id={"gx": gx + d, "gy": gy}, device_id_type=MESH)

        for d in range(1, Y):
            pl.semaphore_signal(sem, inc=1, device_id=at(0, d), device_id_type=MESH)

    def meet(n):
        pl.semaphore_wait(ready.at[n - 2], known)
        if n < rounds:
            greet(ready.at[n - 1])

    greet(barrier)
    inner = pl.ds(PAD, R)
    loads = [
        pltpu.make_async_copy(forcing_in, bands, in_sem.at[0]),
        pltpu.make_async_copy(vel_in, vel.at[:, 0, inner], in_sem.at[1]),
        pltpu.make_async_copy(sig_in, raw_sig.at[:, inner], in_sem.at[2]),
        pltpu.make_async_copy(mass_in, raw_mass.at[inner], in_sem.at[3]),
        pltpu.make_async_copy(strength_in, raw_strength.at[inner], in_sem.at[4]),
        pltpu.make_async_copy(mask_in, raw_mask.at[inner], in_sem.at[5]),
    ]
    for copy in loads:
        copy.start()

    under, over = pl.ds(PAD - DEEP, DEEP), pl.ds(T, DEEP)
    lane8 = lax.broadcasted_iota(jnp.int32, (DEEP, LANES), 1)

    def outside(rows, slot, corners):
        for c in range(2):
            vel[c, 0, rows] = jnp.zeros((DEEP, C), f32)
        for c in range(3):
            raw_sig[c, rows] = jnp.zeros((DEEP, C), f32)
        raw_mass[rows] = jnp.ones((DEEP, C), f32)
        raw_strength[rows] = jnp.zeros((DEEP, C), f32)
        raw_mask[rows] = jnp.zeros((DEEP, C), jnp.int32)
        for c in range(4):
            force[c, rows] = jnp.zeros((DEEP, C), f32)
        f_in[slot] = jnp.zeros((2 * REACH, LANES), f32)
        for c in corners:
            corner_in[c] = jnp.where(lane8 // (2 * DEEP) == 5, 1.0, 0.0)

    has_south, has_north = gy > 0, gy < Y - 1
    pl.when(jnp.logical_not(has_south))(lambda: outside(under, 0, (SW, SE)))
    pl.when(jnp.logical_not(has_north))(lambda: outside(over, G + 1, (NW, NE)))

    for ref in (vel, sig):
        for c in range(ref.shape[0]):
            for w in range(2):
                for r in (0, T + DEEP):
                    ref[c, w, r : r + DEEP] = jnp.zeros((DEEP, C), f32)
    for n in range(PAD - DEEP, T + DEEP, DEEP):
        lat = (gy * R + (n - PAD) + lax.broadcasted_iota(jnp.int32, (DEEP, C), 0)).astype(f32)
        cor[n : n + DEEP] = 0.3 + 1.2 * (lat + 0.5) / (R * Y)

    low_half = gx < G // 2
    own_columns = pl.ds(pl.multiple_of(gx * C, C), C)
    mine = pl.ds(pl.multiple_of(gx * B, B), B)
    padded_mine = pl.ds(pl.multiple_of(PAD + gx * B, DEEP), B)
    pl.semaphore_wait(barrier, known)
    greet(ready.at[0])
    loads[0].wait()
    def to_both(d, send):
        for to, there in ((gx - d, gx >= d), (gx + d, gx + d < G)):
            pl.when(there)(lambda: send(to))

    def send_block(to):
        columns = pl.ds(pl.multiple_of(to * C, C), C)
        where = {"gx": to, "gy": gy}
        remote(bands.at[:, :, columns], force.at[:, padded_mine], f_send.at[0], f_recv.at[gx], where).start()

    def send_strip(to):
        where = {"gx": to, "gy": gy}
        remote(f_out.at[to], f_in.at[gx + 1], f_send.at[1], f_recv.at[gx], where).start()

    def send_both(to):
        send_block(to)
        send_strip(to)

    to_both(hop, send_block)
    chunks = [(n, CHUNK) for n in range(PAD, T, CHUNK)]
    skirts = [(PAD - DEEP, DEEP), (T, DEEP)]

    def prepare(w, p, n, s0, s1, s2, mass, strength, mask):
        ice[w, p : p + n] = mask
        pull[w, p : p + n] = 0.25 * strength * mask
        inv_mass[w, p : p + n] = 1.0 / mass
        sig[0, w, p : p + n] = (s0 + s1) * mask
        sig[1, w, p : p + n] = (s0 - s1) * mask
        sig[2, w, p : p + n] = 2.0 * s2 * mask

    def prepare_main(p, n):
        rows = pl.ds(p, n)
        prepare(
            0, p, n, raw_sig[0, rows], raw_sig[1, rows], raw_sig[2, rows],
            raw_mass[rows], raw_strength[rows], raw_mask[rows].astype(f32),
        )

    for copy in loads[1:]:
        copy.wait()
    fields = [vel.at[0, 0], vel.at[1, 0], raw_sig.at[0], raw_sig.at[1], raw_sig.at[2], raw_mass, raw_strength, raw_mask]
    west_tile = jnp.zeros((DEEP, LANES), f32)
    east_tile = jnp.zeros((DEEP, LANES), f32)
    for q, field in enumerate(fields):
        t = field[PAD:T, :].astype(f32).T
        lo, hi = t[0:DEEP], t[C - DEEP : C]
        low[q] = lo
        high[q] = hi
        spot = lane8 // (2 * DEEP) == q
        turn = 2 * DEEP * q + DEEP

        def corner(rows):
            both = jnp.where(lane8 < DEEP, rows[:, 0:LANES], rows[:, R - LANES : R])
            return pltpu.roll(both, turn, 1)

        west_tile = jnp.where(spot, corner(lo), west_tile)
        east_tile = jnp.where(spot, corner(hi), east_tile)
    corner_out[0] = west_tile
    corner_out[1] = east_tile

    near, far = pl.ds(0, DEEP), pl.ds(DEEP, DEEP)
    centre = pl.ds(LANES, R)
    bottom, top = pl.ds(PAD, DEEP), pl.ds(T - DEEP, DEEP)
    stacks = (vel, raw_sig, raw_mass, raw_strength, raw_mask)

    def rows_of(ref, rows):
        if ref is vel:
            return ref.at[:, 0, rows]
        return ref.at[:, rows] if len(ref.shape) == 3 else ref.at[rows]

    sides = [
        remote(low, strip.at[:, far, centre], h_send.at[0], h_recv.at[0], at(-1, 0)),
        remote(high, strip.at[:, near, centre], h_send.at[1], h_recv.at[1], at(1, 0)),
    ]
    south = [
        remote(corner_out.at[0], corner_in.at[NE], h_send.at[2], h_recv.at[2], at(-1, -1)),
        remote(corner_out.at[1], corner_in.at[NW], h_send.at[3], h_recv.at[3], at(1, -1)),
    ]
    north = [
        remote(corner_out.at[0], corner_in.at[SE], h_send.at[4], h_recv.at[4], at(-1, 1)),
        remote(corner_out.at[1], corner_in.at[SW], h_send.at[5], h_recv.at[5], at(1, 1)),
    ]
    for c in range(G):
        t = bands[:, :, c * C : (c + 1) * C].reshape(4 * B, C).T
        f_out[(c + 1) % G, 0:REACH, 0 : 4 * B] = t[C - REACH : C]
        f_out[(c + G - 1) % G, REACH : 2 * REACH, 0 : 4 * B] = t[0:REACH]
    wraps = ((gx == 0, 0), (gx == G - 1, 1))

    def corners(wrapped):
        for valid, copies in ((has_south, south), (has_north, north)):
            for edge, n in wraps:
                there = edge if wrapped else jnp.logical_not(edge)
                pl.when(jnp.logical_and(valid, there))(copies[n].start)

    for edge, side in wraps:
        pl.when(jnp.logical_not(edge))(sides[side].start)

    @pl.when(has_south)
    def _():
        for ref in stacks:
            remote(rows_of(ref, bottom), rows_of(ref, over), y_send.at[0], y_recv.at[0], at(0, -1)).start()

    @pl.when(has_north)
    def _():
        for ref in stacks:
            remote(rows_of(ref, top), rows_of(ref, under), y_send.at[1], y_recv.at[1], at(0, 1)).start()

    to_both(hop, send_strip)
    meet(2)
    corners(False)
    to_both(2 * hop, send_both)
    f_in[gx + 1] = f_out[gx]
    force[:, padded_mine] = bands[:, :, own_columns]
    meet(3)
    to_both(3 * hop, send_both)
    for p, m in chunks:
        prepare_main(p, m)
    meet(4)
    for edge, side in wraps:
        pl.when(edge)(sides[side].start)
    meet(5)
    corners(True)
    for d in range(G - 1, 0, -1):
        if d % hop:
            to_both(d, send_both)
    pack8 = pl.ds(0, 8 * DEEP)

    @pl.when(has_north)
    def _():
        settle(cor.at[pack8], y_recv.at[0])
        for copy in south:
            copy.wait_recv()

    @pl.when(has_south)
    def _():
        settle(cor.at[pack8], y_recv.at[1])
        for copy in north:
            copy.wait_recv()

    for copy in sides:
        copy.wait_recv()
    for p, n in skirts:
        prepare_main(p, n)
    for q in range(8):
        turn = LANES - (2 * DEEP * q + DEEP)
        for side, (s, n) in ((near, (SW, NW)), (far, (SE, NE))):
            strip[q, side, 0:LANES] = pltpu.roll(corner_in[s], turn, 1)
            strip[q, side, LANES + R : 2 * LANES + R] = pltpu.roll(corner_in[n], turn, 1)
    for tile in range(R // LANES + 2):
        t = strip[:, :, tile * LANES : (tile + 1) * LANES].reshape(8 * 2 * DEEP, LANES).T
        if tile == 0:
            t, p = t[LANES - DEEP :], PAD - DEEP
        elif tile == R // LANES + 1:
            t, p = t[:DEEP], T
        else:
            p = PAD + (tile - 1) * LANES
        for r in range(0, t.shape[0], CHUNK):
            part = t[r : r + CHUNK]
            n = part.shape[0]
            turned = [pltpu.roll(part, LANES - (2 * DEEP * q + DEEP), 1) for q in range(8)]
            vel[0, 1, p + r : p + r + n] = turned[0]
            vel[1, 1, p + r : p + r + n] = turned[1]
            prepare(1, p + r, n, *turned[2:])

    def shifted(a, b, lane):
        ra, rb = pltpu.roll(a, C - 1, 1), pltpu.roll(b, C - 1, 1)
        la, lb = pltpu.roll(a, 1, 1), pltpu.roll(b, 1, 1)
        right, left = lane == C - 1, lane == 0
        return (
            jnp.where(right, rb, ra) - jnp.where(left, lb, la),
            jnp.where(right, ra, rb) - jnp.where(left, la, lb),
        )

    everywhere = skirts[:1] + chunks + skirts[1:]
    row8 = lax.broadcasted_iota(jnp.int32, (DEEP, C), 0)

    def stress_step(last, spans, merge=False):
        for p, n, keep in spans:
            lane = lax.broadcasted_iota(jnp.int32, (n, C), 1)
            rows = pl.ds(p, n)
            dxu = shifted(vel[0, 0, rows], vel[0, 1, rows], lane)
            dxv = shifted(vel[1, 0, rows], vel[1, 1, rows], lane)
            for w in range(2):
                dyu = vel[0, w, p + 1 : p + n + 1] - vel[0, w, p - 1 : p + n - 1]
                dyv = vel[1, w, p + 1 : p + n + 1] - vel[1, w, p - 1 : p + n - 1]
                div = dxu[w] + dyv
                ten = dxu[w] - dyv
                shear = dyu + dxv[w]
                inv = lax.rsqrt(div * div + 0.25 * (ten * ten + shear * shear) + 0.01)
                hold = pull[w, rows]
                scaled = hold * inv
                quarter = 0.25 * scaled
                spread = scaled * div - hold
                twist = quarter * ten
                old = [sig[c, w, rows] for c in range(3)]
                new = [
                    0.75 * old[0] + (spread + twist),
                    0.75 * old[1] + (spread - twist),
                    0.75 * old[2] + quarter * shear,
                ]
                if keep is not None:
                    new = [jnp.where(keep, a, b) for a, b in zip(new, old)]
                for c in range(3):
                    sig[c, w, rows] = new[c]
                if last and w == 0 and PAD <= p < T and (keep is None or merge):
                    sig_out[0, p - PAD : p - PAD + n] = 0.5 * (new[0] + new[1])
                    sig_out[1, p - PAD : p - PAD + n] = 0.5 * (new[0] - new[1])
                    sig_out[2, p - PAD : p - PAD + n] = 0.5 * new[2]

    def drag_of(u, v, cu, cv):
        a = cu - u
        b = cv - v
        y = a * a + b * b + 0.01
        return y * lax.rsqrt(y)

    def velocity_step(k, spans, total, merge=False):
        last = k == ITERS - 1
        for p, n, keep in spans:
            inside = PAD <= p < T
            if last and not inside:
                continue
            lane = lax.broadcasted_iota(jnp.int32, (n, C), 1)
            rows = pl.ds(p, n)
            dxx = shifted(sig[0, 0, rows], sig[0, 1, rows], lane)
            dxy = shifted(sig[2, 0, rows], sig[2, 1, rows], lane)
            spin = cor[rows]
            for w in range(1 if last else 2):
                src = edge_force if w else force
                hi, lo = pl.ds(p + 1, n), pl.ds(p - 1, n)
                east = dxx[w] + (sig[2, w, hi] - sig[2, w, lo])
                north = dxy[w] + (sig[1, w, hi] - sig[1, w, lo])
                u, v = vel[0, w, rows], vel[1, w, rows]
                cu, cv = src[2, rows], src[3, rows]
                im = inv_mass[w, rows]
                if k == 0:
                    bu = u + src[0, rows] * im
                    bv = v + src[1, rows] * im
                    base[0, w, rows] = bu
                    base[1, w, rows] = bv
                else:
                    bu, bv = base[0, w, rows], base[1, w, rows]
                grip = drag_of(u, v, cu, cv) * im
                scale = ice[w, rows] / (5.0 + grip)
                push = 0.25 * im
                new_u = (4.0 * u + bu + east * push + grip * cu + spin * v) * scale
                new_v = (4.0 * v + bv + north * push + grip * cv - spin * u) * scale
                if keep is not None:
                    new_u = jnp.where(keep, new_u, u)
                    new_v = jnp.where(keep, new_v, v)
                if last and (keep is None or merge):
                    vel_out[0, p - PAD : p - PAD + n] = new_u
                    vel_out[1, p - PAD : p - PAD + n] = new_v
                    drag = drag_of(new_u, new_v, cu, cv) * ice[w, rows]
                    ocean[0, p - PAD : p - PAD + n] = drag * (new_u - cu)
                    ocean[1, p - PAD : p - PAD + n] = drag * (new_v - cv)
                else:
                    vel[0, w, rows] = new_u
                    vel[1, w, rows] = new_v
                if w == 0 and inside:
                    du = new_u - u
                    dv = new_v - v
                    square = du * du + dv * dv
                    for g in range(0, n, DEEP):
                        total = total + square[g : g + DEEP]
        return total

    def spans_of(lo, hi):
        return [(p, min(CHUNK, hi - p), None) for p in range(lo, hi, CHUNK)]

    stress_step(False, [(p, n, None) for p, n in everywhere])

    share = pl.ds(0, 4 * B + 2 * REACH)

    def forward(to_north):
        band = jnp.where(to_north, G - 1, 0)

        @pl.when(band != gx)
        def _():
            settle(cor.at[share], f_recv.at[band])

        src = pl.ds(pl.multiple_of(jnp.where(to_north, T - DEEP, PAD), DEEP), DEEP)
        dst = pl.ds(pl.multiple_of(jnp.where(to_north, PAD - DEEP, T), DEEP), DEEP)
        step = jnp.where(to_north, 1, Y - 1)
        way = to_north.astype(jnp.int32)

        @pl.when(jnp.where(to_north, gy < Y - 1, gy > 0))
        def _():
            remote(force.at[:, src], force.at[:, dst], p_send.at[way], p_recv.at[way], at(0, step)).start()
            remote(
                f_in.at[band + 1], f_in.at[jnp.where(to_north, 0, G + 1)], p_send.at[way], p_recv.at[way], at(0, step)
            ).start()

    forward(low_half)
    forward(jnp.logical_not(low_half))
    skirt = pl.ds(0, 4 * DEEP + 2 * REACH)

    def arrive(bs):
        for b in bs:

            @pl.when(gx != b)
            def _():
                settle(cor.at[share], f_recv.at[b])

    def edges(bs):
        for s in range(0, len(bs), 8):
            group = bs[s : s + 8]
            parts = [f_in[b + 1] for b in group]
            fill = LANES - 2 * REACH * len(group)
            t = jnp.concatenate(parts + [jnp.zeros((fill, LANES), f32)], axis=0).T
            for n, b in enumerate(group):
                turn = LANES - (2 * REACH * n + REACH)
                for c in range(4):
                    part = t[c * B : (c + 1) * B]
                    if b == -1:
                        edge_force[c, under] = pltpu.roll(part[B - DEEP :], turn, 1)
                    elif b == G:
                        edge_force[c, over] = pltpu.roll(part[:DEEP], turn, 1)
                    else:
                        edge_force[c, PAD + b * B : PAD + (b + 1) * B] = pltpu.roll(part, turn, 1)

    def send_rows(b, r, n):
        @pl.when(gx != b)
        def _():
            remote(
                ocean.at[:, pl.ds(b * B + r, n)], os_out.at[:, pl.ds(r, n), own_columns],
                o_sem.at[0], o_sem.at[1], {"gx": b, "gy": gy},
            ).start()

    def phases(is_low):
        late = list(range(G // 2, G // 2 + G // 4)) if is_low else list(range(G // 2 - G // 4, G // 2))
        early = [b for b in range(G) if b not in late]
        w0, w1 = PAD + late[0] * B, PAD + (late[-1] + 1) * B
        arrive([b for b in early if 0 < b < G - 1])

        @pl.when(has_south)
        def _():
            settle(cor.at[pack8], y_send.at[0])
            settle(cor.at[skirt], p_recv.at[1])

        @pl.when(has_north)
        def _():
            settle(cor.at[pack8], y_send.at[1])
            settle(cor.at[skirt], p_recv.at[0])

        edges([-1] + early + [G])
        outer = (
            [(PAD - DEEP, DEEP, None)] + spans_of(PAD, w0 - DEEP) + spans_of(w1 + DEEP, T) + [(T, DEEP, None)]
        )
        rims = ((w0 - DEEP, DEEP), (w1, DEEP))

        def first(h):
            if h == 0:
                return outer + [(p, n, None) for p, n in rims]
            return outer + [(*rims[0], row8 < DEEP - h), (*rims[1], row8 >= h)]

        def second(h):
            inside = spans_of(w0, w1)
            if h == 0:
                return inside
            return inside + [(*rims[0], row8 >= DEEP - h), (*rims[1], row8 < h)]

        totals = [jnp.zeros((DEEP, C), f32)] * ITERS
        totals[0] = velocity_step(0, first(0), totals[0])
        for k in range(1, ITERS):
            stress_step(k == ITERS - 1, first(2 * k - 1))
            totals[k] = velocity_step(k, first(2 * k), totals[k])
        order = list(range(G - 1, -1, -1)) if is_low else list(range(G))
        rest = []
        for b in order:
            if b in late:
                rest.append((b, 0, B))
                continue
            r, n = 0, B
            if b == late[0] - 1:
                n -= DEEP
                rest.append((b, n, DEEP))
            elif b == late[-1] + 1:
                r, n = DEEP, n - DEEP
                rest.append((b, 0, DEEP))
            if n:
                send_rows(b, r, n)
        arrive(late)
        edges(late)
        totals[0] = velocity_step(0, second(0), totals[0])
        for k in range(1, ITERS):
            stress_step(k == ITERS - 1, second(2 * k - 1), True)
            totals[k] = velocity_step(k, second(2 * k), totals[k], True)
        answer = jnp.zeros((1, LANES), f32)
        for k in range(ITERS):
            answer = jnp.where(lane1 == k, jnp.sum(totals[k]), answer)
        sums[...] = answer
        me = gx * Y + gy
        for dx, dy in partners:
            remote(sums, partial.at[me], r_send.at[0], r_recv.at[0], at(dx, dy)).start()
        partial[me] = answer
        for b, r, n in rest:
            send_rows(b, r, n)

    lane1 = lax.broadcasted_iota(jnp.int32, (1, LANES), 1)
    pl.when(low_half)(lambda: phases(True))
    pl.when(jnp.logical_not(low_half))(lambda: phases(False))
    os_out[:, :, own_columns] = ocean[:, mine]
    most = pl.ds(0, (G - 1) * C)
    settle(os_out.at[:, :, most], o_sem.at[1])
    peers = pl.ds(0, len(partners))
    settle(partial.at[peers], r_recv.at[0])
    res_out[...] = jnp.sum(partial[...], axis=0)[0, :ITERS]
    settle(bands.at[:, :, most], f_send.at[0])
    settle(f_out.at[pl.ds(0, G - 1)], f_send.at[1])
    settle(os_out.at[:, :, most], o_sem.at[0])
    for copy in sides:
        copy.wait_send()

    @pl.when(has_south)
    def _():
        for copy in south:
            copy.wait_send()
        settle(cor.at[skirt], p_send.at[0])

    @pl.when(has_north)
    def _():
        for copy in north:
            copy.wait_send()
        settle(cor.at[skirt], p_send.at[1])

    settle(partial.at[peers], r_send.at[0])


def store(vel, sig, res, ocean, vel_out, sig_out, res_out, ocean_out, sem):
    pairs = ((sig, sig_out), (vel, vel_out), (ocean, ocean_out), (res, res_out))
    copies = [pltpu.make_async_copy(src, dst, sem.at[n]) for n, (src, dst) in enumerate(pairs)]
    for copy in copies:
        copy.start()
    for copy in copies:
        copy.wait()


def local(velocity, stress, ice_mass, strength, land_mask, ocean_forcing):
    G, Y = lax.axis_size("gx"), lax.axis_size("gy")
    R, C = velocity.shape[1:]
    B = ocean_forcing.shape[1]
    f32 = jnp.float32
    rows = R + 2 * PAD
    dma = pltpu.SemaphoreType.DMA
    any_space = pl.BlockSpec(memory_space=pl.ANY)
    vmem_space = pl.BlockSpec(memory_space=pltpu.VMEM)
    done = pl.pallas_call(
        functools.partial(kernel, G, Y, R, C, B),
        out_shape=(
            pltpu.VMEM(velocity.shape, f32),
            pltpu.VMEM(stress.shape, f32),
            pltpu.VMEM((ITERS,), f32),
            pltpu.VMEM((2,) + ocean_forcing.shape[1:], f32),
        ),
        in_specs=[any_space] * 6,
        out_specs=(vmem_space,) * 4,
        scratch_shapes=[
            pltpu.VMEM((2, 2, rows, C), f32),
            pltpu.VMEM((3, 2, rows, C), f32),
            pltpu.VMEM((3, rows, C), f32),
            pltpu.VMEM((rows, C), f32),
            pltpu.VMEM((rows, C), f32),
            pltpu.VMEM((rows, C), jnp.int32),
            pltpu.VMEM((2, rows, C), f32),
            pltpu.VMEM((2, rows, C), f32),
            pltpu.VMEM((2, rows, C), f32),
            pltpu.VMEM((2, 2, rows, C), f32),
            pltpu.VMEM((4, rows, C), f32),
            pltpu.VMEM((4, rows, C), f32),
            pltpu.VMEM((rows, C), f32),
            pltpu.VMEM(ocean_forcing.shape, f32),
            pltpu.VMEM((2, R, C), f32),
            pltpu.VMEM((8, DEEP, R), f32),
            pltpu.VMEM((8, DEEP, R), f32),
            pltpu.VMEM((2, DEEP, LANES), f32),
            pltpu.VMEM((4, DEEP, LANES), f32),
            pltpu.VMEM((8, 2 * DEEP, R + 2 * LANES), f32),
            pltpu.VMEM((G, 2 * REACH, LANES), f32),
            pltpu.VMEM((G + 2, 2 * REACH, LANES), f32),
            pltpu.VMEM((1, LANES), f32),
            pltpu.VMEM((G * Y, 1, LANES), f32),
            dma((6,)),
            dma((2,)),
            dma((G,)),
            dma((6,)),
            dma((6,)),
            dma((2,)),
            dma((2,)),
            dma((2,)),
            dma((2,)),
            dma((2,)),
            dma((1,)),
            dma((1,)),
            pltpu.SemaphoreType.REGULAR((4,)),
        ],
        compiler_params=pltpu.CompilerParams(collective_id=0, has_side_effects=True),
    )(velocity, stress, ice_mass, strength, land_mask, ocean_forcing)
    return pl.pallas_call(
        store,
        out_shape=tuple(jax.ShapeDtypeStruct(x.shape, f32) for x in done),
        in_specs=[vmem_space] * 4,
        out_specs=(any_space,) * 4,
        scratch_shapes=[dma((4,))],
    )(*[pltpu.with_memory_space_constraint(x, pltpu.VMEM) for x in done])


def solution(mesh):
    placed = (
        P(None, "gy", "gx"),
        P(None, "gy", "gx"),
        P("gy", "gx"),
        P("gy", "gx"),
        P("gy", "gx"),
        P(None, ("gy", "gx"), None),
    )
    return jax.shard_map(
        local,
        mesh=mesh,
        in_specs=placed,
        out_specs=(P(None, "gy", "gx"), P(None, "gy", "gx"), P(), P(None, ("gy", "gx"), None)),
        check_vma=False,
    )
```

```python
import functools

import jax
import jax.numpy as jnp
from jax import lax
from jax.experimental import pallas as pl
from jax.experimental.pallas import tpu as pltpu
from jax.sharding import PartitionSpec as P

ITERS = 4
DEEP = 8
PAD = 16
LANES = 128
CHUNK = 16
REACH = 6
MESH = pl.DeviceIdType.MESH
SW, SE, NW, NE = range(4)


def kernel(
    G, Y, R, C, B,
    vel_in, sig_in, mass_in, strength_in, mask_in, forcing_in,
    vel_out, sig_out, res_out, os_out,
    vel, sig, raw_sig, raw_mass, raw_strength, raw_mask, pull, inv_mass, ice, base, force, edge_force, cor,
    bands, ocean, low, high, corner_out, corner_in, strip, f_out, f_in, sums, partial,
    in_sem, f_send, f_recv, e_recv, h_send, h_recv, y_send, y_recv, p_send, p_recv, o_sem, r_send, r_recv, ready,
):
    gx = lax.axis_index("gx")
    gy = lax.axis_index("gy")
    f32 = jnp.float32
    T = PAD + R

    def at(dx, dy):
        return {"gx": lax.rem(gx + dx + G, G), "gy": lax.rem(gy + dy + Y, Y)}

    def remote(src, dst, send, recv, where):
        return pltpu.make_async_remote_copy(
            src_ref=src, dst_ref=dst, send_sem=send, recv_sem=recv, device_id=where, device_id_type=MESH
        )

    def settle(ref, sem):
        pltpu.make_async_copy(ref, ref, sem).wait()

    barrier = pltpu.get_barrier_semaphore()
    partners = [(dx, dy) for dx in range(G) for dy in range(Y) if dx or dy]
    hop = G // 4
    rounds = 5
    known = Y - 1
    for n in range(1, hop + 1):
        known = known + (gx >= n).astype(jnp.int32) + (gx + n < G).astype(jnp.int32)

    def greet(sem):
        for n in range(1, hop + 1):
            for d, there in ((-n, gx >= n), (n, gx + n < G)):

                @pl.when(there)
                def _():
                    pl.semaphore_signal(sem, inc=1, device_id={"gx": gx + d, "gy": gy}, device_id_type=MESH)

        for d in range(1, Y):
            pl.semaphore_signal(sem, inc=1, device_id=at(0, d), device_id_type=MESH)

    def meet(n):
        pl.semaphore_wait(ready.at[n - 2], known)
        if n < rounds:
            greet(ready.at[n - 1])

    greet(barrier)
    inner = pl.ds(PAD, R)
    loads = [
        pltpu.make_async_copy(forcing_in, bands, in_sem.at[0]),
        pltpu.make_async_copy(vel_in, vel.at[:, 0, inner], in_sem.at[1]),
        pltpu.make_async_copy(sig_in, raw_sig.at[:, inner], in_sem.at[2]),
        pltpu.make_async_copy(mass_in, raw_mass.at[inner], in_sem.at[3]),
        pltpu.make_async_copy(strength_in, raw_strength.at[inner], in_sem.at[4]),
        pltpu.make_async_copy(mask_in, raw_mask.at[inner], in_sem.at[5]),
    ]
    for copy in loads:
        copy.start()

    under, over = pl.ds(PAD - DEEP, DEEP), pl.ds(T, DEEP)
    lane8 = lax.broadcasted_iota(jnp.int32, (DEEP, LANES), 1)

    def outside(rows, slot, corners):
        for c in range(2):
            vel[c, 0, rows] = jnp.zeros((DEEP, C), f32)
        for c in range(3):
            raw_sig[c, rows] = jnp.zeros((DEEP, C), f32)
        raw_mass[rows] = jnp.ones((DEEP, C), f32)
        raw_strength[rows] = jnp.zeros((DEEP, C), f32)
        raw_mask[rows] = jnp.zeros((DEEP, C), jnp.int32)
        for c in range(4):
            force[c, rows] = jnp.zeros((DEEP, C), f32)
        f_in[slot] = jnp.zeros((2 * REACH, LANES), f32)
        for c in corners:
            corner_in[c] = jnp.where(lane8 // (2 * DEEP) == 5, 1.0, 0.0)

    has_south, has_north = gy > 0, gy < Y - 1
    pl.when(jnp.logical_not(has_south))(lambda: outside(under, 0, (SW, SE)))
    pl.when(jnp.logical_not(has_north))(lambda: outside(over, G + 1, (NW, NE)))

    for ref in (vel, sig):
        for c in range(ref.shape[0]):
            for w in range(2):
                for r in (0, T + DEEP):
                    ref[c, w, r : r + DEEP] = jnp.zeros((DEEP, C), f32)
    for n in range(PAD - DEEP, T + DEEP, DEEP):
        lat = (gy * R + (n - PAD) + lax.broadcasted_iota(jnp.int32, (DEEP, C), 0)).astype(f32)
        cor[n : n + DEEP] = 0.3 + 1.2 * (lat + 0.5) / (R * Y)

    low_half = gx < G // 2
    own_columns = pl.ds(pl.multiple_of(gx * C, C), C)
    mine = pl.ds(pl.multiple_of(gx * B, B), B)
    padded_mine = pl.ds(pl.multiple_of(PAD + gx * B, DEEP), B)
    pl.semaphore_wait(barrier, known)
    greet(ready.at[0])
    loads[0].wait()
    at_end = jnp.logical_or(gx == 0, gx == G - 1)
    on_top = (gx == G - 1).astype(jnp.int32)
    rim_row = on_top * (B - DEEP)
    rest_row = (1 - on_top) * DEEP

    def to_each(d, send, ways=(-1, 1), only=None):
        for way in ways:
            to = gx + way * d
            there = gx >= d if way < 0 else gx + d < G
            if only is not None:
                there = jnp.logical_and(there, only)
            pl.when(there)(lambda: send(to))

    def send_rows_of(to, row, n, sem):
        columns = pl.ds(pl.multiple_of(to * C, C), C)
        src = pl.ds(pl.multiple_of(row, DEEP), n)
        dst = pl.ds(pl.multiple_of(PAD + gx * B + row, DEEP), n)
        where = {"gx": to, "gy": gy}
        remote(bands.at[:, src, columns], force.at[:, dst], f_send.at[0], sem, where).start()

    def send_block(to):
        pl.when(jnp.logical_not(at_end))(lambda: send_rows_of(to, 0, B, f_recv.at[gx]))
        if B > DEEP:
            pl.when(at_end)(lambda: send_rows_of(to, rest_row, B - DEEP, f_recv.at[gx]))

    def strip_to(to, sem):
        where = {"gx": to, "gy": gy}
        remote(f_out.at[to], f_in.at[gx + 1], f_send.at[1], sem, where).start()

    def send_strip(to):
        pl.when(jnp.logical_not(at_end))(lambda: strip_to(to, f_recv.at[gx]))

    def send_both(to):
        send_block(to)
        send_strip(to)

    def send_rim(to):
        send_rows_of(to, rim_row, DEEP, e_recv.at[on_top])
        strip_to(to, e_recv.at[on_top])

    def send_rims(reach):
        for d in range(max(reach - hop, 0) + 1, min(reach, G - 1) + 1):
            to_each(d, send_rim, only=at_end)

    def outward(d, send):
        to_each(d, send, (-1,), low_half)
        to_each(d, send, (1,), jnp.logical_not(low_half))

    def inward(d, send):
        to_each(d, send, (1,), low_half)
        to_each(d, send, (-1,), jnp.logical_not(low_half))

    to_each(hop, send_block)
    chunks = [(n, CHUNK) for n in range(PAD, T, CHUNK)]
    skirts = [(PAD - DEEP, DEEP), (T, DEEP)]

    def prepare(w, p, n, s0, s1, s2, mass, strength, mask):
        ice[w, p : p + n] = mask
        pull[w, p : p + n] = 0.25 * strength * mask
        inv_mass[w, p : p + n] = 1.0 / mass
        sig[0, w, p : p + n] = (s0 + s1) * mask
        sig[1, w, p : p + n] = (s0 - s1) * mask
        sig[2, w, p : p + n] = 2.0 * s2 * mask

    def prepare_main(p, n):
        rows = pl.ds(p, n)
        prepare(
            0, p, n, raw_sig[0, rows], raw_sig[1, rows], raw_sig[2, rows],
            raw_mass[rows], raw_strength[rows], raw_mask[rows].astype(f32),
        )

    for copy in loads[1:]:
        copy.wait()
    fields = [vel.at[0, 0], vel.at[1, 0], raw_sig.at[0], raw_sig.at[1], raw_sig.at[2], raw_mass, raw_strength, raw_mask]
    west_tile = jnp.zeros((DEEP, LANES), f32)
    east_tile = jnp.zeros((DEEP, LANES), f32)
    for q, field in enumerate(fields):
        t = field[PAD:T, :].astype(f32).T
        lo, hi = t[0:DEEP], t[C - DEEP : C]
        low[q] = lo
        high[q] = hi
        spot = lane8 // (2 * DEEP) == q
        turn = 2 * DEEP * q + DEEP

        def corner(rows):
            both = jnp.where(lane8 < DEEP, rows[:, 0:LANES], rows[:, R - LANES : R])
            return pltpu.roll(both, turn, 1)

        west_tile = jnp.where(spot, corner(lo), west_tile)
        east_tile = jnp.where(spot, corner(hi), east_tile)
    corner_out[0] = west_tile
    corner_out[1] = east_tile

    near, far = pl.ds(0, DEEP), pl.ds(DEEP, DEEP)
    centre = pl.ds(LANES, R)
    bottom, top = pl.ds(PAD, DEEP), pl.ds(T - DEEP, DEEP)
    stacks = (vel, raw_sig, raw_mass, raw_strength, raw_mask)

    def rows_of(ref, rows):
        if ref is vel:
            return ref.at[:, 0, rows]
        return ref.at[:, rows] if len(ref.shape) == 3 else ref.at[rows]

    sides = [
        remote(low, strip.at[:, far, centre], h_send.at[0], h_recv.at[0], at(-1, 0)),
        remote(high, strip.at[:, near, centre], h_send.at[1], h_recv.at[1], at(1, 0)),
    ]
    south = [
        remote(corner_out.at[0], corner_in.at[NE], h_send.at[2], h_recv.at[2], at(-1, -1)),
        remote(corner_out.at[1], corner_in.at[NW], h_send.at[3], h_recv.at[3], at(1, -1)),
    ]
    north = [
        remote(corner_out.at[0], corner_in.at[SE], h_send.at[4], h_recv.at[4], at(-1, 1)),
        remote(corner_out.at[1], corner_in.at[SW], h_send.at[5], h_recv.at[5], at(1, 1)),
    ]
    for c in range(G):
        t = bands[:, :, c * C : (c + 1) * C].reshape(4 * B, C).T
        f_out[(c + 1) % G, 0:REACH, 0 : 4 * B] = t[C - REACH : C]
        f_out[(c + G - 1) % G, REACH : 2 * REACH, 0 : 4 * B] = t[0:REACH]
    wraps = ((gx == 0, 0), (gx == G - 1, 1))

    def corners(wrapped):
        for valid, copies in ((has_south, south), (has_north, north)):
            for edge, n in wraps:
                there = edge if wrapped else jnp.logical_not(edge)
                pl.when(jnp.logical_and(valid, there))(copies[n].start)

    for edge, side in wraps:
        pl.when(jnp.logical_not(edge))(sides[side].start)

    @pl.when(has_south)
    def _():
        for ref in stacks:
            remote(rows_of(ref, bottom), rows_of(ref, over), y_send.at[0], y_recv.at[0], at(0, -1)).start()

    @pl.when(has_north)
    def _():
        for ref in stacks:
            remote(rows_of(ref, top), rows_of(ref, under), y_send.at[1], y_recv.at[1], at(0, 1)).start()

    to_each(hop, send_strip)
    send_rims(hop)
    meet(2)
    corners(False)
    send_rims(2 * hop)
    for d in range(2 * hop - 1, 0, -1):
        if d % hop:
            outward(d, send_both)
    to_each(2 * hop, send_both)
    f_in[gx + 1] = f_out[gx]
    force[:, padded_mine] = bands[:, :, own_columns]
    meet(3)
    send_rims(3 * hop)
    to_each(3 * hop, send_both)
    for p, m in chunks:
        prepare_main(p, m)
    meet(4)
    send_rims(4 * hop)
    for edge, side in wraps:
        pl.when(edge)(sides[side].start)
    meet(5)
    corners(True)
    for d in range(G - 1, 0, -1):
        if d % hop:
            inward(d, send_both)
            if d > 2 * hop:
                outward(d, send_both)
    skirt = pl.ds(0, 4 * DEEP + 2 * REACH)

    def forward(to_north):
        band = G - 1 if to_north else 0
        way = int(to_north)
        src = pl.ds(T - DEEP if to_north else PAD, DEEP)
        dst = pl.ds(PAD - DEEP if to_north else T, DEEP)

        @pl.when(gx != band)
        def _():
            settle(cor.at[skirt], e_recv.at[way])

        @pl.when(has_north if to_north else has_south)
        def _():
            to = at(0, 1 if to_north else -1)
            remote(force.at[:, src], force.at[:, dst], p_send.at[way], p_recv.at[way], to).start()
            remote(f_in.at[band + 1], f_in.at[0 if to_north else G + 1], p_send.at[way], p_recv.at[way], to).start()

    forward(True)
    forward(False)
    pack8 = pl.ds(0, 8 * DEEP)

    @pl.when(has_north)
    def _():
        settle(cor.at[pack8], y_recv.at[0])
        for copy in south:
            copy.wait_recv()

    @pl.when(has_south)
    def _():
        settle(cor.at[pack8], y_recv.at[1])
        for copy in north:
            copy.wait_recv()

    for copy in sides:
        copy.wait_recv()
    for p, n in skirts:
        prepare_main(p, n)
    for q in range(8):
        turn = LANES - (2 * DEEP * q + DEEP)
        for side, (s, n) in ((near, (SW, NW)), (far, (SE, NE))):
            strip[q, side, 0:LANES] = pltpu.roll(corner_in[s], turn, 1)
            strip[q, side, LANES + R : 2 * LANES + R] = pltpu.roll(corner_in[n], turn, 1)
    for tile in range(R // LANES + 2):
        t = strip[:, :, tile * LANES : (tile + 1) * LANES].reshape(8 * 2 * DEEP, LANES).T
        if tile == 0:
            t, p = t[LANES - DEEP :], PAD - DEEP
        elif tile == R // LANES + 1:
            t, p = t[:DEEP], T
        else:
            p = PAD + (tile - 1) * LANES
        for r in range(0, t.shape[0], CHUNK):
            part = t[r : r + CHUNK]
            n = part.shape[0]
            turned = [pltpu.roll(part, LANES - (2 * DEEP * q + DEEP), 1) for q in range(8)]
            vel[0, 1, p + r : p + r + n] = turned[0]
            vel[1, 1, p + r : p + r + n] = turned[1]
            prepare(1, p + r, n, *turned[2:])

    def shifted(a, b, lane):
        ra, rb = pltpu.roll(a, C - 1, 1), pltpu.roll(b, C - 1, 1)
        la, lb = pltpu.roll(a, 1, 1), pltpu.roll(b, 1, 1)
        right, left = lane == C - 1, lane == 0
        return (
            jnp.where(right, rb, ra) - jnp.where(left, lb, la),
            jnp.where(right, ra, rb) - jnp.where(left, la, lb),
        )

    everywhere = skirts[:1] + chunks + skirts[1:]
    row8 = lax.broadcasted_iota(jnp.int32, (DEEP, C), 0)

    def stress_step(last, spans, merge=False):
        for p, n, keep in spans:
            lane = lax.broadcasted_iota(jnp.int32, (n, C), 1)
            rows = pl.ds(p, n)
            dxu = shifted(vel[0, 0, rows], vel[0, 1, rows], lane)
            dxv = shifted(vel[1, 0, rows], vel[1, 1, rows], lane)
            for w in range(2):
                dyu = vel[0, w, p + 1 : p + n + 1] - vel[0, w, p - 1 : p + n - 1]
                dyv = vel[1, w, p + 1 : p + n + 1] - vel[1, w, p - 1 : p + n - 1]
                div = dxu[w] + dyv
                ten = dxu[w] - dyv
                shear = dyu + dxv[w]
                inv = lax.rsqrt(div * div + 0.25 * (ten * ten + shear * shear) + 0.01)
                hold = pull[w, rows]
                scaled = hold * inv
                quarter = 0.25 * scaled
                spread = scaled * div - hold
                twist = quarter * ten
                old = [sig[c, w, rows] for c in range(3)]
                new = [
                    0.75 * old[0] + (spread + twist),
                    0.75 * old[1] + (spread - twist),
                    0.75 * old[2] + quarter * shear,
                ]
                if keep is not None:
                    new = [jnp.where(keep, a, b) for a, b in zip(new, old)]
                for c in range(3):
                    sig[c, w, rows] = new[c]
                if last and w == 0 and PAD <= p < T and (keep is None or merge):
                    sig_out[0, p - PAD : p - PAD + n] = 0.5 * (new[0] + new[1])
                    sig_out[1, p - PAD : p - PAD + n] = 0.5 * (new[0] - new[1])
                    sig_out[2, p - PAD : p - PAD + n] = 0.5 * new[2]

    def drag_of(u, v, cu, cv):
        a = cu - u
        b = cv - v
        y = a * a + b * b + 0.01
        return y * lax.rsqrt(y)

    def velocity_step(k, spans, total, merge=False):
        last = k == ITERS - 1
        for p, n, keep in spans:
            inside = PAD <= p < T
            if last and not inside:
                continue
            lane = lax.broadcasted_iota(jnp.int32, (n, C), 1)
            rows = pl.ds(p, n)
            dxx = shifted(sig[0, 0, rows], sig[0, 1, rows], lane)
            dxy = shifted(sig[2, 0, rows], sig[2, 1, rows], lane)
            spin = cor[rows]
            for w in range(1 if last else 2):
                src = edge_force if w else force
                hi, lo = pl.ds(p + 1, n), pl.ds(p - 1, n)
                east = dxx[w] + (sig[2, w, hi] - sig[2, w, lo])
                north = dxy[w] + (sig[1, w, hi] - sig[1, w, lo])
                u, v = vel[0, w, rows], vel[1, w, rows]
                cu, cv = src[2, rows], src[3, rows]
                im = inv_mass[w, rows]
                if k == 0:
                    bu = u + src[0, rows] * im
                    bv = v + src[1, rows] * im
                    base[0, w, rows] = bu
                    base[1, w, rows] = bv
                else:
                    bu, bv = base[0, w, rows], base[1, w, rows]
                grip = drag_of(u, v, cu, cv) * im
                scale = ice[w, rows] / (5.0 + grip)
                push = 0.25 * im
                new_u = (4.0 * u + bu + east * push + grip * cu + spin * v) * scale
                new_v = (4.0 * v + bv + north * push + grip * cv - spin * u) * scale
                if keep is not None:
                    new_u = jnp.where(keep, new_u, u)
                    new_v = jnp.where(keep, new_v, v)
                if last and (keep is None or merge):
                    vel_out[0, p - PAD : p - PAD + n] = new_u
                    vel_out[1, p - PAD : p - PAD + n] = new_v
                    drag = drag_of(new_u, new_v, cu, cv) * ice[w, rows]
                    ocean[0, p - PAD : p - PAD + n] = drag * (new_u - cu)
                    ocean[1, p - PAD : p - PAD + n] = drag * (new_v - cv)
                else:
                    vel[0, w, rows] = new_u
                    vel[1, w, rows] = new_v
                if w == 0 and inside:
                    du = new_u - u
                    dv = new_v - v
                    square = du * du + dv * dv
                    for g in range(0, n, DEEP):
                        total = total + square[g : g + DEEP]
        return total

    def spans_of(lo, hi):
        return [(p, min(CHUNK, hi - p), None) for p in range(lo, hi, CHUNK)]

    stress_step(False, [(p, n, None) for p, n in everywhere])

    share = pl.ds(0, 4 * B + 2 * REACH)
    rest = pl.ds(0, 4 * (B - DEEP))
    def arrive(bs):
        for b in bs:

            @pl.when(gx != b)
            def _():
                if 0 < b < G - 1:
                    settle(cor.at[share], f_recv.at[b])
                elif B > DEEP:
                    settle(cor.at[rest], f_recv.at[b])

    def edges(bs):
        for s in range(0, len(bs), 8):
            group = bs[s : s + 8]
            parts = [f_in[b + 1] for b in group]
            fill = LANES - 2 * REACH * len(group)
            t = jnp.concatenate(parts + [jnp.zeros((fill, LANES), f32)], axis=0).T
            for n, b in enumerate(group):
                turn = LANES - (2 * REACH * n + REACH)
                for c in range(4):
                    part = t[c * B : (c + 1) * B]
                    if b == -1:
                        edge_force[c, under] = pltpu.roll(part[B - DEEP :], turn, 1)
                    elif b == G:
                        edge_force[c, over] = pltpu.roll(part[:DEEP], turn, 1)
                    else:
                        edge_force[c, PAD + b * B : PAD + (b + 1) * B] = pltpu.roll(part, turn, 1)

    def send_rows(b, r, n):
        @pl.when(gx != b)
        def _():
            remote(
                ocean.at[:, pl.ds(b * B + r, n)], os_out.at[:, pl.ds(r, n), own_columns],
                o_sem.at[0], o_sem.at[1], {"gx": b, "gy": gy},
            ).start()

    def phases(is_low):
        late = list(range(G // 2, G // 2 + G // 4)) if is_low else list(range(G // 2 - G // 4, G // 2))
        early = [b for b in range(G) if b not in late]
        w0, w1 = PAD + late[0] * B, PAD + (late[-1] + 1) * B
        arrive(early)

        @pl.when(has_south)
        def _():
            settle(cor.at[pack8], y_send.at[0])
            settle(cor.at[skirt], p_recv.at[1])

        @pl.when(has_north)
        def _():
            settle(cor.at[pack8], y_send.at[1])
            settle(cor.at[skirt], p_recv.at[0])

        edges([-1] + early + [G])
        outer = (
            [(PAD - DEEP, DEEP, None)] + spans_of(PAD, w0 - DEEP) + spans_of(w1 + DEEP, T) + [(T, DEEP, None)]
        )
        rims = ((w0 - DEEP, DEEP), (w1, DEEP))

        def first(h):
            if h == 0:
                return outer + [(p, n, None) for p, n in rims]
            return outer + [(*rims[0], row8 < DEEP - h), (*rims[1], row8 >= h)]

        def second(h):
            inside = spans_of(w0, w1)
            if h == 0:
                return inside
            return inside + [(*rims[0], row8 >= DEEP - h), (*rims[1], row8 < h)]

        totals = [jnp.zeros((DEEP, C), f32)] * ITERS
        totals[0] = velocity_step(0, first(0), totals[0])
        for k in range(1, ITERS):
            stress_step(k == ITERS - 1, first(2 * k - 1))
            totals[k] = velocity_step(k, first(2 * k), totals[k])
        order = list(range(G - 1, -1, -1)) if is_low else list(range(G))
        left = []
        for b in order:
            if b in late:
                left.append((b, 0, B))
                continue
            r, n = 0, B
            if b == late[0] - 1:
                n -= DEEP
                left.append((b, n, DEEP))
            elif b == late[-1] + 1:
                r, n = DEEP, n - DEEP
                left.append((b, 0, DEEP))
            if n:
                send_rows(b, r, n)
        arrive(late)
        edges(late)
        totals[0] = velocity_step(0, second(0), totals[0])
        for k in range(1, ITERS):
            stress_step(k == ITERS - 1, second(2 * k - 1), True)
            totals[k] = velocity_step(k, second(2 * k), totals[k], True)
        answer = jnp.zeros((1, LANES), f32)
        for k in range(ITERS):
            answer = jnp.where(lane1 == k, jnp.sum(totals[k]), answer)
        sums[...] = answer
        me = gx * Y + gy
        for dx, dy in partners:
            remote(sums, partial.at[me], r_send.at[0], r_recv.at[0], at(dx, dy)).start()
        partial[me] = answer
        for b, r, n in left:
            send_rows(b, r, n)

    lane1 = lax.broadcasted_iota(jnp.int32, (1, LANES), 1)
    pl.when(low_half)(lambda: phases(True))
    pl.when(jnp.logical_not(low_half))(lambda: phases(False))
    os_out[:, :, own_columns] = ocean[:, mine]
    most = pl.ds(0, (G - 1) * C)
    settle(os_out.at[:, :, most], o_sem.at[1])
    peers = pl.ds(0, len(partners))
    settle(partial.at[peers], r_recv.at[0])
    res_out[...] = jnp.sum(partial[...], axis=0)[0, :ITERS]
    settle(bands.at[:, :, most], f_send.at[0])
    settle(f_out.at[pl.ds(0, G - 1)], f_send.at[1])
    settle(os_out.at[:, :, most], o_sem.at[0])
    for copy in sides:
        copy.wait_send()

    @pl.when(has_south)
    def _():
        for copy in south:
            copy.wait_send()
        settle(cor.at[skirt], p_send.at[0])

    @pl.when(has_north)
    def _():
        for copy in north:
            copy.wait_send()
        settle(cor.at[skirt], p_send.at[1])

    settle(partial.at[peers], r_send.at[0])


def store(vel, sig, res, ocean, vel_out, sig_out, res_out, ocean_out, sem):
    pairs = ((sig, sig_out), (vel, vel_out), (ocean, ocean_out), (res, res_out))
    copies = [pltpu.make_async_copy(src, dst, sem.at[n]) for n, (src, dst) in enumerate(pairs)]
    for copy in copies:
        copy.start()
    for copy in copies:
        copy.wait()


def local(velocity, stress, ice_mass, strength, land_mask, ocean_forcing):
    G, Y = lax.axis_size("gx"), lax.axis_size("gy")
    R, C = velocity.shape[1:]
    B = ocean_forcing.shape[1]
    f32 = jnp.float32
    rows = R + 2 * PAD
    dma = pltpu.SemaphoreType.DMA
    any_space = pl.BlockSpec(memory_space=pl.ANY)
    vmem_space = pl.BlockSpec(memory_space=pltpu.VMEM)
    done = pl.pallas_call(
        functools.partial(kernel, G, Y, R, C, B),
        out_shape=(
            pltpu.VMEM(velocity.shape, f32),
            pltpu.VMEM(stress.shape, f32),
            pltpu.VMEM((ITERS,), f32),
            pltpu.VMEM((2,) + ocean_forcing.shape[1:], f32),
        ),
        in_specs=[any_space] * 6,
        out_specs=(vmem_space,) * 4,
        scratch_shapes=[
            pltpu.VMEM((2, 2, rows, C), f32),
            pltpu.VMEM((3, 2, rows, C), f32),
            pltpu.VMEM((3, rows, C), f32),
            pltpu.VMEM((rows, C), f32),
            pltpu.VMEM((rows, C), f32),
            pltpu.VMEM((rows, C), jnp.int32),
            pltpu.VMEM((2, rows, C), f32),
            pltpu.VMEM((2, rows, C), f32),
            pltpu.VMEM((2, rows, C), f32),
            pltpu.VMEM((2, 2, rows, C), f32),
            pltpu.VMEM((4, rows, C), f32),
            pltpu.VMEM((4, rows, C), f32),
            pltpu.VMEM((rows, C), f32),
            pltpu.VMEM(ocean_forcing.shape, f32),
            pltpu.VMEM((2, R, C), f32),
            pltpu.VMEM((8, DEEP, R), f32),
            pltpu.VMEM((8, DEEP, R), f32),
            pltpu.VMEM((2, DEEP, LANES), f32),
            pltpu.VMEM((4, DEEP, LANES), f32),
            pltpu.VMEM((8, 2 * DEEP, R + 2 * LANES), f32),
            pltpu.VMEM((G, 2 * REACH, LANES), f32),
            pltpu.VMEM((G + 2, 2 * REACH, LANES), f32),
            pltpu.VMEM((1, LANES), f32),
            pltpu.VMEM((G * Y, 1, LANES), f32),
            dma((6,)),
            dma((2,)),
            dma((G,)),
            dma((2,)),
            dma((6,)),
            dma((6,)),
            dma((2,)),
            dma((2,)),
            dma((2,)),
            dma((2,)),
            dma((2,)),
            dma((1,)),
            dma((1,)),
            pltpu.SemaphoreType.REGULAR((4,)),
        ],
        compiler_params=pltpu.CompilerParams(collective_id=0, has_side_effects=True),
    )(velocity, stress, ice_mass, strength, land_mask, ocean_forcing)
    return pl.pallas_call(
        store,
        out_shape=tuple(jax.ShapeDtypeStruct(x.shape, f32) for x in done),
        in_specs=[vmem_space] * 4,
        out_specs=(any_space,) * 4,
        scratch_shapes=[dma((4,))],
    )(*[pltpu.with_memory_space_constraint(x, pltpu.VMEM) for x in done])


def solution(mesh):
    placed = (
        P(None, "gy", "gx"),
        P(None, "gy", "gx"),
        P("gy", "gx"),
        P("gy", "gx"),
        P("gy", "gx"),
        P(None, ("gy", "gx"), None),
    )
    return jax.shard_map(
        local,
        mesh=mesh,
        in_specs=placed,
        out_specs=(P(None, "gy", "gx"), P(None, "gy", "gx"), P(), P(None, ("gy", "gx"), None)),
        check_vma=False,
    )
```

```python
import functools

import jax
import jax.numpy as jnp
from jax import lax
from jax.experimental import pallas as pl
from jax.experimental.pallas import tpu as pltpu
from jax.sharding import PartitionSpec as P

ITERS = 4
DEEP = 8
PAD = 16
LANES = 128
CHUNK = 16
REACH = 6
MESH = pl.DeviceIdType.MESH
SW, SE, NW, NE = range(4)


def kernel(
    G, Y, R, C, B,
    vel_in, sig_in, mass_in, strength_in, mask_in, forcing_in,
    vel_out, sig_out, res_out, os_out,
    vel, sig, raw_sig, raw_mass, raw_strength, raw_mask, pull, inv_mass, ice, base, force, edge_force, cor,
    bands, ocean, low, high, corner_out, corner_in, strip, f_out, f_in, sums, partial,
    in_sem, f_send, f_recv, e_recv, h_send, h_recv, y_send, y_recv, p_send, p_recv, o_sem, r_send, r_recv, ready,
):
    gx = lax.axis_index("gx")
    gy = lax.axis_index("gy")
    f32 = jnp.float32
    T = PAD + R

    def at(dx, dy):
        return {"gx": lax.rem(gx + dx + G, G), "gy": lax.rem(gy + dy + Y, Y)}

    def remote(src, dst, send, recv, where):
        return pltpu.make_async_remote_copy(
            src_ref=src, dst_ref=dst, send_sem=send, recv_sem=recv, device_id=where, device_id_type=MESH
        )

    def settle(ref, sem):
        pltpu.make_async_copy(ref, ref, sem).wait()

    barrier = pltpu.get_barrier_semaphore()
    partners = [(dx, dy) for dx in range(G) for dy in range(Y) if dx or dy]
    hop = G // 4
    rounds = 5
    known = Y - 1
    for n in range(1, hop + 1):
        known = known + (gx >= n).astype(jnp.int32) + (gx + n < G).astype(jnp.int32)

    def greet(sem):
        for n in range(1, hop + 1):
            for d, there in ((-n, gx >= n), (n, gx + n < G)):

                @pl.when(there)
                def _():
                    pl.semaphore_signal(sem, inc=1, device_id={"gx": gx + d, "gy": gy}, device_id_type=MESH)

        for d in range(1, Y):
            pl.semaphore_signal(sem, inc=1, device_id=at(0, d), device_id_type=MESH)

    def meet(n):
        pl.semaphore_wait(ready.at[n - 2], known)
        if n < rounds:
            greet(ready.at[n - 1])

    greet(barrier)
    inner = pl.ds(PAD, R)
    loads = [
        pltpu.make_async_copy(forcing_in, bands, in_sem.at[0]),
        pltpu.make_async_copy(vel_in, vel.at[:, 0, inner], in_sem.at[1]),
        pltpu.make_async_copy(sig_in, raw_sig.at[:, inner], in_sem.at[2]),
        pltpu.make_async_copy(mass_in, raw_mass.at[inner], in_sem.at[1]),
        pltpu.make_async_copy(strength_in, raw_strength.at[inner], in_sem.at[1]),
        pltpu.make_async_copy(mask_in, raw_mask.at[inner], in_sem.at[2]),
    ]
    for copy in loads:
        copy.start()

    under, over = pl.ds(PAD - DEEP, DEEP), pl.ds(T, DEEP)
    lane8 = lax.broadcasted_iota(jnp.int32, (DEEP, LANES), 1)

    def outside(rows, slot, corners):
        for c in range(2):
            vel[c, 0, rows] = jnp.zeros((DEEP, C), f32)
        for c in range(3):
            raw_sig[c, rows] = jnp.zeros((DEEP, C), f32)
        raw_mass[rows] = jnp.ones((DEEP, C), f32)
        raw_strength[rows] = jnp.zeros((DEEP, C), f32)
        raw_mask[rows] = jnp.zeros((DEEP, C), jnp.int32)
        for c in range(4):
            force[c, rows] = jnp.zeros((DEEP, C), f32)
        f_in[slot] = jnp.zeros((2 * REACH, LANES), f32)
        for c in corners:
            corner_in[c] = jnp.where(lane8 // (2 * DEEP) == 5, 1.0, 0.0)

    has_south, has_north = gy > 0, gy < Y - 1
    pl.when(jnp.logical_not(has_south))(lambda: outside(under, 0, (SW, SE)))
    pl.when(jnp.logical_not(has_north))(lambda: outside(over, G + 1, (NW, NE)))

    for ref in (vel, sig):
        for c in range(ref.shape[0]):
            for w in range(2):
                for r in (0, T + DEEP):
                    ref[c, w, r : r + DEEP] = jnp.zeros((DEEP, C), f32)
    for n in range(PAD - DEEP, T + DEEP, DEEP):
        lat = (gy * R + (n - PAD) + lax.broadcasted_iota(jnp.int32, (DEEP, C), 0)).astype(f32)
        cor[n : n + DEEP] = 0.3 + 1.2 * (lat + 0.5) / (R * Y)

    low_half = gx < G // 2
    own_columns = pl.ds(pl.multiple_of(gx * C, C), C)
    mine = pl.ds(pl.multiple_of(gx * B, B), B)
    padded_mine = pl.ds(pl.multiple_of(PAD + gx * B, DEEP), B)
    pl.semaphore_wait(barrier, known)
    greet(ready.at[0])
    loads[0].wait()
    at_end = jnp.logical_or(gx == 0, gx == G - 1)
    on_top = (gx == G - 1).astype(jnp.int32)
    rim_row = on_top * (B - DEEP)
    rest_row = (1 - on_top) * DEEP

    def to_each(d, send, ways=(-1, 1), only=None):
        for way in ways:
            to = gx + way * d
            there = gx >= d if way < 0 else gx + d < G
            if only is not None:
                there = jnp.logical_and(there, only)
            pl.when(there)(lambda: send(to))

    def send_rows_of(to, row, n, sem):
        columns = pl.ds(pl.multiple_of(to * C, C), C)
        src = pl.ds(pl.multiple_of(row, DEEP), n)
        dst = pl.ds(pl.multiple_of(PAD + gx * B + row, DEEP), n)
        where = {"gx": to, "gy": gy}
        remote(bands.at[:, src, columns], force.at[:, dst], f_send.at[0], sem, where).start()

    def send_block(to):
        pl.when(jnp.logical_not(at_end))(lambda: send_rows_of(to, 0, B, f_recv.at[gx]))
        if B > DEEP:
            pl.when(at_end)(lambda: send_rows_of(to, rest_row, B - DEEP, f_recv.at[gx]))

    def strip_to(to, sem):
        where = {"gx": to, "gy": gy}
        remote(f_out.at[to], f_in.at[gx + 1], f_send.at[1], sem, where).start()

    def send_strip(to):
        pl.when(jnp.logical_not(at_end))(lambda: strip_to(to, f_recv.at[gx]))

    def send_both(to):
        send_block(to)
        send_strip(to)

    def send_rim(to):
        send_rows_of(to, rim_row, DEEP, e_recv.at[on_top])
        strip_to(to, e_recv.at[on_top])

    def send_rims(reach):
        for d in range(max(reach - hop, 0) + 1, min(reach, G - 1) + 1):
            to_each(d, send_rim, only=at_end)

    def outward(d, send):
        to_each(d, send, (-1,), low_half)
        to_each(d, send, (1,), jnp.logical_not(low_half))

    def inward(d, send):
        to_each(d, send, (1,), low_half)
        to_each(d, send, (-1,), jnp.logical_not(low_half))

    to_each(hop, send_block)
    chunks = [(n, CHUNK) for n in range(PAD, T, CHUNK)]
    skirts = [(PAD - DEEP, DEEP), (T, DEEP)]

    def prepare(w, p, n, s0, s1, s2, mass, strength, mask):
        ice[w, p : p + n] = mask
        pull[w, p : p + n] = 0.25 * strength * mask
        inv_mass[w, p : p + n] = 1.0 / mass
        sig[0, w, p : p + n] = (s0 + s1) * mask
        sig[1, w, p : p + n] = (s0 - s1) * mask
        sig[2, w, p : p + n] = 2.0 * s2 * mask

    def prepare_main(p, n):
        rows = pl.ds(p, n)
        prepare(
            0, p, n, raw_sig[0, rows], raw_sig[1, rows], raw_sig[2, rows],
            raw_mass[rows], raw_strength[rows], raw_mask[rows].astype(f32),
        )

    settle(bands, in_sem.at[1])
    settle(bands, in_sem.at[2])
    fields = [vel.at[0, 0], vel.at[1, 0], raw_sig.at[0], raw_sig.at[1], raw_sig.at[2], raw_mass, raw_strength, raw_mask]
    west_tile = jnp.zeros((DEEP, LANES), f32)
    east_tile = jnp.zeros((DEEP, LANES), f32)
    for q, field in enumerate(fields):
        t = field[PAD:T, :].astype(f32).T
        lo, hi = t[0:DEEP], t[C - DEEP : C]
        low[q] = lo
        high[q] = hi
        spot = lane8 // (2 * DEEP) == q
        turn = 2 * DEEP * q + DEEP

        def corner(rows):
            both = jnp.where(lane8 < DEEP, rows[:, 0:LANES], rows[:, R - LANES : R])
            return pltpu.roll(both, turn, 1)

        west_tile = jnp.where(spot, corner(lo), west_tile)
        east_tile = jnp.where(spot, corner(hi), east_tile)
    corner_out[0] = west_tile
    corner_out[1] = east_tile

    near, far = pl.ds(0, DEEP), pl.ds(DEEP, DEEP)
    centre = pl.ds(LANES, R)
    bottom, top = pl.ds(PAD, DEEP), pl.ds(T - DEEP, DEEP)
    stacks = (vel, raw_sig, raw_mass, raw_strength, raw_mask)

    def rows_of(ref, rows):
        if ref is vel:
            return ref.at[:, 0, rows]
        return ref.at[:, rows] if len(ref.shape) == 3 else ref.at[rows]

    sides = [
        remote(low, strip.at[:, far, centre], h_send.at[0], h_recv.at[0], at(-1, 0)),
        remote(high, strip.at[:, near, centre], h_send.at[0], h_recv.at[0], at(1, 0)),
    ]
    south = [
        remote(corner_out.at[0], corner_in.at[NE], h_send.at[1], h_recv.at[1], at(-1, -1)),
        remote(corner_out.at[1], corner_in.at[NW], h_send.at[1], h_recv.at[1], at(1, -1)),
    ]
    north = [
        remote(corner_out.at[0], corner_in.at[SE], h_send.at[2], h_recv.at[2], at(-1, 1)),
        remote(corner_out.at[1], corner_in.at[SW], h_send.at[2], h_recv.at[2], at(1, 1)),
    ]
    for c in range(G):
        t = bands[:, :, c * C : (c + 1) * C].reshape(4 * B, C).T
        f_out[(c + 1) % G, 0:REACH, 0 : 4 * B] = t[C - REACH : C]
        f_out[(c + G - 1) % G, REACH : 2 * REACH, 0 : 4 * B] = t[0:REACH]
    wraps = ((gx == 0, 0), (gx == G - 1, 1))

    def corners(wrapped):
        for valid, copies in ((has_south, south), (has_north, north)):
            for edge, n in wraps:
                there = edge if wrapped else jnp.logical_not(edge)
                pl.when(jnp.logical_and(valid, there))(copies[n].start)

    for edge, side in wraps:
        pl.when(jnp.logical_not(edge))(sides[side].start)

    @pl.when(has_south)
    def _():
        for ref in stacks:
            remote(rows_of(ref, bottom), rows_of(ref, over), y_send.at[0], y_recv.at[0], at(0, -1)).start()

    @pl.when(has_north)
    def _():
        for ref in stacks:
            remote(rows_of(ref, top), rows_of(ref, under), y_send.at[1], y_recv.at[1], at(0, 1)).start()

    to_each(hop, send_strip)
    send_rims(hop)
    meet(2)
    corners(False)
    send_rims(2 * hop)
    for d in range(2 * hop - 1, 0, -1):
        if d % hop:
            outward(d, send_both)
    to_each(2 * hop, send_both)
    f_in[gx + 1] = f_out[gx]
    force[:, padded_mine] = bands[:, :, own_columns]
    meet(3)
    send_rims(3 * hop)
    to_each(3 * hop, send_both)
    for p, m in chunks:
        prepare_main(p, m)
    meet(4)
    send_rims(4 * hop)
    for edge, side in wraps:
        pl.when(edge)(sides[side].start)
    meet(5)
    corners(True)
    for d in range(G - 1, 0, -1):
        if d % hop:
            inward(d, send_both)
            if d > 2 * hop:
                outward(d, send_both)
    skirt = pl.ds(0, 4 * DEEP + 2 * REACH)

    def forward(to_north):
        band = G - 1 if to_north else 0
        way = int(to_north)
        src = pl.ds(T - DEEP if to_north else PAD, DEEP)
        dst = pl.ds(PAD - DEEP if to_north else T, DEEP)

        @pl.when(gx != band)
        def _():
            settle(cor.at[skirt], e_recv.at[way])

        @pl.when(has_north if to_north else has_south)
        def _():
            to = at(0, 1 if to_north else -1)
            remote(force.at[:, src], force.at[:, dst], p_send.at[way], p_recv.at[way], to).start()
            remote(f_in.at[band + 1], f_in.at[0 if to_north else G + 1], p_send.at[way], p_recv.at[way], to).start()

    forward(True)
    forward(False)
    pack8 = pl.ds(0, 8 * DEEP)
    pair = pl.ds(0, 2)

    @pl.when(has_north)
    def _():
        settle(cor.at[pack8], y_recv.at[0])
        settle(corner_in.at[pair], h_recv.at[1])

    @pl.when(has_south)
    def _():
        settle(cor.at[pack8], y_recv.at[1])
        settle(corner_in.at[pair], h_recv.at[2])

    settle(strip.at[:, :, centre], h_recv.at[0])
    for p, n in skirts:
        prepare_main(p, n)
    for q in range(8):
        turn = LANES - (2 * DEEP * q + DEEP)
        for side, (s, n) in ((near, (SW, NW)), (far, (SE, NE))):
            strip[q, side, 0:LANES] = pltpu.roll(corner_in[s], turn, 1)
            strip[q, side, LANES + R : 2 * LANES + R] = pltpu.roll(corner_in[n], turn, 1)
    for tile in range(R // LANES + 2):
        t = strip[:, :, tile * LANES : (tile + 1) * LANES].reshape(8 * 2 * DEEP, LANES).T
        if tile == 0:
            t, p = t[LANES - DEEP :], PAD - DEEP
        elif tile == R // LANES + 1:
            t, p = t[:DEEP], T
        else:
            p = PAD + (tile - 1) * LANES
        for r in range(0, t.shape[0], CHUNK):
            part = t[r : r + CHUNK]
            n = part.shape[0]
            turned = [pltpu.roll(part, LANES - (2 * DEEP * q + DEEP), 1) for q in range(8)]
            vel[0, 1, p + r : p + r + n] = turned[0]
            vel[1, 1, p + r : p + r + n] = turned[1]
            prepare(1, p + r, n, *turned[2:])

    def shifted(a, b, lane):
        ra, rb = pltpu.roll(a, C - 1, 1), pltpu.roll(b, C - 1, 1)
        la, lb = pltpu.roll(a, 1, 1), pltpu.roll(b, 1, 1)
        right, left = lane == C - 1, lane == 0
        return (
            jnp.where(right, rb, ra) - jnp.where(left, lb, la),
            jnp.where(right, ra, rb) - jnp.where(left, la, lb),
        )

    everywhere = skirts[:1] + chunks + skirts[1:]
    row8 = lax.broadcasted_iota(jnp.int32, (DEEP, C), 0)

    def stress_step(last, spans, merge=False):
        for p, n, keep in spans:
            lane = lax.broadcasted_iota(jnp.int32, (n, C), 1)
            rows = pl.ds(p, n)
            dxu = shifted(vel[0, 0, rows], vel[0, 1, rows], lane)
            dxv = shifted(vel[1, 0, rows], vel[1, 1, rows], lane)
            for w in range(2):
                dyu = vel[0, w, p + 1 : p + n + 1] - vel[0, w, p - 1 : p + n - 1]
                dyv = vel[1, w, p + 1 : p + n + 1] - vel[1, w, p - 1 : p + n - 1]
                div = dxu[w] + dyv
                ten = dxu[w] - dyv
                shear = dyu + dxv[w]
                inv = lax.rsqrt(div * div + 0.25 * (ten * ten + shear * shear) + 0.01)
                hold = pull[w, rows]
                scaled = hold * inv
                quarter = 0.25 * scaled
                spread = scaled * div - hold
                twist = quarter * ten
                old = [sig[c, w, rows] for c in range(3)]
                new = [
                    0.75 * old[0] + (spread + twist),
                    0.75 * old[1] + (spread - twist),
                    0.75 * old[2] + quarter * shear,
                ]
                if keep is not None:
                    new = [jnp.where(keep, a, b) for a, b in zip(new, old)]
                for c in range(3):
                    sig[c, w, rows] = new[c]
                if last and w == 0 and PAD <= p < T and (keep is None or merge):
                    sig_out[0, p - PAD : p - PAD + n] = 0.5 * (new[0] + new[1])
                    sig_out[1, p - PAD : p - PAD + n] = 0.5 * (new[0] - new[1])
                    sig_out[2, p - PAD : p - PAD + n] = 0.5 * new[2]

    def drag_of(u, v, cu, cv):
        a = cu - u
        b = cv - v
        y = a * a + b * b + 0.01
        return y * lax.rsqrt(y)

    def velocity_step(k, spans, total, merge=False):
        last = k == ITERS - 1
        for p, n, keep in spans:
            inside = PAD <= p < T
            if last and not inside:
                continue
            lane = lax.broadcasted_iota(jnp.int32, (n, C), 1)
            rows = pl.ds(p, n)
            dxx = shifted(sig[0, 0, rows], sig[0, 1, rows], lane)
            dxy = shifted(sig[2, 0, rows], sig[2, 1, rows], lane)
            spin = cor[rows]
            for w in range(1 if last else 2):
                src = edge_force if w else force
                hi, lo = pl.ds(p + 1, n), pl.ds(p - 1, n)
                east = dxx[w] + (sig[2, w, hi] - sig[2, w, lo])
                north = dxy[w] + (sig[1, w, hi] - sig[1, w, lo])
                u, v = vel[0, w, rows], vel[1, w, rows]
                cu, cv = src[2, rows], src[3, rows]
                im = inv_mass[w, rows]
                if k == 0:
                    bu = u + src[0, rows] * im
                    bv = v + src[1, rows] * im
                    base[0, w, rows] = bu
                    base[1, w, rows] = bv
                else:
                    bu, bv = base[0, w, rows], base[1, w, rows]
                grip = drag_of(u, v, cu, cv) * im
                scale = ice[w, rows] / (5.0 + grip)
                push = 0.25 * im
                new_u = (4.0 * u + bu + east * push + grip * cu + spin * v) * scale
                new_v = (4.0 * v + bv + north * push + grip * cv - spin * u) * scale
                if keep is not None:
                    new_u = jnp.where(keep, new_u, u)
                    new_v = jnp.where(keep, new_v, v)
                if last and (keep is None or merge):
                    vel_out[0, p - PAD : p - PAD + n] = new_u
                    vel_out[1, p - PAD : p - PAD + n] = new_v
                    drag = drag_of(new_u, new_v, cu, cv) * ice[w, rows]
                    ocean[0, p - PAD : p - PAD + n] = drag * (new_u - cu)
                    ocean[1, p - PAD : p - PAD + n] = drag * (new_v - cv)
                else:
                    vel[0, w, rows] = new_u
                    vel[1, w, rows] = new_v
                if w == 0 and inside:
                    du = new_u - u
                    dv = new_v - v
                    square = du * du + dv * dv
                    for g in range(0, n, DEEP):
                        total = total + square[g : g + DEEP]
        return total

    def spans_of(lo, hi):
        return [(p, min(CHUNK, hi - p), None) for p in range(lo, hi, CHUNK)]

    stress_step(False, [(p, n, None) for p, n in everywhere])

    share = pl.ds(0, 4 * B + 2 * REACH)
    rest = pl.ds(0, 4 * (B - DEEP))
    def arrive(bs):
        for b in bs:

            @pl.when(gx != b)
            def _():
                if 0 < b < G - 1:
                    settle(cor.at[share], f_recv.at[b])
                elif B > DEEP:
                    settle(cor.at[rest], f_recv.at[b])

    def edges(bs):
        for s in range(0, len(bs), 8):
            group = bs[s : s + 8]
            parts = [f_in[b + 1] for b in group]
            fill = LANES - 2 * REACH * len(group)
            t = jnp.concatenate(parts + [jnp.zeros((fill, LANES), f32)], axis=0).T
            for n, b in enumerate(group):
                turn = LANES - (2 * REACH * n + REACH)
                for c in range(4):
                    part = t[c * B : (c + 1) * B]
                    if b == -1:
                        edge_force[c, under] = pltpu.roll(part[B - DEEP :], turn, 1)
                    elif b == G:
                        edge_force[c, over] = pltpu.roll(part[:DEEP], turn, 1)
                    else:
                        edge_force[c, PAD + b * B : PAD + (b + 1) * B] = pltpu.roll(part, turn, 1)

    def send_rows(b, r, n):
        @pl.when(gx != b)
        def _():
            remote(
                ocean.at[:, pl.ds(b * B + r, n)], os_out.at[:, pl.ds(r, n), own_columns],
                o_sem.at[0], o_sem.at[1], {"gx": b, "gy": gy},
            ).start()

    outer = gx >= G - hop

    def phases(is_low):
        late = list(range(G // 2, G // 2 + G // 4)) if is_low else list(range(G // 2 - G // 4, G // 2))
        early = [b for b in range(G) if b not in late]
        w0, w1 = PAD + late[0] * B, PAD + (late[-1] + 1) * B
        def first(h, side):
            if side == 0:
                keep = None if h == 0 else row8 < DEEP - h
                return [(PAD - DEEP, DEEP, None)] + spans_of(PAD, w0 - DEEP) + [(w0 - DEEP, DEEP, keep)]
            keep = None if h == 0 else row8 >= h
            return [(w1, DEEP, keep)] + spans_of(w1 + DEEP, T) + [(T, DEEP, None)]

        def second(h):
            inside = spans_of(w0, w1)
            if h == 0:
                return inside
            return inside + [(w0 - DEEP, DEEP, row8 >= DEEP - h), (w1, DEEP, row8 < h)]

        totals = [jnp.zeros((DEEP, C), f32)] * ITERS
        left = [(b, 0, B) for b in late]
        for side in range(2):
            bs = [b for b in early if (b > late[0]) == bool(side)]
            arrive(bs)

            @pl.when(has_north if side else has_south)
            def _():
                settle(cor.at[pack8], y_send.at[side])
                settle(cor.at[skirt], p_recv.at[1 - side])

            edges(bs + [G] if side else [-1] + bs)
            totals[0] = velocity_step(0, first(0, side), totals[0])
            for k in range(1, ITERS):
                stress_step(k == ITERS - 1, first(2 * k - 1, side))
                totals[k] = velocity_step(k, first(2 * k, side), totals[k])
            ready_rows = []
            for b in reversed(bs) if side else bs:
                r, n = 0, B
                if b == late[0] - 1:
                    n -= DEEP
                    left.append((b, n, DEEP))
                elif b == late[-1] + 1:
                    r, n = DEEP, n - DEEP
                    left.append((b, 0, DEEP))
                if n:
                    ready_rows.append((b, r, n))

            def send_ready(pieces=tuple(ready_rows)):
                for piece in pieces:
                    send_rows(*piece)

            if side == 0:
                pl.when(jnp.logical_not(outer))(send_ready)
                later = send_ready
            else:
                send_ready()
                pl.when(outer)(later)
        arrive(late)
        edges(late)
        totals[0] = velocity_step(0, second(0), totals[0])
        for k in range(1, ITERS):
            stress_step(k == ITERS - 1, second(2 * k - 1), True)
            totals[k] = velocity_step(k, second(2 * k), totals[k], True)
        answer = jnp.zeros((1, LANES), f32)
        for k in range(ITERS):
            answer = jnp.where(lane1 == k, jnp.sum(totals[k]), answer)
        sums[...] = answer
        me = gx * Y + gy
        for dx, dy in partners:
            remote(sums, partial.at[me], r_send.at[0], r_recv.at[0], at(dx, dy)).start()
        partial[me] = answer
        for b, r, n in left:
            send_rows(b, r, n)

    lane1 = lax.broadcasted_iota(jnp.int32, (1, LANES), 1)
    pl.when(low_half)(lambda: phases(True))
    pl.when(jnp.logical_not(low_half))(lambda: phases(False))
    os_out[:, :, own_columns] = ocean[:, mine]
    most = pl.ds(0, (G - 1) * C)
    settle(os_out.at[:, :, most], o_sem.at[1])
    peers = pl.ds(0, len(partners))
    settle(partial.at[peers], r_recv.at[0])
    res_out[...] = jnp.sum(partial[...], axis=0)[0, :ITERS]
    settle(bands.at[:, :, most], f_send.at[0])
    settle(f_out.at[pl.ds(0, G - 1)], f_send.at[1])
    settle(os_out.at[:, :, most], o_sem.at[0])
    settle(strip.at[:, :, centre], h_send.at[0])

    @pl.when(has_south)
    def _():
        settle(corner_in.at[pair], h_send.at[1])
        settle(cor.at[skirt], p_send.at[0])

    @pl.when(has_north)
    def _():
        settle(corner_in.at[pair], h_send.at[2])
        settle(cor.at[skirt], p_send.at[1])

    settle(partial.at[peers], r_send.at[0])


def store(vel, sig, res, ocean, vel_out, sig_out, res_out, ocean_out, sem):
    pairs = ((sig, sig_out), (vel, vel_out), (ocean, ocean_out), (res, res_out))
    copies = [pltpu.make_async_copy(src, dst, sem.at[n]) for n, (src, dst) in enumerate(pairs)]
    for copy in copies:
        copy.start()
    for copy in copies:
        copy.wait()


def local(velocity, stress, ice_mass, strength, land_mask, ocean_forcing):
    G, Y = lax.axis_size("gx"), lax.axis_size("gy")
    R, C = velocity.shape[1:]
    B = ocean_forcing.shape[1]
    f32 = jnp.float32
    rows = R + 2 * PAD
    dma = pltpu.SemaphoreType.DMA
    any_space = pl.BlockSpec(memory_space=pl.ANY)
    vmem_space = pl.BlockSpec(memory_space=pltpu.VMEM)
    done = pl.pallas_call(
        functools.partial(kernel, G, Y, R, C, B),
        out_shape=(
            pltpu.VMEM(velocity.shape, f32),
            pltpu.VMEM(stress.shape, f32),
            pltpu.VMEM((ITERS,), f32),
            pltpu.VMEM((2,) + ocean_forcing.shape[1:], f32),
        ),
        in_specs=[any_space] * 6,
        out_specs=(vmem_space,) * 4,
        scratch_shapes=[
            pltpu.VMEM((2, 2, rows, C), f32),
            pltpu.VMEM((3, 2, rows, C), f32),
            pltpu.VMEM((3, rows, C), f32),
            pltpu.VMEM((rows, C), f32),
            pltpu.VMEM((rows, C), f32),
            pltpu.VMEM((rows, C), jnp.int32),
            pltpu.VMEM((2, rows, C), f32),
            pltpu.VMEM((2, rows, C), f32),
            pltpu.VMEM((2, rows, C), f32),
            pltpu.VMEM((2, 2, rows, C), f32),
            pltpu.VMEM((4, rows, C), f32),
            pltpu.VMEM((4, rows, C), f32),
            pltpu.VMEM((rows, C), f32),
            pltpu.VMEM(ocean_forcing.shape, f32),
            pltpu.VMEM((2, R, C), f32),
            pltpu.VMEM((8, DEEP, R), f32),
            pltpu.VMEM((8, DEEP, R), f32),
            pltpu.VMEM((2, DEEP, LANES), f32),
            pltpu.VMEM((4, DEEP, LANES), f32),
            pltpu.VMEM((8, 2 * DEEP, R + 2 * LANES), f32),
            pltpu.VMEM((G, 2 * REACH, LANES), f32),
            pltpu.VMEM((G + 2, 2 * REACH, LANES), f32),
            pltpu.VMEM((1, LANES), f32),
            pltpu.VMEM((G * Y, 1, LANES), f32),
            dma((3,)),
            dma((2,)),
            dma((G,)),
            dma((2,)),
            dma((3,)),
            dma((3,)),
            dma((2,)),
            dma((2,)),
            dma((2,)),
            dma((2,)),
            dma((2,)),
            dma((1,)),
            dma((1,)),
            pltpu.SemaphoreType.REGULAR((4,)),
        ],
        compiler_params=pltpu.CompilerParams(collective_id=0, has_side_effects=True),
    )(velocity, stress, ice_mass, strength, land_mask, ocean_forcing)
    return pl.pallas_call(
        store,
        out_shape=tuple(jax.ShapeDtypeStruct(x.shape, f32) for x in done),
        in_specs=[vmem_space] * 4,
        out_specs=(any_space,) * 4,
        scratch_shapes=[dma((4,))],
    )(*[pltpu.with_memory_space_constraint(x, pltpu.VMEM) for x in done])


def solution(mesh):
    placed = (
        P(None, "gy", "gx"),
        P(None, "gy", "gx"),
        P("gy", "gx"),
        P("gy", "gx"),
        P("gy", "gx"),
        P(None, ("gy", "gx"), None),
    )
    return jax.shard_map(
        local,
        mesh=mesh,
        in_specs=placed,
        out_specs=(P(None, "gy", "gx"), P(None, "gy", "gx"), P(), P(None, ("gy", "gx"), None)),
        check_vma=False,
    )
```

```python
import functools

import jax
import jax.numpy as jnp
from jax import lax
from jax.experimental import pallas as pl
from jax.experimental.pallas import tpu as pltpu
from jax.sharding import PartitionSpec as P

ITERS = 4
DEEP = 8
PAD = 16
LANES = 128
CHUNK = 16
REACH = 6
MESH = pl.DeviceIdType.MESH
SW, SE, NW, NE = range(4)


def kernel(
    G, Y, R, C, B,
    vel_in, sig_in, mass_in, strength_in, mask_in, forcing_in,
    vel_out, sig_out, res_out, os_out,
    vel, sig, raw_sig, raw_mass, raw_strength, raw_mask, pull, inv_mass, ice, base, force, edge_force, cor,
    bands, ocean, low, high, corner_out, corner_in, strip, f_out, f_in, sums, partial,
    in_sem, f_send, f_recv, e_recv, h_send, h_recv, y_send, y_recv, p_send, p_recv, o_sem, r_send, r_recv, ready,
):
    gx = lax.axis_index("gx")
    gy = lax.axis_index("gy")
    f32 = jnp.float32
    T = PAD + R

    def at(dx, dy):
        return {"gx": lax.rem(gx + dx + G, G), "gy": lax.rem(gy + dy + Y, Y)}

    def remote(src, dst, send, recv, where):
        return pltpu.make_async_remote_copy(
            src_ref=src, dst_ref=dst, send_sem=send, recv_sem=recv, device_id=where, device_id_type=MESH
        )

    def settle(ref, sem):
        pltpu.make_async_copy(ref, ref, sem).wait()

    barrier = pltpu.get_barrier_semaphore()
    partners = [(dx, dy) for dx in range(G) for dy in range(Y) if dx or dy]
    hop = G // 4
    rounds = 5
    known = Y - 1
    for n in range(1, hop + 1):
        known = known + (gx >= n).astype(jnp.int32) + (gx + n < G).astype(jnp.int32)

    def greet(sem):
        for n in range(1, hop + 1):
            for d, there in ((-n, gx >= n), (n, gx + n < G)):

                @pl.when(there)
                def _():
                    pl.semaphore_signal(sem, inc=1, device_id={"gx": gx + d, "gy": gy}, device_id_type=MESH)

        for d in range(1, Y):
            pl.semaphore_signal(sem, inc=1, device_id=at(0, d), device_id_type=MESH)

    def meet(n):
        pl.semaphore_wait(ready.at[n - 2], known)
        if n < rounds:
            greet(ready.at[n - 1])

    greet(barrier)
    inner = pl.ds(PAD, R)
    loads = [
        pltpu.make_async_copy(forcing_in, bands, in_sem.at[0]),
        pltpu.make_async_copy(vel_in, vel.at[:, 0, inner], in_sem.at[1]),
        pltpu.make_async_copy(sig_in, raw_sig.at[:, inner], in_sem.at[2]),
        pltpu.make_async_copy(mass_in, raw_mass.at[inner], in_sem.at[1]),
        pltpu.make_async_copy(strength_in, raw_strength.at[inner], in_sem.at[1]),
        pltpu.make_async_copy(mask_in, raw_mask.at[inner], in_sem.at[2]),
    ]
    for copy in loads:
        copy.start()

    under, over = pl.ds(PAD - DEEP, DEEP), pl.ds(T, DEEP)
    lane8 = lax.broadcasted_iota(jnp.int32, (DEEP, LANES), 1)

    def outside(rows, slot, corners):
        for c in range(2):
            vel[c, 0, rows] = jnp.zeros((DEEP, C), f32)
        for c in range(3):
            raw_sig[c, rows] = jnp.zeros((DEEP, C), f32)
        raw_mass[rows] = jnp.ones((DEEP, C), f32)
        raw_strength[rows] = jnp.zeros((DEEP, C), f32)
        raw_mask[rows] = jnp.zeros((DEEP, C), jnp.int32)
        for c in range(4):
            force[c, rows] = jnp.zeros((DEEP, C), f32)
        f_in[slot] = jnp.zeros((2 * REACH, LANES), f32)
        for c in corners:
            corner_in[c] = jnp.where(lane8 // (2 * DEEP) == 5, 1.0, 0.0)

    has_south, has_north = gy > 0, gy < Y - 1
    pl.when(jnp.logical_not(has_south))(lambda: outside(under, 0, (SW, SE)))
    pl.when(jnp.logical_not(has_north))(lambda: outside(over, G + 1, (NW, NE)))

    for ref in (vel, sig):
        for c in range(ref.shape[0]):
            for w in range(2):
                for r in (0, T + DEEP):
                    ref[c, w, r : r + DEEP] = jnp.zeros((DEEP, C), f32)
    for n in range(PAD - DEEP, T + DEEP, DEEP):
        lat = (gy * R + (n - PAD) + lax.broadcasted_iota(jnp.int32, (DEEP, C), 0)).astype(f32)
        cor[n : n + DEEP] = 0.3 + 1.2 * (lat + 0.5) / (R * Y)

    low_half = gx < G // 2
    own_columns = pl.ds(pl.multiple_of(gx * C, C), C)
    mine = pl.ds(pl.multiple_of(gx * B, B), B)
    padded_mine = pl.ds(pl.multiple_of(PAD + gx * B, DEEP), B)
    pl.semaphore_wait(barrier, known)
    greet(ready.at[0])
    loads[0].wait()
    at_end = jnp.logical_or(gx == 0, gx == G - 1)
    on_top = (gx == G - 1).astype(jnp.int32)
    rim_row = on_top * (B - DEEP)
    rest_row = (1 - on_top) * DEEP

    def to_each(d, send, ways=(-1, 1), only=None):
        for way in ways:
            to = gx + way * d
            there = gx >= d if way < 0 else gx + d < G
            if only is not None:
                there = jnp.logical_and(there, only)
            pl.when(there)(lambda: send(to))

    def send_rows_of(to, row, n, sem):
        columns = pl.ds(pl.multiple_of(to * C, C), C)
        src = pl.ds(pl.multiple_of(row, DEEP), n)
        dst = pl.ds(pl.multiple_of(PAD + gx * B + row, DEEP), n)
        where = {"gx": to, "gy": gy}
        remote(bands.at[:, src, columns], force.at[:, dst], f_send.at[0], sem, where).start()

    def send_block(to):
        pl.when(jnp.logical_not(at_end))(lambda: send_rows_of(to, 0, B, f_recv.at[gx]))
        if B > DEEP:
            pl.when(at_end)(lambda: send_rows_of(to, rest_row, B - DEEP, f_recv.at[gx]))

    def strip_to(to, sem):
        where = {"gx": to, "gy": gy}
        remote(f_out.at[to], f_in.at[gx + 1], f_send.at[1], sem, where).start()

    def send_strip(to):
        pl.when(jnp.logical_not(at_end))(lambda: strip_to(to, f_recv.at[gx]))

    def send_both(to):
        send_block(to)
        send_strip(to)

    def send_rim(to):
        send_rows_of(to, rim_row, DEEP, e_recv.at[on_top])
        strip_to(to, e_recv.at[on_top])

    def send_rims(reach):
        for d in range(max(reach - hop, 0) + 1, min(reach, G - 1) + 1):
            to_each(d, send_rim, only=at_end)

    def outward(d, send):
        to_each(d, send, (-1,), low_half)
        to_each(d, send, (1,), jnp.logical_not(low_half))

    def inward(d, send):
        to_each(d, send, (1,), low_half)
        to_each(d, send, (-1,), jnp.logical_not(low_half))

    to_each(hop, send_block)
    chunks = [(n, CHUNK) for n in range(PAD, T, CHUNK)]
    skirts = [(PAD - DEEP, DEEP), (T, DEEP)]

    def prepare(w, p, n, s0, s1, s2, mass, strength, mask):
        ice[w, p : p + n] = mask
        pull[w, p : p + n] = 0.25 * strength * mask
        inv_mass[w, p : p + n] = 1.0 / mass
        sig[0, w, p : p + n] = (s0 + s1) * mask
        sig[1, w, p : p + n] = (s0 - s1) * mask
        sig[2, w, p : p + n] = 2.0 * s2 * mask

    def prepare_main(p, n):
        rows = pl.ds(p, n)
        prepare(
            0, p, n, raw_sig[0, rows], raw_sig[1, rows], raw_sig[2, rows],
            raw_mass[rows], raw_strength[rows], raw_mask[rows].astype(f32),
        )

    settle(bands, in_sem.at[1])
    settle(bands, in_sem.at[2])
    fields = [vel.at[0, 0], vel.at[1, 0], raw_sig.at[0], raw_sig.at[1], raw_sig.at[2], raw_mass, raw_strength, raw_mask]
    west_tile = jnp.zeros((DEEP, LANES), f32)
    east_tile = jnp.zeros((DEEP, LANES), f32)
    for q, field in enumerate(fields):
        t = field[PAD:T, :].astype(f32).T
        lo, hi = t[0:DEEP], t[C - DEEP : C]
        low[q] = lo
        high[q] = hi
        spot = lane8 // (2 * DEEP) == q
        turn = 2 * DEEP * q + DEEP

        def corner(rows):
            both = jnp.where(lane8 < DEEP, rows[:, 0:LANES], rows[:, R - LANES : R])
            return pltpu.roll(both, turn, 1)

        west_tile = jnp.where(spot, corner(lo), west_tile)
        east_tile = jnp.where(spot, corner(hi), east_tile)
    corner_out[0] = west_tile
    corner_out[1] = east_tile

    near, far = pl.ds(0, DEEP), pl.ds(DEEP, DEEP)
    centre = pl.ds(LANES, R)
    bottom, top = pl.ds(PAD, DEEP), pl.ds(T - DEEP, DEEP)
    stacks = (vel, raw_sig, raw_mass, raw_strength, raw_mask)

    def rows_of(ref, rows):
        if ref is vel:
            return ref.at[:, 0, rows]
        return ref.at[:, rows] if len(ref.shape) == 3 else ref.at[rows]

    sides = [
        remote(low, strip.at[:, far, centre], h_send.at[0], h_recv.at[0], at(-1, 0)),
        remote(high, strip.at[:, near, centre], h_send.at[0], h_recv.at[0], at(1, 0)),
    ]
    south = [
        remote(corner_out.at[0], corner_in.at[NE], h_send.at[1], h_recv.at[1], at(-1, -1)),
        remote(corner_out.at[1], corner_in.at[NW], h_send.at[1], h_recv.at[1], at(1, -1)),
    ]
    north = [
        remote(corner_out.at[0], corner_in.at[SE], h_send.at[2], h_recv.at[2], at(-1, 1)),
        remote(corner_out.at[1], corner_in.at[SW], h_send.at[2], h_recv.at[2], at(1, 1)),
    ]
    for c in range(G):
        t = bands[:, :, c * C : (c + 1) * C].reshape(4 * B, C).T
        f_out[(c + 1) % G, 0:REACH, 0 : 4 * B] = t[C - REACH : C]
        f_out[(c + G - 1) % G, REACH : 2 * REACH, 0 : 4 * B] = t[0:REACH]
    wraps = ((gx == 0, 0), (gx == G - 1, 1))

    def corners(wrapped):
        for valid, copies in ((has_south, south), (has_north, north)):
            for edge, n in wraps:
                there = edge if wrapped else jnp.logical_not(edge)
                pl.when(jnp.logical_and(valid, there))(copies[n].start)

    for edge, side in wraps:
        pl.when(jnp.logical_not(edge))(sides[side].start)

    @pl.when(has_south)
    def _():
        for ref in stacks:
            remote(rows_of(ref, bottom), rows_of(ref, over), y_send.at[0], y_recv.at[0], at(0, -1)).start()

    @pl.when(has_north)
    def _():
        for ref in stacks:
            remote(rows_of(ref, top), rows_of(ref, under), y_send.at[1], y_recv.at[1], at(0, 1)).start()

    to_each(hop, send_strip)
    send_rims(hop)
    meet(2)
    corners(False)
    send_rims(2 * hop)
    for d in range(2 * hop - 1, 0, -1):
        if d % hop:
            outward(d, send_both)
    to_each(2 * hop, send_both)
    f_in[gx + 1] = f_out[gx]
    force[:, padded_mine] = bands[:, :, own_columns]
    meet(3)
    send_rims(3 * hop)
    to_each(3 * hop, send_both)
    for p, m in chunks:
        prepare_main(p, m)
    meet(4)
    send_rims(4 * hop)
    for edge, side in wraps:
        pl.when(edge)(sides[side].start)
    meet(5)
    corners(True)
    for d in range(G - 1, 0, -1):
        if d % hop:
            inward(d, send_both)
            if d > 2 * hop:
                outward(d, send_both)
    skirt = pl.ds(0, 4 * DEEP + 2 * REACH)

    def forward(to_north):
        band = G - 1 if to_north else 0
        way = int(to_north)
        src = pl.ds(T - DEEP if to_north else PAD, DEEP)
        dst = pl.ds(PAD - DEEP if to_north else T, DEEP)

        @pl.when(gx != band)
        def _():
            settle(cor.at[skirt], e_recv.at[way])

        @pl.when(has_north if to_north else has_south)
        def _():
            to = at(0, 1 if to_north else -1)
            remote(force.at[:, src], force.at[:, dst], p_send.at[way], p_recv.at[way], to).start()
            remote(f_in.at[band + 1], f_in.at[0 if to_north else G + 1], p_send.at[way], p_recv.at[way], to).start()

    forward(True)
    forward(False)
    pack8 = pl.ds(0, 8 * DEEP)
    pair = pl.ds(0, 2)

    @pl.when(has_north)
    def _():
        settle(cor.at[pack8], y_recv.at[0])
        settle(corner_in.at[pair], h_recv.at[1])

    @pl.when(has_south)
    def _():
        settle(cor.at[pack8], y_recv.at[1])
        settle(corner_in.at[pair], h_recv.at[2])

    settle(strip.at[:, :, centre], h_recv.at[0])
    for p, n in skirts:
        prepare_main(p, n)
    for q in range(8):
        turn = LANES - (2 * DEEP * q + DEEP)
        for side, (s, n) in ((near, (SW, NW)), (far, (SE, NE))):
            strip[q, side, 0:LANES] = pltpu.roll(corner_in[s], turn, 1)
            strip[q, side, LANES + R : 2 * LANES + R] = pltpu.roll(corner_in[n], turn, 1)
    for tile in range(R // LANES + 2):
        t = strip[:, :, tile * LANES : (tile + 1) * LANES].reshape(8 * 2 * DEEP, LANES).T
        if tile == 0:
            t, p = t[LANES - DEEP :], PAD - DEEP
        elif tile == R // LANES + 1:
            t, p = t[:DEEP], T
        else:
            p = PAD + (tile - 1) * LANES
        for r in range(0, t.shape[0], CHUNK):
            part = t[r : r + CHUNK]
            n = part.shape[0]
            turned = [pltpu.roll(part, LANES - (2 * DEEP * q + DEEP), 1) for q in range(8)]
            vel[0, 1, p + r : p + r + n] = turned[0]
            vel[1, 1, p + r : p + r + n] = turned[1]
            prepare(1, p + r, n, *turned[2:])

    def shifted(a, b, lane):
        ra, rb = pltpu.roll(a, C - 1, 1), pltpu.roll(b, C - 1, 1)
        la, lb = pltpu.roll(a, 1, 1), pltpu.roll(b, 1, 1)
        right, left = lane == C - 1, lane == 0
        return (
            jnp.where(right, rb, ra) - jnp.where(left, lb, la),
            jnp.where(right, ra, rb) - jnp.where(left, la, lb),
        )

    everywhere = skirts[:1] + chunks + skirts[1:]
    row8 = lax.broadcasted_iota(jnp.int32, (DEEP, C), 0)

    def stress_step(last, spans, merge=False):
        for p, n, keep in spans:
            lane = lax.broadcasted_iota(jnp.int32, (n, C), 1)
            rows = pl.ds(p, n)
            dxu = shifted(vel[0, 0, rows], vel[0, 1, rows], lane)
            dxv = shifted(vel[1, 0, rows], vel[1, 1, rows], lane)
            for w in range(2):
                dyu = vel[0, w, p + 1 : p + n + 1] - vel[0, w, p - 1 : p + n - 1]
                dyv = vel[1, w, p + 1 : p + n + 1] - vel[1, w, p - 1 : p + n - 1]
                div = dxu[w] + dyv
                ten = dxu[w] - dyv
                shear = dyu + dxv[w]
                inv = lax.rsqrt(div * div + 0.25 * (ten * ten + shear * shear) + 0.01)
                hold = pull[w, rows]
                scaled = hold * inv
                quarter = 0.25 * scaled
                spread = scaled * div - hold
                twist = quarter * ten
                old = [sig[c, w, rows] for c in range(3)]
                new = [
                    0.75 * old[0] + (spread + twist),
                    0.75 * old[1] + (spread - twist),
                    0.75 * old[2] + quarter * shear,
                ]
                if keep is not None:
                    new = [jnp.where(keep, a, b) for a, b in zip(new, old)]
                for c in range(3):
                    sig[c, w, rows] = new[c]
                if last and w == 0 and PAD <= p < T and (keep is None or merge):
                    sig_out[0, p - PAD : p - PAD + n] = 0.5 * (new[0] + new[1])
                    sig_out[1, p - PAD : p - PAD + n] = 0.5 * (new[0] - new[1])
                    sig_out[2, p - PAD : p - PAD + n] = 0.5 * new[2]

    def drag_of(u, v, cu, cv):
        a = cu - u
        b = cv - v
        y = a * a + b * b + 0.01
        return y * lax.rsqrt(y)

    def velocity_step(k, spans, total, merge=False):
        last = k == ITERS - 1
        for p, n, keep in spans:
            inside = PAD <= p < T
            if last and not inside:
                continue
            lane = lax.broadcasted_iota(jnp.int32, (n, C), 1)
            rows = pl.ds(p, n)
            dxx = shifted(sig[0, 0, rows], sig[0, 1, rows], lane)
            dxy = shifted(sig[2, 0, rows], sig[2, 1, rows], lane)
            spin = cor[rows]
            for w in range(1 if last else 2):
                src = edge_force if w else force
                hi, lo = pl.ds(p + 1, n), pl.ds(p - 1, n)
                east = dxx[w] + (sig[2, w, hi] - sig[2, w, lo])
                north = dxy[w] + (sig[1, w, hi] - sig[1, w, lo])
                u, v = vel[0, w, rows], vel[1, w, rows]
                cu, cv = src[2, rows], src[3, rows]
                im = inv_mass[w, rows]
                if k == 0:
                    bu = u + src[0, rows] * im
                    bv = v + src[1, rows] * im
                    base[0, w, rows] = bu
                    base[1, w, rows] = bv
                else:
                    bu, bv = base[0, w, rows], base[1, w, rows]
                grip = drag_of(u, v, cu, cv) * im
                scale = ice[w, rows] / (5.0 + grip)
                push = 0.25 * im
                new_u = (4.0 * u + bu + east * push + grip * cu + spin * v) * scale
                new_v = (4.0 * v + bv + north * push + grip * cv - spin * u) * scale
                if keep is not None:
                    new_u = jnp.where(keep, new_u, u)
                    new_v = jnp.where(keep, new_v, v)
                if last and (keep is None or merge):
                    vel_out[0, p - PAD : p - PAD + n] = new_u
                    vel_out[1, p - PAD : p - PAD + n] = new_v
                    drag = drag_of(new_u, new_v, cu, cv) * ice[w, rows]
                    ocean[0, p - PAD : p - PAD + n] = drag * (new_u - cu)
                    ocean[1, p - PAD : p - PAD + n] = drag * (new_v - cv)
                else:
                    vel[0, w, rows] = new_u
                    vel[1, w, rows] = new_v
                if w == 0 and inside:
                    du = new_u - u
                    dv = new_v - v
                    square = du * du + dv * dv
                    for g in range(0, n, DEEP):
                        total = total + square[g : g + DEEP]
        return total

    def spans_of(lo, hi):
        return [(p, min(CHUNK, hi - p), None) for p in range(lo, hi, CHUNK)]

    stress_step(False, [(p, n, None) for p, n in everywhere])

    share = pl.ds(0, 4 * B + 2 * REACH)
    rest = pl.ds(0, 4 * (B - DEEP))
    def arrive(bs):
        for b in bs:

            @pl.when(gx != b)
            def _():
                if 0 < b < G - 1:
                    settle(cor.at[share], f_recv.at[b])
                elif B > DEEP:
                    settle(cor.at[rest], f_recv.at[b])

    def edges(bs):
        for s in range(0, len(bs), 8):
            group = bs[s : s + 8]
            parts = [f_in[b + 1] for b in group]
            fill = LANES - 2 * REACH * len(group)
            t = jnp.concatenate(parts + [jnp.zeros((fill, LANES), f32)], axis=0).T
            for n, b in enumerate(group):
                turn = LANES - (2 * REACH * n + REACH)
                for c in range(4):
                    part = t[c * B : (c + 1) * B]
                    if b == -1:
                        edge_force[c, under] = pltpu.roll(part[B - DEEP :], turn, 1)
                    elif b == G:
                        edge_force[c, over] = pltpu.roll(part[:DEEP], turn, 1)
                    else:
                        edge_force[c, PAD + b * B : PAD + (b + 1) * B] = pltpu.roll(part, turn, 1)

    def send_rows(b, r, n):
        @pl.when(gx != b)
        def _():
            remote(
                ocean.at[:, pl.ds(b * B + r, n)], os_out.at[:, pl.ds(r, n), own_columns],
                o_sem.at[0], o_sem.at[1], {"gx": b, "gy": gy},
            ).start()

    outer = gx >= G - hop

    def phases(is_low):
        late = list(range(G // 2, G // 2 + G // 4)) if is_low else list(range(G // 2 - G // 4, G // 2))
        early = [b for b in range(G) if b not in late]
        w0, w1 = PAD + late[0] * B, PAD + (late[-1] + 1) * B
        def first(h, side):
            if side == 0:
                keep = None if h == 0 else row8 < DEEP - h
                return [(PAD - DEEP, DEEP, None)] + spans_of(PAD, w0 - DEEP) + [(w0 - DEEP, DEEP, keep)]
            keep = None if h == 0 else row8 >= h
            return [(w1, DEEP, keep)] + spans_of(w1 + DEEP, T) + [(T, DEEP, None)]

        def second(h):
            inside = spans_of(w0, w1)
            if h == 0:
                return inside
            return inside + [(w0 - DEEP, DEEP, row8 >= DEEP - h), (w1, DEEP, row8 < h)]

        totals = [jnp.zeros((DEEP, C), f32)] * ITERS
        left = [(b, 0, B) for b in late]
        for side in range(2):
            bs = [b for b in early if (b > late[0]) == bool(side)]
            arrive(bs)

            @pl.when(has_north if side else has_south)
            def _():
                settle(cor.at[pack8], y_send.at[side])
                settle(cor.at[skirt], p_recv.at[1 - side])

            edges(bs + [G] if side else [-1] + bs)
            totals[0] = velocity_step(0, first(0, side), totals[0])
            for k in range(1, ITERS):
                stress_step(k == ITERS - 1, first(2 * k - 1, side))
                totals[k] = velocity_step(k, first(2 * k, side), totals[k])
            ready_rows = []
            for b in reversed(bs) if side else bs:
                r, n = 0, B
                if b == late[0] - 1:
                    n -= DEEP
                    left.append((b, n, DEEP))
                elif b == late[-1] + 1:
                    r, n = DEEP, n - DEEP
                    left.append((b, 0, DEEP))
                if n:
                    ready_rows.append((b, r, n))

            def send_ready(pieces=tuple(ready_rows)):
                for piece in pieces:
                    send_rows(*piece)

            if side == 0:
                pl.when(jnp.logical_not(outer))(send_ready)
                later = send_ready
            else:
                send_ready()
                pl.when(outer)(later)
        arrive(late)
        edges(late)
        totals[0] = velocity_step(0, second(0), totals[0])
        for k in range(1, ITERS):
            stress_step(k == ITERS - 1, second(2 * k - 1), True)
            totals[k] = velocity_step(k, second(2 * k), totals[k], True)
        answer = jnp.zeros((1, LANES), f32)
        for k in range(ITERS):
            answer = jnp.where(lane1 == k, jnp.sum(jnp.sum(totals[k], axis=0, keepdims=True), axis=1, keepdims=True), answer)
        sums[...] = answer
        me = gx * Y + gy
        for j in range(len(partners)):
            peer = j + (j >= me).astype(jnp.int32)
            where = {"gx": lax.div(peer, Y), "gy": lax.rem(peer, Y)}
            remote(sums, partial.at[me], r_send.at[0], r_recv.at[0], where).start()
        partial[me] = answer
        for b, r, n in left:
            send_rows(b, r, n)

    lane1 = lax.broadcasted_iota(jnp.int32, (1, LANES), 1)
    pl.when(low_half)(lambda: phases(True))
    pl.when(jnp.logical_not(low_half))(lambda: phases(False))
    os_out[:, :, own_columns] = ocean[:, mine]
    most = pl.ds(0, (G - 1) * C)
    settle(os_out.at[:, :, most], o_sem.at[1])
    peers = pl.ds(0, len(partners))
    settle(partial.at[peers], r_recv.at[0])
    res_out[...] = jnp.sum(partial[...], axis=0)[0, :ITERS]
    settle(bands.at[:, :, most], f_send.at[0])
    settle(f_out.at[pl.ds(0, G - 1)], f_send.at[1])
    settle(os_out.at[:, :, most], o_sem.at[0])
    settle(strip.at[:, :, centre], h_send.at[0])

    @pl.when(has_south)
    def _():
        settle(corner_in.at[pair], h_send.at[1])
        settle(cor.at[skirt], p_send.at[0])

    @pl.when(has_north)
    def _():
        settle(corner_in.at[pair], h_send.at[2])
        settle(cor.at[skirt], p_send.at[1])

    settle(partial.at[peers], r_send.at[0])


def store(vel, sig, res, ocean, vel_out, sig_out, res_out, ocean_out, sem):
    pairs = ((sig, sig_out), (vel, vel_out), (ocean, ocean_out), (res, res_out))
    copies = [pltpu.make_async_copy(src, dst, sem.at[n]) for n, (src, dst) in enumerate(pairs)]
    for copy in copies:
        copy.start()
    for copy in copies:
        copy.wait()


def local(velocity, stress, ice_mass, strength, land_mask, ocean_forcing):
    G, Y = lax.axis_size("gx"), lax.axis_size("gy")
    R, C = velocity.shape[1:]
    B = ocean_forcing.shape[1]
    f32 = jnp.float32
    rows = R + 2 * PAD
    dma = pltpu.SemaphoreType.DMA
    any_space = pl.BlockSpec(memory_space=pl.ANY)
    vmem_space = pl.BlockSpec(memory_space=pltpu.VMEM)
    done = pl.pallas_call(
        functools.partial(kernel, G, Y, R, C, B),
        out_shape=(
            pltpu.VMEM(velocity.shape, f32),
            pltpu.VMEM(stress.shape, f32),
            pltpu.VMEM((ITERS,), f32),
            pltpu.VMEM((2,) + ocean_forcing.shape[1:], f32),
        ),
        in_specs=[any_space] * 6,
        out_specs=(vmem_space,) * 4,
        scratch_shapes=[
            pltpu.VMEM((2, 2, rows, C), f32),
            pltpu.VMEM((3, 2, rows, C), f32),
            pltpu.VMEM((3, rows, C), f32),
            pltpu.VMEM((rows, C), f32),
            pltpu.VMEM((rows, C), f32),
            pltpu.VMEM((rows, C), jnp.int32),
            pltpu.VMEM((2, rows, C), f32),
            pltpu.VMEM((2, rows, C), f32),
            pltpu.VMEM((2, rows, C), f32),
            pltpu.VMEM((2, 2, rows, C), f32),
            pltpu.VMEM((4, rows, C), f32),
            pltpu.VMEM((4, rows, C), f32),
            pltpu.VMEM((rows, C), f32),
            pltpu.VMEM(ocean_forcing.shape, f32),
            pltpu.VMEM((2, R, C), f32),
            pltpu.VMEM((8, DEEP, R), f32),
            pltpu.VMEM((8, DEEP, R), f32),
            pltpu.VMEM((2, DEEP, LANES), f32),
            pltpu.VMEM((4, DEEP, LANES), f32),
            pltpu.VMEM((8, 2 * DEEP, R + 2 * LANES), f32),
            pltpu.VMEM((G, 2 * REACH, LANES), f32),
            pltpu.VMEM((G + 2, 2 * REACH, LANES), f32),
            pltpu.VMEM((1, LANES), f32),
            pltpu.VMEM((G * Y, 1, LANES), f32),
            dma((3,)),
            dma((2,)),
            dma((G,)),
            dma((2,)),
            dma((3,)),
            dma((3,)),
            dma((2,)),
            dma((2,)),
            dma((2,)),
            dma((2,)),
            dma((2,)),
            dma((1,)),
            dma((1,)),
            pltpu.SemaphoreType.REGULAR((4,)),
        ],
        compiler_params=pltpu.CompilerParams(collective_id=0, has_side_effects=True),
    )(velocity, stress, ice_mass, strength, land_mask, ocean_forcing)
    return pl.pallas_call(
        store,
        out_shape=tuple(jax.ShapeDtypeStruct(x.shape, f32) for x in done),
        in_specs=[vmem_space] * 4,
        out_specs=(any_space,) * 4,
        scratch_shapes=[dma((4,))],
    )(*[pltpu.with_memory_space_constraint(x, pltpu.VMEM) for x in done])


def solution(mesh):
    placed = (
        P(None, "gy", "gx"),
        P(None, "gy", "gx"),
        P("gy", "gx"),
        P("gy", "gx"),
        P("gy", "gx"),
        P(None, ("gy", "gx"), None),
    )
    return jax.shard_map(
        local,
        mesh=mesh,
        in_specs=placed,
        out_specs=(P(None, "gy", "gx"), P(None, "gy", "gx"), P(), P(None, ("gy", "gx"), None)),
        check_vma=False,
    )
```

```python
import functools

import jax
import jax.numpy as jnp
from jax import lax
from jax.experimental import pallas as pl
from jax.experimental.pallas import tpu as pltpu
from jax.sharding import PartitionSpec as P

ITERS = 4
DEEP = 8
PAD = 16
LANES = 128
CHUNK = 16
REACH = 6
MESH = pl.DeviceIdType.MESH
SW, SE, NW, NE = range(4)


def kernel(
    G, Y, R, C, B,
    vel_in, sig_in, mass_in, strength_in, mask_in, forcing_in,
    vel_out, sig_out, res_out, os_out,
    vel, sig, raw_sig, raw_mass, raw_strength, raw_mask, pull, inv_mass, ice, base, force, edge_force, cor,
    bands, ocean, low, high, corner_out, corner_in, strip, f_out, f_in, sums, partial,
    in_sem, f_send, f_recv, e_recv, h_send, h_recv, y_send, y_recv, p_send, p_recv, o_sem, r_send, r_recv, ready,
):
    gx = lax.axis_index("gx")
    gy = lax.axis_index("gy")
    f32 = jnp.float32
    T = PAD + R

    def at(dx, dy):
        return {"gx": lax.rem(gx + dx + G, G), "gy": lax.rem(gy + dy + Y, Y)}

    def remote(src, dst, send, recv, where):
        return pltpu.make_async_remote_copy(
            src_ref=src, dst_ref=dst, send_sem=send, recv_sem=recv, device_id=where, device_id_type=MESH
        )

    def settle(ref, sem):
        pltpu.make_async_copy(ref, ref, sem).wait()

    barrier = pltpu.get_barrier_semaphore()
    partners = [(dx, dy) for dx in range(G) for dy in range(Y) if dx or dy]
    hop = G // 4
    rounds = 5
    known = Y - 1
    for n in range(1, hop + 1):
        known = known + (gx >= n).astype(jnp.int32) + (gx + n < G).astype(jnp.int32)

    def greet(sem):
        for n in range(1, hop + 1):
            for d, there in ((-n, gx >= n), (n, gx + n < G)):

                @pl.when(there)
                def _():
                    pl.semaphore_signal(sem, inc=1, device_id={"gx": gx + d, "gy": gy}, device_id_type=MESH)

        for d in range(1, Y):
            pl.semaphore_signal(sem, inc=1, device_id=at(0, d), device_id_type=MESH)

    def meet(n):
        pl.semaphore_wait(ready.at[n - 2], known)
        if n < rounds:
            greet(ready.at[n - 1])

    greet(barrier)
    inner = pl.ds(PAD, R)
    loads = [
        pltpu.make_async_copy(forcing_in, bands, in_sem.at[0]),
        pltpu.make_async_copy(vel_in, vel.at[:, 0, inner], in_sem.at[1]),
        pltpu.make_async_copy(sig_in, raw_sig.at[:, inner], in_sem.at[2]),
        pltpu.make_async_copy(mass_in, raw_mass.at[inner], in_sem.at[1]),
        pltpu.make_async_copy(strength_in, raw_strength.at[inner], in_sem.at[1]),
        pltpu.make_async_copy(mask_in, raw_mask.at[inner], in_sem.at[2]),
    ]
    for copy in loads:
        copy.start()

    under, over = pl.ds(PAD - DEEP, DEEP), pl.ds(T, DEEP)
    lane8 = lax.broadcasted_iota(jnp.int32, (DEEP, LANES), 1)

    def outside(rows, slot, corners):
        for c in range(2):
            vel[c, 0, rows] = jnp.zeros((DEEP, C), f32)
        for c in range(3):
            raw_sig[c, rows] = jnp.zeros((DEEP, C), f32)
        raw_mass[rows] = jnp.ones((DEEP, C), f32)
        raw_strength[rows] = jnp.zeros((DEEP, C), f32)
        raw_mask[rows] = jnp.zeros((DEEP, C), jnp.int32)
        for c in range(4):
            force[c, rows] = jnp.zeros((DEEP, C), f32)
        f_in[slot] = jnp.zeros((2 * REACH, LANES), f32)
        for c in corners:
            corner_in[c] = jnp.where(lane8 // (2 * DEEP) == 5, 1.0, 0.0)

    has_south, has_north = gy > 0, gy < Y - 1
    pl.when(jnp.logical_not(has_south))(lambda: outside(under, 0, (SW, SE)))
    pl.when(jnp.logical_not(has_north))(lambda: outside(over, G + 1, (NW, NE)))

    for ref in (vel, sig):
        for c in range(ref.shape[0]):
            for w in range(2):
                for r in (0, T + DEEP):
                    ref[c, w, r : r + DEEP] = jnp.zeros((DEEP, C), f32)
    for n in range(PAD - DEEP, T + DEEP, DEEP):
        lat = (gy * R + (n - PAD) + lax.broadcasted_iota(jnp.int32, (DEEP, C), 0)).astype(f32)
        cor[n : n + DEEP] = 0.3 + 1.2 * (lat + 0.5) / (R * Y)

    low_half = gx < G // 2
    own_columns = pl.ds(pl.multiple_of(gx * C, C), C)
    mine = pl.ds(pl.multiple_of(gx * B, B), B)
    padded_mine = pl.ds(pl.multiple_of(PAD + gx * B, DEEP), B)
    pl.semaphore_wait(barrier, known)
    greet(ready.at[0])
    loads[0].wait()
    at_end = jnp.logical_or(gx == 0, gx == G - 1)
    on_top = (gx == G - 1).astype(jnp.int32)
    rim_row = on_top * (B - DEEP)
    rest_row = (1 - on_top) * DEEP

    def to_each(d, send, ways=(-1, 1), only=None):
        for way in ways:
            to = gx + way * d
            there = gx >= d if way < 0 else gx + d < G
            if only is not None:
                there = jnp.logical_and(there, only)
            pl.when(there)(lambda: send(to))

    def send_rows_of(to, row, n, sem):
        columns = pl.ds(pl.multiple_of(to * C, C), C)
        src = pl.ds(pl.multiple_of(row, DEEP), n)
        dst = pl.ds(pl.multiple_of(PAD + gx * B + row, DEEP), n)
        where = {"gx": to, "gy": gy}
        remote(bands.at[:, src, columns], force.at[:, dst], f_send.at[0], sem, where).start()

    def send_block(to):
        pl.when(jnp.logical_not(at_end))(lambda: send_rows_of(to, 0, B, f_recv.at[gx]))
        if B > DEEP:
            pl.when(at_end)(lambda: send_rows_of(to, rest_row, B - DEEP, f_recv.at[gx]))

    def strip_to(to, sem):
        where = {"gx": to, "gy": gy}
        remote(f_out.at[to], f_in.at[gx + 1], f_send.at[1], sem, where).start()

    def send_strip(to):
        pl.when(jnp.logical_not(at_end))(lambda: strip_to(to, f_recv.at[gx]))

    def send_both(to):
        send_block(to)
        send_strip(to)

    def send_rim(to):
        send_rows_of(to, rim_row, DEEP, e_recv.at[on_top])
        strip_to(to, e_recv.at[on_top])

    def send_rims(reach):
        for d in range(max(reach - hop, 0) + 1, min(reach, G - 1) + 1):
            to_each(d, send_rim, only=at_end)

    def outward(d, send):
        to_each(d, send, (-1,), low_half)
        to_each(d, send, (1,), jnp.logical_not(low_half))

    def inward(d, send):
        to_each(d, send, (1,), low_half)
        to_each(d, send, (-1,), jnp.logical_not(low_half))

    to_each(hop, send_block)
    chunks = [(n, CHUNK) for n in range(PAD, T, CHUNK)]
    skirts = [(PAD - DEEP, DEEP), (T, DEEP)]

    def prepare(w, p, n, s0, s1, s2, mass, strength, mask):
        ice[w, p : p + n] = mask
        pull[w, p : p + n] = 0.25 * strength * mask
        inv_mass[w, p : p + n] = 1.0 / mass
        sig[0, w, p : p + n] = (s0 + s1) * mask
        sig[1, w, p : p + n] = (s0 - s1) * mask
        sig[2, w, p : p + n] = 2.0 * s2 * mask

    def prepare_main(p, n):
        rows = pl.ds(p, n)
        prepare(
            0, p, n, raw_sig[0, rows], raw_sig[1, rows], raw_sig[2, rows],
            raw_mass[rows], raw_strength[rows], raw_mask[rows].astype(f32),
        )

    settle(bands, in_sem.at[1])
    settle(bands, in_sem.at[2])
    fields = [vel.at[0, 0], vel.at[1, 0], raw_sig.at[0], raw_sig.at[1], raw_sig.at[2], raw_mass, raw_strength, raw_mask]
    west_tile = jnp.zeros((DEEP, LANES), f32)
    east_tile = jnp.zeros((DEEP, LANES), f32)
    for q, field in enumerate(fields):
        t = field[PAD:T, :].astype(f32).T
        lo, hi = t[0:DEEP], t[C - DEEP : C]
        low[q] = lo
        high[q] = hi
        spot = lane8 // (2 * DEEP) == q
        turn = 2 * DEEP * q + DEEP

        def corner(rows):
            both = jnp.where(lane8 < DEEP, rows[:, 0:LANES], rows[:, R - LANES : R])
            return pltpu.roll(both, turn, 1)

        west_tile = jnp.where(spot, corner(lo), west_tile)
        east_tile = jnp.where(spot, corner(hi), east_tile)
    corner_out[0] = west_tile
    corner_out[1] = east_tile

    near, far = pl.ds(0, DEEP), pl.ds(DEEP, DEEP)
    centre = pl.ds(LANES, R)
    bottom, top = pl.ds(PAD, DEEP), pl.ds(T - DEEP, DEEP)
    stacks = (vel, raw_sig, raw_mass, raw_strength, raw_mask)

    def rows_of(ref, rows):
        if ref is vel:
            return ref.at[:, 0, rows]
        return ref.at[:, rows] if len(ref.shape) == 3 else ref.at[rows]

    sides = [
        remote(low, strip.at[:, far, centre], h_send.at[0], h_recv.at[0], at(-1, 0)),
        remote(high, strip.at[:, near, centre], h_send.at[0], h_recv.at[0], at(1, 0)),
    ]
    south = [
        remote(corner_out.at[0], corner_in.at[NE], y_send.at[0], y_recv.at[0], at(-1, -1)),
        remote(corner_out.at[1], corner_in.at[NW], y_send.at[0], y_recv.at[0], at(1, -1)),
    ]
    north = [
        remote(corner_out.at[0], corner_in.at[SE], y_send.at[1], y_recv.at[1], at(-1, 1)),
        remote(corner_out.at[1], corner_in.at[SW], y_send.at[1], y_recv.at[1], at(1, 1)),
    ]
    for c in range(G):
        t = bands[:, :, c * C : (c + 1) * C].reshape(4 * B, C).T
        f_out[(c + 1) % G, 0:REACH, 0 : 4 * B] = t[C - REACH : C]
        f_out[(c + G - 1) % G, REACH : 2 * REACH, 0 : 4 * B] = t[0:REACH]
    wraps = ((gx == 0, 0), (gx == G - 1, 1))

    def corners(wrapped):
        for valid, copies in ((has_south, south), (has_north, north)):
            for edge, n in wraps:
                there = edge if wrapped else jnp.logical_not(edge)
                pl.when(jnp.logical_and(valid, there))(copies[n].start)

    for edge, side in wraps:
        pl.when(jnp.logical_not(edge))(sides[side].start)

    @pl.when(has_south)
    def _():
        for ref in stacks:
            remote(rows_of(ref, bottom), rows_of(ref, over), y_send.at[0], y_recv.at[0], at(0, -1)).start()

    @pl.when(has_north)
    def _():
        for ref in stacks:
            remote(rows_of(ref, top), rows_of(ref, under), y_send.at[1], y_recv.at[1], at(0, 1)).start()

    to_each(hop, send_strip)
    send_rims(hop)
    meet(2)
    corners(False)
    send_rims(2 * hop)
    for d in range(2 * hop - 1, 0, -1):
        if d % hop:
            outward(d, send_both)
    to_each(2 * hop, send_both)
    f_in[gx + 1] = f_out[gx]
    force[:, padded_mine] = bands[:, :, own_columns]
    meet(3)
    send_rims(3 * hop)
    to_each(3 * hop, send_both)
    for p, m in chunks:
        prepare_main(p, m)
    meet(4)
    send_rims(4 * hop)
    for edge, side in wraps:
        pl.when(edge)(sides[side].start)
    meet(5)
    corners(True)
    for d in range(G - 1, 0, -1):
        if d % hop:
            inward(d, send_both)
            if d > 2 * hop:
                outward(d, send_both)
    skirt = pl.ds(0, 4 * DEEP + 2 * REACH)

    def forward(to_north):
        band = G - 1 if to_north else 0
        way = int(to_north)
        src = pl.ds(T - DEEP if to_north else PAD, DEEP)
        dst = pl.ds(PAD - DEEP if to_north else T, DEEP)

        @pl.when(gx != band)
        def _():
            settle(cor.at[skirt], e_recv.at[way])

        @pl.when(has_north if to_north else has_south)
        def _():
            to = at(0, 1 if to_north else -1)
            remote(force.at[:, src], force.at[:, dst], p_send.at[way], p_recv.at[way], to).start()
            remote(f_in.at[band + 1], f_in.at[0 if to_north else G + 1], p_send.at[way], p_recv.at[way], to).start()

    forward(True)
    forward(False)
    pack8 = pl.ds(0, 8 * DEEP + 2 * DEEP)

    @pl.when(has_north)
    def _():
        settle(cor.at[pack8], y_recv.at[0])

    @pl.when(has_south)
    def _():
        settle(cor.at[pack8], y_recv.at[1])

    settle(strip.at[:, :, centre], h_recv.at[0])
    for p, n in skirts:
        prepare_main(p, n)
    for q in range(8):
        turn = LANES - (2 * DEEP * q + DEEP)
        for side, (s, n) in ((near, (SW, NW)), (far, (SE, NE))):
            strip[q, side, 0:LANES] = pltpu.roll(corner_in[s], turn, 1)
            strip[q, side, LANES + R : 2 * LANES + R] = pltpu.roll(corner_in[n], turn, 1)
    for tile in range(R // LANES + 2):
        t = strip[:, :, tile * LANES : (tile + 1) * LANES].reshape(8 * 2 * DEEP, LANES).T
        if tile == 0:
            t, p = t[LANES - DEEP :], PAD - DEEP
        elif tile == R // LANES + 1:
            t, p = t[:DEEP], T
        else:
            p = PAD + (tile - 1) * LANES
        for r in range(0, t.shape[0], CHUNK):
            part = t[r : r + CHUNK]
            n = part.shape[0]
            turned = [pltpu.roll(part, LANES - (2 * DEEP * q + DEEP), 1) for q in range(8)]
            vel[0, 1, p + r : p + r + n] = turned[0]
            vel[1, 1, p + r : p + r + n] = turned[1]
            prepare(1, p + r, n, *turned[2:])

    def shifted(a, b, lane):
        ra, rb = pltpu.roll(a, C - 1, 1), pltpu.roll(b, C - 1, 1)
        la, lb = pltpu.roll(a, 1, 1), pltpu.roll(b, 1, 1)
        right, left = lane == C - 1, lane == 0
        return (
            jnp.where(right, rb, ra) - jnp.where(left, lb, la),
            jnp.where(right, ra, rb) - jnp.where(left, la, lb),
        )

    everywhere = skirts[:1] + chunks + skirts[1:]
    row8 = lax.broadcasted_iota(jnp.int32, (DEEP, C), 0)

    def stress_step(last, spans, merge=False):
        for p, n, keep in spans:
            lane = lax.broadcasted_iota(jnp.int32, (n, C), 1)
            rows = pl.ds(p, n)
            dxu = shifted(vel[0, 0, rows], vel[0, 1, rows], lane)
            dxv = shifted(vel[1, 0, rows], vel[1, 1, rows], lane)
            for w in range(2):
                dyu = vel[0, w, p + 1 : p + n + 1] - vel[0, w, p - 1 : p + n - 1]
                dyv = vel[1, w, p + 1 : p + n + 1] - vel[1, w, p - 1 : p + n - 1]
                div = dxu[w] + dyv
                ten = dxu[w] - dyv
                shear = dyu + dxv[w]
                inv = lax.rsqrt(div * div + 0.25 * (ten * ten + shear * shear) + 0.01)
                hold = pull[w, rows]
                scaled = hold * inv
                quarter = 0.25 * scaled
                spread = scaled * div - hold
                twist = quarter * ten
                old = [sig[c, w, rows] for c in range(3)]
                new = [
                    0.75 * old[0] + (spread + twist),
                    0.75 * old[1] + (spread - twist),
                    0.75 * old[2] + quarter * shear,
                ]
                if keep is not None:
                    new = [jnp.where(keep, a, b) for a, b in zip(new, old)]
                for c in range(3):
                    sig[c, w, rows] = new[c]
                if last and w == 0 and PAD <= p < T and (keep is None or merge):
                    sig_out[0, p - PAD : p - PAD + n] = 0.5 * (new[0] + new[1])
                    sig_out[1, p - PAD : p - PAD + n] = 0.5 * (new[0] - new[1])
                    sig_out[2, p - PAD : p - PAD + n] = 0.5 * new[2]

    def drag_of(u, v, cu, cv):
        a = cu - u
        b = cv - v
        y = a * a + b * b + 0.01
        return y * lax.rsqrt(y)

    def velocity_step(k, spans, total, merge=False):
        last = k == ITERS - 1
        for p, n, keep in spans:
            inside = PAD <= p < T
            if last and not inside:
                continue
            lane = lax.broadcasted_iota(jnp.int32, (n, C), 1)
            rows = pl.ds(p, n)
            dxx = shifted(sig[0, 0, rows], sig[0, 1, rows], lane)
            dxy = shifted(sig[2, 0, rows], sig[2, 1, rows], lane)
            spin = cor[rows]
            for w in range(1 if last else 2):
                src = edge_force if w else force
                hi, lo = pl.ds(p + 1, n), pl.ds(p - 1, n)
                east = dxx[w] + (sig[2, w, hi] - sig[2, w, lo])
                north = dxy[w] + (sig[1, w, hi] - sig[1, w, lo])
                u, v = vel[0, w, rows], vel[1, w, rows]
                cu, cv = src[2, rows], src[3, rows]
                im = inv_mass[w, rows]
                if k == 0:
                    bu = u + src[0, rows] * im
                    bv = v + src[1, rows] * im
                    base[0, w, rows] = bu
                    base[1, w, rows] = bv
                else:
                    bu, bv = base[0, w, rows], base[1, w, rows]
                grip = drag_of(u, v, cu, cv) * im
                scale = ice[w, rows] / (5.0 + grip)
                push = 0.25 * im
                new_u = (4.0 * u + bu + east * push + grip * cu + spin * v) * scale
                new_v = (4.0 * v + bv + north * push + grip * cv - spin * u) * scale
                if keep is not None:
                    new_u = jnp.where(keep, new_u, u)
                    new_v = jnp.where(keep, new_v, v)
                if last and (keep is None or merge):
                    vel_out[0, p - PAD : p - PAD + n] = new_u
                    vel_out[1, p - PAD : p - PAD + n] = new_v
                    drag = drag_of(new_u, new_v, cu, cv) * ice[w, rows]
                    ocean[0, p - PAD : p - PAD + n] = drag * (new_u - cu)
                    ocean[1, p - PAD : p - PAD + n] = drag * (new_v - cv)
                else:
                    vel[0, w, rows] = new_u
                    vel[1, w, rows] = new_v
                if w == 0 and inside:
                    du = new_u - u
                    dv = new_v - v
                    square = du * du + dv * dv
                    for g in range(0, n, DEEP):
                        total = total + square[g : g + DEEP]
        return total

    def spans_of(lo, hi):
        return [(p, min(CHUNK, hi - p), None) for p in range(lo, hi, CHUNK)]

    stress_step(False, [(p, n, None) for p, n in everywhere])

    share = pl.ds(0, 4 * B + 2 * REACH)
    rest = pl.ds(0, 4 * (B - DEEP))
    def arrive(bs):
        for b in bs:

            @pl.when(gx != b)
            def _():
                if 0 < b < G - 1:
                    settle(cor.at[share], f_recv.at[b])
                elif B > DEEP:
                    settle(cor.at[rest], f_recv.at[b])

    def edges(bs):
        for s in range(0, len(bs), 8):
            group = bs[s : s + 8]
            parts = [f_in[b + 1] for b in group]
            fill = LANES - 2 * REACH * len(group)
            t = jnp.concatenate(parts + [jnp.zeros((fill, LANES), f32)], axis=0).T
            for n, b in enumerate(group):
                turn = LANES - (2 * REACH * n + REACH)
                for c in range(4):
                    part = t[c * B : (c + 1) * B]
                    if b == -1:
                        edge_force[c, under] = pltpu.roll(part[B - DEEP :], turn, 1)
                    elif b == G:
                        edge_force[c, over] = pltpu.roll(part[:DEEP], turn, 1)
                    else:
                        edge_force[c, PAD + b * B : PAD + (b + 1) * B] = pltpu.roll(part, turn, 1)

    def send_rows(b, r, n):
        @pl.when(gx != b)
        def _():
            remote(
                ocean.at[:, pl.ds(b * B + r, n)], os_out.at[:, pl.ds(r, n), own_columns],
                o_sem.at[0], o_sem.at[1], {"gx": b, "gy": gy},
            ).start()

    outer = gx >= G - hop

    def phases(is_low):
        late = list(range(G // 2, G // 2 + G // 4)) if is_low else list(range(G // 2 - G // 4, G // 2))
        early = [b for b in range(G) if b not in late]
        w0, w1 = PAD + late[0] * B, PAD + (late[-1] + 1) * B
        def first(h, side):
            if side == 0:
                keep = None if h == 0 else row8 < DEEP - h
                return [(PAD - DEEP, DEEP, None)] + spans_of(PAD, w0 - DEEP) + [(w0 - DEEP, DEEP, keep)]
            keep = None if h == 0 else row8 >= h
            return [(w1, DEEP, keep)] + spans_of(w1 + DEEP, T) + [(T, DEEP, None)]

        def second(h):
            inside = spans_of(w0, w1)
            if h == 0:
                return inside
            return inside + [(w0 - DEEP, DEEP, row8 >= DEEP - h), (w1, DEEP, row8 < h)]

        totals = [jnp.zeros((DEEP, C), f32)] * ITERS
        left = [(b, 0, B) for b in late]
        for side in range(2):
            bs = [b for b in early if (b > late[0]) == bool(side)]
            arrive(bs)

            @pl.when(has_north if side else has_south)
            def _():
                settle(cor.at[pack8], y_send.at[side])
                settle(cor.at[skirt], p_recv.at[1 - side])

            edges(bs + [G] if side else [-1] + bs)
            totals[0] = velocity_step(0, first(0, side), totals[0])
            for k in range(1, ITERS):
                stress_step(k == ITERS - 1, first(2 * k - 1, side))
                totals[k] = velocity_step(k, first(2 * k, side), totals[k])
            ready_rows = []
            for b in reversed(bs) if side else bs:
                r, n = 0, B
                if b == late[0] - 1:
                    n -= DEEP
                    left.append((b, n, DEEP))
                elif b == late[-1] + 1:
                    r, n = DEEP, n - DEEP
                    left.append((b, 0, DEEP))
                if n:
                    ready_rows.append((b, r, n))

            def send_ready(pieces=tuple(ready_rows)):
                for piece in pieces:
                    send_rows(*piece)

            if side == 0:
                pl.when(jnp.logical_not(outer))(send_ready)
                later = send_ready
            else:
                send_ready()
                pl.when(outer)(later)
        arrive(late)
        edges(late)
        totals[0] = velocity_step(0, second(0), totals[0])
        for k in range(1, ITERS):
            stress_step(k == ITERS - 1, second(2 * k - 1), True)
            totals[k] = velocity_step(k, second(2 * k), totals[k], True)
        answer = jnp.zeros((1, LANES), f32)
        for k in range(ITERS):
            answer = jnp.where(lane1 == k, jnp.sum(jnp.sum(totals[k], axis=0, keepdims=True), axis=1, keepdims=True), answer)
        sums[...] = answer
        me = gx * Y + gy
        for j in range(len(partners)):
            peer = j + (j >= me).astype(jnp.int32)
            where = {"gx": lax.div(peer, Y), "gy": lax.rem(peer, Y)}
            remote(sums, partial.at[me], r_send.at[0], r_recv.at[0], where).start()
        partial[me] = answer
        for b, r, n in left:
            send_rows(b, r, n)

    lane1 = lax.broadcasted_iota(jnp.int32, (1, LANES), 1)
    pl.when(low_half)(lambda: phases(True))
    pl.when(jnp.logical_not(low_half))(lambda: phases(False))
    os_out[:, :, own_columns] = ocean[:, mine]
    most = pl.ds(0, (G - 1) * C)
    settle(os_out.at[:, :, most], o_sem.at[1])
    peers = pl.ds(0, len(partners))
    settle(partial.at[peers], r_recv.at[0])
    res_out[...] = jnp.sum(partial[...], axis=0)[0, :ITERS]
    settle(bands.at[:, :, most], f_send.at[0])
    settle(f_out.at[pl.ds(0, G - 1)], f_send.at[1])
    settle(os_out.at[:, :, most], o_sem.at[0])
    settle(strip.at[:, :, centre], h_send.at[0])

    @pl.when(has_south)
    def _():
        settle(cor.at[skirt], p_send.at[0])

    @pl.when(has_north)
    def _():
        settle(cor.at[skirt], p_send.at[1])

    settle(partial.at[peers], r_send.at[0])


def store(vel, sig, res, ocean, vel_out, sig_out, res_out, ocean_out, sem):
    pairs = ((sig, sig_out), (vel, vel_out), (ocean, ocean_out), (res, res_out))
    copies = [pltpu.make_async_copy(src, dst, sem.at[n]) for n, (src, dst) in enumerate(pairs)]
    for copy in copies:
        copy.start()
    for copy in copies:
        copy.wait()


def local(velocity, stress, ice_mass, strength, land_mask, ocean_forcing):
    G, Y = lax.axis_size("gx"), lax.axis_size("gy")
    R, C = velocity.shape[1:]
    B = ocean_forcing.shape[1]
    f32 = jnp.float32
    rows = R + 2 * PAD
    dma = pltpu.SemaphoreType.DMA
    any_space = pl.BlockSpec(memory_space=pl.ANY)
    vmem_space = pl.BlockSpec(memory_space=pltpu.VMEM)
    done = pl.pallas_call(
        functools.partial(kernel, G, Y, R, C, B),
        out_shape=(
            pltpu.VMEM(velocity.shape, f32),
            pltpu.VMEM(stress.shape, f32),
            pltpu.VMEM((ITERS,), f32),
            pltpu.VMEM((2,) + ocean_forcing.shape[1:], f32),
        ),
        in_specs=[any_space] * 6,
        out_specs=(vmem_space,) * 4,
        scratch_shapes=[
            pltpu.VMEM((2, 2, rows, C), f32),
            pltpu.VMEM((3, 2, rows, C), f32),
            pltpu.VMEM((3, rows, C), f32),
            pltpu.VMEM((rows, C), f32),
            pltpu.VMEM((rows, C), f32),
            pltpu.VMEM((rows, C), jnp.int32),
            pltpu.VMEM((2, rows, C), f32),
            pltpu.VMEM((2, rows, C), f32),
            pltpu.VMEM((2, rows, C), f32),
            pltpu.VMEM((2, 2, rows, C), f32),
            pltpu.VMEM((4, rows, C), f32),
            pltpu.VMEM((4, rows, C), f32),
            pltpu.VMEM((rows, C), f32),
            pltpu.VMEM(ocean_forcing.shape, f32),
            pltpu.VMEM((2, R, C), f32),
            pltpu.VMEM((8, DEEP, R), f32),
            pltpu.VMEM((8, DEEP, R), f32),
            pltpu.VMEM((2, DEEP, LANES), f32),
            pltpu.VMEM((4, DEEP, LANES), f32),
            pltpu.VMEM((8, 2 * DEEP, R + 2 * LANES), f32),
            pltpu.VMEM((G, 2 * REACH, LANES), f32),
            pltpu.VMEM((G + 2, 2 * REACH, LANES), f32),
            pltpu.VMEM((1, LANES), f32),
            pltpu.VMEM((G * Y, 1, LANES), f32),
            dma((3,)),
            dma((2,)),
            dma((G,)),
            dma((2,)),
            dma((1,)),
            dma((1,)),
            dma((2,)),
            dma((2,)),
            dma((2,)),
            dma((2,)),
            dma((2,)),
            dma((1,)),
            dma((1,)),
            pltpu.SemaphoreType.REGULAR((4,)),
        ],
        compiler_params=pltpu.CompilerParams(collective_id=0, has_side_effects=True),
    )(velocity, stress, ice_mass, strength, land_mask, ocean_forcing)
    return pl.pallas_call(
        store,
        out_shape=tuple(jax.ShapeDtypeStruct(x.shape, f32) for x in done),
        in_specs=[vmem_space] * 4,
        out_specs=(any_space,) * 4,
        scratch_shapes=[dma((4,))],
    )(*[pltpu.with_memory_space_constraint(x, pltpu.VMEM) for x in done])


def solution(mesh):
    placed = (
        P(None, "gy", "gx"),
        P(None, "gy", "gx"),
        P("gy", "gx"),
        P("gy", "gx"),
        P("gy", "gx"),
        P(None, ("gy", "gx"), None),
    )
    return jax.shard_map(
        local,
        mesh=mesh,
        in_specs=placed,
        out_specs=(P(None, "gy", "gx"), P(None, "gy", "gx"), P(), P(None, ("gy", "gx"), None)),
        check_vma=False,
    )
```
